8 devices in a mesh: dp: 1 (over z), tp: 2 (over y), cp: 4 (over x, core).
Axes of the slice: x: 2, y: 2, z: 1, core: 2. Of those that a mesh axis runs over, the one named last changes fastest.
Arguments:
- hidden_in: bfloat16 [64, 64, 1024], P('dp')
- lengths: int32 [64], P('dp')
- k_cache: bfloat16 [64, 16, 2048, 64], P('dp', 'tp', 'cp')
- v_cache: bfloat16 [64, 16, 2048, 64], P('dp', 'tp', 'cp')
- ln1_gain: float32 [1024], replicated
- ln1_bias: float32 [1024], replicated
- ln2_gain: float32 [1024], replicated
- ln2_bias: float32 [1024], replicated
- w_qkv: bfloat16 [1024, 3072], P(None, 'tp')
- b_qkv: bfloat16 [3072], P('tp')
- w_out: bfloat16 [1024, 1024], P('tp')
- b_out: bfloat16 [1024], replicated
- w_up: bfloat16 [1024, 4096], P(None, 'tp')
- b_up: bfloat16 [4096], P('tp')
- w_down: bfloat16 [4096, 1024], P('tp')
- b_down: bfloat16 [1024], replicated
Outputs:
- output 1: bfloat16 [64, 64, 1024], P('dp')
- output 2: bfloat16 [64, 16, 64, 64], P('dp', 'tp')
- output 3: bfloat16 [64, 16, 64, 64], P('dp', 'tp')
All inputs are finite; a program needn't handle non-finite values.
Results may differ from the reference program's by a relative error of at most 0.00426027.
Values sent between devices are 32-bit elements.
A program may use at most 1 GiB of HBM per device.

```python
import math
import jax
import jax.numpy as jnp
from jax import lax

D_MODEL = 1024
NUM_HEADS = 16
HEAD_DIM = 64
FF_DIM = 4096
NUM_ROWS = 64
CHUNK_LEN = 64
CACHE_LEN = 2048
ROT_DIM = HEAD_DIM // 4
SCORE_SCALE = HEAD_DIM ** -0.5
Q_SCALE = math.sqrt(math.log(CACHE_LEN / 4.0))
NEG_BIG = -1e30
EPSILON = 1e-5
ROPE_BASE = 10000.0


def draw_lengths(len_key):
    draw_keys = jax.random.split(len_key, 2)
    drawn = jax.random.randint(draw_keys[0], (NUM_ROWS,), 1, CACHE_LEN + 1, dtype=jnp.int32)
    full_row = jax.random.randint(draw_keys[1], (), 0, NUM_ROWS, dtype=jnp.int32)
    row_ids = jnp.arange(NUM_ROWS, dtype=jnp.int32)
    drawn = jnp.where(row_ids == full_row, CACHE_LEN, drawn)
    return jnp.where(row_ids == (full_row + 1) % NUM_ROWS, 1, drawn).astype(jnp.int32)


def draw_cache(cache_key):
    row_keys = jax.random.split(cache_key, NUM_ROWS)
    return lax.map(lambda row_key: jax.random.normal(row_key, (NUM_HEADS, CACHE_LEN, HEAD_DIM), jnp.float32).astype(jnp.bfloat16), row_keys)


def setup_inputs(seed: int = 0, part: int = 0) -> dict:
    shared = jax.random.split(jax.random.key(seed), 12)
    part_keys = jax.random.split(jax.random.fold_in(jax.random.key(seed + 1), part), 4)
    qkv_gain = jnp.array([Q_SCALE, 1.0, 1.0], jnp.float32).reshape(1, 3, 1)
    hidden_in = 0.5 * jax.random.normal(part_keys[0], (NUM_ROWS, CHUNK_LEN, D_MODEL), jnp.float32)
    w_qkv = jax.random.normal(shared[0], (D_MODEL, NUM_HEADS, 3, HEAD_DIM), jnp.float32) * qkv_gain * D_MODEL ** -0.5
    b_qkv = 0.5 * jax.random.normal(shared[1], (NUM_HEADS, 3, HEAD_DIM), jnp.float32) * qkv_gain
    return {
        "hidden_in": hidden_in.astype(jnp.bfloat16),
        "lengths": draw_lengths(part_keys[1]),
        "k_cache": draw_cache(part_keys[2]),
        "v_cache": draw_cache(part_keys[3]),
        "ln1_gain": 1.0 + 0.2 * jax.random.normal(shared[2], (D_MODEL,), jnp.float32),
        "ln1_bias": 0.2 * jax.random.normal(shared[3], (D_MODEL,), jnp.float32),
        "ln2_gain": 1.0 + 0.2 * jax.random.normal(shared[4], (D_MODEL,), jnp.float32),
        "ln2_bias": 0.2 * jax.random.normal(shared[5], (D_MODEL,), jnp.float32),
        "w_qkv": w_qkv.reshape(D_MODEL, NUM_HEADS * 3 * HEAD_DIM).astype(jnp.bfloat16),
        "b_qkv": b_qkv.reshape(NUM_HEADS * 3 * HEAD_DIM).astype(jnp.bfloat16),
        "w_out": (1.5 * D_MODEL ** -0.5 * jax.random.normal(shared[6], (D_MODEL, D_MODEL), jnp.float32)).astype(jnp.bfloat16),
        "b_out": (0.5 * jax.random.normal(shared[7], (D_MODEL,), jnp.float32)).astype(jnp.bfloat16),
        "w_up": (D_MODEL ** -0.5 * jax.random.normal(shared[8], (D_MODEL, FF_DIM), jnp.float32)).astype(jnp.bfloat16),
        "b_up": (0.5 * jax.random.normal(shared[9], (FF_DIM,), jnp.float32)).astype(jnp.bfloat16),
        "w_down": (FF_DIM ** -0.5 * jax.random.normal(shared[10], (FF_DIM, D_MODEL), jnp.float32)).astype(jnp.bfloat16),
        "b_down": (0.5 * jax.random.normal(shared[11], (D_MODEL,), jnp.float32)).astype(jnp.bfloat16),
    }


def layer_norm(values_in, gain_vec, bias_vec):
    x_f32 = values_in.astype(jnp.float32)
    row_mean = jnp.mean(x_f32, axis=-1, keepdims=True)
    centered = x_f32 - row_mean
    variance = jnp.mean(centered * centered, axis=-1, keepdims=True)
    return (centered * lax.rsqrt(variance + EPSILON) * gain_vec + bias_vec).astype(jnp.bfloat16)


def rotary(values_in, positions):
    half_rot = ROT_DIM // 2
    inv_freq = ROPE_BASE ** (-2.0 * jnp.arange(half_rot, dtype=jnp.float32) / ROT_DIM)
    angles = positions.astype(jnp.float32)[..., None] * inv_freq
    cos_tab = jnp.cos(angles)[..., None, :]
    sin_tab = jnp.sin(angles)[..., None, :]
    rot_first = values_in[..., :half_rot].astype(jnp.float32)
    rot_second = values_in[..., half_rot:ROT_DIM].astype(jnp.float32)
    new_first = rot_first * cos_tab - rot_second * sin_tab
    new_second = rot_second * cos_tab + rot_first * sin_tab
    return jnp.concatenate([new_first.astype(jnp.bfloat16), new_second.astype(jnp.bfloat16), values_in[..., ROT_DIM:]], axis=-1)


def attend_row(operands):
    q_row, kn_row, vn_row, kc_row, vc_row, row_len = operands
    cache_valid = (jnp.arange(CACHE_LEN) < row_len)[None, :]
    causal = jnp.arange(CHUNK_LEN)[:, None] >= jnp.arange(CHUNK_LEN)[None, :]

    def attend_head(head_ops):
        q_head, kn_head, vn_head, kc_head, vc_head = head_ops
        s_cache = jnp.where(cache_valid, jnp.dot(q_head, kc_head.T, preferred_element_type=jnp.float32) * SCORE_SCALE, NEG_BIG)
        s_self = jnp.where(causal, jnp.dot(q_head, kn_head.T, preferred_element_type=jnp.float32) * SCORE_SCALE, NEG_BIG)
        row_max = jnp.maximum(s_cache.max(axis=1), s_self.max(axis=1))[:, None]
        p_cache = jnp.where(cache_valid, jnp.exp(s_cache - row_max), 0.0)
        p_self = jnp.where(causal, jnp.exp(s_self - row_max), 0.0)
        prob_sum = p_cache.sum(axis=1) + p_self.sum(axis=1)
        weighted = jnp.dot(p_cache.astype(jnp.bfloat16), vc_head, preferred_element_type=jnp.float32) + jnp.dot(p_self.astype(jnp.bfloat16), vn_head, preferred_element_type=jnp.float32)
        return (weighted / prob_sum[:, None]).astype(jnp.bfloat16)

    return lax.map(attend_head, (q_row, kn_row, vn_row, kc_row, vc_row))


def reference(hidden_in, lengths, k_cache, v_cache, ln1_gain, ln1_bias, ln2_gain, ln2_bias, w_qkv, b_qkv, w_out, b_out, w_up, b_up, w_down, b_down):
    flat_in = hidden_in.reshape(NUM_ROWS * CHUNK_LEN, D_MODEL)
    normed_attn = layer_norm(flat_in, ln1_gain, ln1_bias)
    normed_mlp = layer_norm(flat_in, ln2_gain, ln2_bias)
    qkv_all = (jnp.dot(normed_attn, w_qkv, preferred_element_type=jnp.float32) + b_qkv.astype(jnp.float32)).astype(jnp.bfloat16)
    qkv_all = qkv_all.reshape(NUM_ROWS, CHUNK_LEN, NUM_HEADS, 3, HEAD_DIM)
    positions = lengths[:, None] + jnp.arange(CHUNK_LEN, dtype=jnp.int32)[None, :]
    q_rot = jnp.swapaxes(rotary(qkv_all[:, :, :, 0], positions), 1, 2)
    k_new = jnp.swapaxes(rotary(qkv_all[:, :, :, 1], positions), 1, 2)
    v_new = jnp.swapaxes(qkv_all[:, :, :, 2], 1, 2)
    context = lax.map(attend_row, (q_rot, k_new, v_new, k_cache, v_cache, lengths))
    context = jnp.swapaxes(context, 1, 2).reshape(NUM_ROWS * CHUNK_LEN, D_MODEL)
    attn_out = jnp.dot(context, w_out, preferred_element_type=jnp.float32)
    hidden = jax.nn.gelu(jnp.dot(normed_mlp, w_up, preferred_element_type=jnp.float32) + b_up.astype(jnp.float32), approximate=False).astype(jnp.bfloat16)
    mlp_out = jnp.dot(hidden, w_down, preferred_element_type=jnp.float32)
    out_sum = flat_in.astype(jnp.float32) + attn_out + b_out.astype(jnp.float32) + mlp_out + b_down.astype(jnp.float32)
    hidden_out = out_sum.astype(jnp.bfloat16).reshape(NUM_ROWS, CHUNK_LEN, D_MODEL)
    return (hidden_out, k_new, v_new)
```

```python
import functools
import numpy as np
import jax
import jax.numpy as jnp
from jax import lax
from jax.experimental import pallas as pl
from jax.experimental.pallas import tpu as pltpu
from jax.sharding import PartitionSpec as P

EPSILON = 1e-5
NEG_BIG = -1e30
MAX_FLOOR = -1e29
ROPE_BASE = 10000.0
HEAD_DIM = 64
ROT_DIM = 16
PAIR = 2 * HEAD_DIM
ROWS = 64
CHUNK = 64
HEADS = 8
WIDTH = HEADS * HEAD_DIM
SLOTS = 512
D_MODEL = 1024
FF = 2048
GROUP = 8
GROUPS = ROWS // GROUP
KV_BUFS = 3
QKV_ROWS = 4
QKV_TOKENS = QKV_ROWS * CHUNK
F32 = jnp.float32
BF16 = jnp.bfloat16
ANY = pl.BlockSpec(memory_space=pl.ANY)


def normalize(x_f32, gain, bias):
    row_mean = jnp.mean(x_f32, axis=-1, keepdims=True)
    centered = x_f32 - row_mean
    variance = jnp.mean(centered * centered, axis=-1, keepdims=True)
    return (centered * lax.rsqrt(variance + EPSILON) * gain + bias).astype(BF16)


def rotate_matrix():
    matrix = np.zeros((PAIR, PAIR), np.float32)
    half = ROT_DIM // 2
    for base in (0, HEAD_DIM):
        for i in range(half):
            matrix[base + half + i, base + i] = -1.0
            matrix[base + i, base + half + i] = 1.0
    return matrix


def qkv_kernel(len_ref, x_ref, gain_ref, bias_ref, w_ref, bq_ref, freq_ref, rot_ref, q_out, k_out, v_out, kd_out, vd_out, w_perm):
    step = pl.program_id(0)

    @pl.when(step == 0)
    def _():
        for part in range(3):
            for pair in range(HEADS // 2):
                first = 2 * pair * 3 * HEAD_DIM + part * HEAD_DIM
                second = first + 3 * HEAD_DIM
                w_perm[:, part * WIDTH + pair * PAIR:part * WIDTH + (pair + 1) * PAIR] = jnp.concatenate([w_ref[:, first:first + HEAD_DIM], w_ref[:, second:second + HEAD_DIM]], axis=1)

    normed = normalize(x_ref[...].astype(F32), gain_ref[...], bias_ref[...])
    lane_token = lax.broadcasted_iota(jnp.int32, (ROT_DIM // 2, QKV_TOKENS), 1)
    base = jnp.zeros((ROT_DIM // 2, QKV_TOKENS), jnp.int32)
    for row in range(QKV_ROWS):
        base = jnp.where(lane_token // CHUNK == row, len_ref[step * QKV_ROWS + row], base)
    angles = (base + lane_token % CHUNK).astype(F32) * freq_ref[:, 0:1]
    cos8 = jnp.cos(angles)
    sin8 = jnp.sin(angles)
    rest = HEAD_DIM - ROT_DIM
    ones = jnp.ones((rest, QKV_TOKENS), F32)
    zeros = jnp.zeros((rest, QKV_TOKENS), F32)
    cos_tab = jnp.concatenate([cos8, cos8, ones, cos8, cos8, ones], axis=0).T
    sin_tab = jnp.concatenate([sin8, sin8, zeros, sin8, sin8, zeros], axis=0).T

    def section(part):
        cols = pl.ds(part * WIDTH, WIDTH)
        return (jnp.dot(normed, w_perm[:, cols], preferred_element_type=F32) + bq_ref[:, cols]).astype(BF16)

    def turn(values):
        pieces = []
        for pair in range(HEADS // 2):
            x = values[:, pair * PAIR:(pair + 1) * PAIR]
            turned = jnp.dot(x, rot_ref[...], preferred_element_type=F32)
            pieces.append(x.astype(F32) * cos_tab + turned * sin_tab)
        return pieces

    q_parts = turn(section(0))
    for pair in range(HEADS // 2):
        q_out[:, pair * PAIR:(pair + 1) * PAIR] = (q_parts[pair] * (HEAD_DIM ** -0.5)).astype(BF16)
    k_parts = turn(section(1))
    v_all = section(2)
    vd_out[...] = v_all
    for pair in range(HEADS // 2):
        k_pair = k_parts[pair].astype(BF16)
        kd_out[:, pair * PAIR:(pair + 1) * PAIR] = k_pair
        v_pair = v_all[:, pair * PAIR:(pair + 1) * PAIR]
        for row in range(QKV_ROWS):
            tokens = slice(row * CHUNK, (row + 1) * CHUNK)
            for sub in range(2):
                dims = slice(sub * HEAD_DIM, (sub + 1) * HEAD_DIM)
                k_out[row, 2 * pair + sub] = k_pair[tokens, dims]
                v_out[row, 2 * pair + sub] = v_pair[tokens, dims]


def qkv_call(lengths, x_flat, gain, bias, w_qkv, b_perm, freq, rot):
    tokens = ROWS * CHUNK
    steps = ROWS // QKV_ROWS
    whole = lambda shape: pl.BlockSpec(shape, lambda i: (0,) * len(shape))
    dense = pl.BlockSpec((QKV_TOKENS, WIDTH), lambda i: (i, 0))
    heads = pl.BlockSpec((QKV_ROWS, HEADS, CHUNK, HEAD_DIM), lambda i: (i, 0, 0, 0))
    return pl.pallas_call(
        qkv_kernel,
        grid=(steps,),
        in_specs=[
            pl.BlockSpec(memory_space=pltpu.SMEM),
            pl.BlockSpec((QKV_TOKENS, D_MODEL), lambda i: (i, 0)),
            whole((1, D_MODEL)), whole((1, D_MODEL)), whole((D_MODEL, 3 * WIDTH)), whole((1, 3 * WIDTH)),
            whole((ROT_DIM // 2, 128)), whole((PAIR, PAIR)),
        ],
        out_specs=[dense, heads, heads, dense, dense],
        out_shape=[
            jax.ShapeDtypeStruct((tokens, WIDTH), BF16),
            jax.ShapeDtypeStruct((ROWS, HEADS, CHUNK, HEAD_DIM), BF16),
            jax.ShapeDtypeStruct((ROWS, HEADS, CHUNK, HEAD_DIM), BF16),
            jax.ShapeDtypeStruct((tokens, WIDTH), BF16),
            jax.ShapeDtypeStruct((tokens, WIDTH), BF16),
        ],
        scratch_shapes=[pltpu.VMEM((D_MODEL, 3 * WIDTH), BF16)],
        cost_estimate=pl.CostEstimate(flops=2 * tokens * D_MODEL * 3 * WIDTH, bytes_accessed=40 << 20, transcendentals=0),
        name="qkv",
    )(lengths, x_flat, gain, bias, w_qkv, b_perm, freq, rot)


def layer_kernel(len_ref, q_hbm, kd_hbm, vd_hbm, kc_hbm, vc_hbm, x_hbm, gain_ref, bias_ref, wo_hbm, wu_hbm, bu_ref, wd_hbm, bo_ref, bd_ref, out_hbm,
                 wo, wu, wd, kbuf, vbuf, qbuf, self_buf, x_buf, o_buf, stat, c_recv, c_stat, cx_stat, x_recv, x_stat, ctx, y_send, y_keep, y_recv, fin, stage,
                 w_sem, kv_sem, self_sem, c_ssem, c_rsem, x_ssem, x_rsem, y_ssem, y_rsem, f_ssem, f_rsem, out_sem):
    tp_id = lax.axis_index("tp")
    cp_id = lax.axis_index("cp")
    chip_x = cp_id // 2
    core = cp_id % 2
    to_core = {"cp": 2 * chip_x + 1 - core}
    to_x = {"cp": 2 * (1 - chip_x) + core}
    to_y = {"tp": 1 - tp_id}

    def flip(bit, mine):
        return bit + mine - 2 * bit * mine

    def row_of(group, slot):
        return group * GROUP + 4 * flip(slot // 4, core) + 2 * flip((slot // 2) % 2, chip_x) + flip(slot % 2, tp_id)

    def remote(src, dst, ssem, rsem, device):
        return pltpu.make_async_remote_copy(src_ref=src, dst_ref=dst, send_sem=ssem, recv_sem=rsem, device_id=device, device_id_type=pl.DeviceIdType.MESH)

    def kv_copies(n):
        b = n % KV_BUFS
        row = row_of(n // GROUP, (n % GROUP + 4) % GROUP)
        return (pltpu.make_async_copy(kc_hbm.at[row], kbuf.at[b], kv_sem.at[b, 0]), pltpu.make_async_copy(vc_hbm.at[row], vbuf.at[b], kv_sem.at[b, 1]), pltpu.make_async_copy(q_hbm.at[row], qbuf.at[b], kv_sem.at[b, 2]))

    def self_copies(g):
        b = g % 2
        copies = []
        for slot in range(2):
            row = row_of(g, slot)
            for k, src in enumerate((q_hbm, kd_hbm, vd_hbm)):
                copies.append(pltpu.make_async_copy(src.at[row], self_buf.at[b, slot, k], self_sem.at[b, slot * 4 + k]))
            copies.append(pltpu.make_async_copy(x_hbm.at[row], x_buf.at[b, slot], self_sem.at[b, slot * 4 + 3]))
        return copies

    w_copies = (pltpu.make_async_copy(wo_hbm, wo, w_sem.at[0]), pltpu.make_async_copy(wu_hbm, wu, w_sem.at[1]), pltpu.make_async_copy(wd_hbm, wd, w_sem.at[2]))

    def c_copies(g):
        return (remote(o_buf.at[g, pl.ds(4, 4)], c_recv.at[g], c_ssem.at[g, 0], c_rsem.at[g, 0], to_core), remote(stat.at[g, 0], c_stat.at[g], c_ssem.at[g, 1], c_rsem.at[g, 1], to_core))

    def x_copies(g):
        return (remote(o_buf.at[g, pl.ds(2, 2)], x_recv.at[g], x_ssem.at[g, 0], x_rsem.at[g, 0], to_x), remote(cx_stat.at[g], x_stat.at[g], x_ssem.at[g, 1], x_rsem.at[g, 1], to_x))

    def y_copy(g):
        return remote(y_send.at[g], y_recv.at[g], y_ssem.at[g], y_rsem.at[g], to_y)

    def f_copy(g, src, dst, k, device):
        return remote(fin.at[g, src], fin.at[g, dst], f_ssem.at[g, k], f_rsem.at[g, dst], device)

    def out_copy(g, slot):
        return pltpu.make_async_copy(stage.at[g % 2, slot], out_hbm.at[row_of(g, slot)], out_sem.at[g % 2, slot])

    lane = lax.broadcasted_iota(jnp.int32, (CHUNK, PAIR), 1)
    low_half = lane < HEAD_DIM
    is_max = lane % 16 < 8

    def stacked_heads(q_pair):
        zero = jnp.zeros_like(q_pair)
        return jnp.concatenate([jnp.where(low_half, q_pair, zero), jnp.where(low_half, zero, q_pair)], axis=0)

    def spread(weights, column):
        return jnp.where(low_half, weights[:, column:column + 1], weights[:, column + 1:column + 2])

    def attend(g, j):
        n = g * GROUP + j
        slot = (j + 4) % GROUP
        b = n % KV_BUFS
        for copy in kv_copies(n):
            copy.wait()

        @pl.when(n + KV_BUFS - 1 < ROWS)
        def _():
            for copy in kv_copies(n + KV_BUFS - 1):
                copy.start()

        row_len = len_ref[row_of(g, slot)]
        slot_ids = cp_id * SLOTS + lax.broadcasted_iota(jnp.int32, (PAIR, SLOTS), 1)
        valid = slot_ids < row_len
        packed = stat[g, j // 4]
        for pair in range(HEADS // 2):
            cols = slice(pair * PAIR, (pair + 1) * PAIR)
            q2 = stacked_heads(qbuf[b, :, cols])
            scores = jnp.where(valid, jnp.dot(q2, kbuf[b, cols, :], preferred_element_type=F32), NEG_BIG)
            top = jnp.maximum(jnp.max(scores, axis=1, keepdims=True), MAX_FLOOR)
            probs = jnp.exp(scores - top)
            total = jnp.sum(probs, axis=1, keepdims=True)
            both = lax.dot_general(probs.astype(BF16), vbuf[b, cols, :], (((1,), (1,)), ((), ())), preferred_element_type=F32)
            o_buf[g, slot, :, cols] = jnp.where(low_half, both[:CHUNK], both[CHUNK:])
            for sub in range(2):
                column = slot % 4 * 16 + 2 * pair + sub
                rows = slice(sub * CHUNK, (sub + 1) * CHUNK)
                packed = jnp.where(lane == column, top[rows], packed)
                packed = jnp.where(lane == column + 8, total[rows], packed)
        stat[g, j // 4] = packed

    def core_stage(g):
        for copy in c_copies(g):
            copy.wait_recv()
        mine = stat[g, 1]
        theirs = c_stat[g]
        top = jnp.maximum(mine, theirs)
        w_mine = jnp.exp(mine - top)
        w_theirs = jnp.exp(theirs - top)
        total = mine * pltpu.roll(w_mine, 8, 1) + theirs * pltpu.roll(w_theirs, 8, 1)
        cx_stat[g] = jnp.where(is_max, top, total)
        for slot in (2, 3, 0, 1):
            for pair in range(HEADS // 2):
                cols = slice(pair * PAIR, (pair + 1) * PAIR)
                column = slot * 16 + 2 * pair
                o_buf[g, slot, :, cols] = o_buf[g, slot, :, cols] * spread(w_mine, column) + c_recv[g, slot, :, cols] * spread(w_theirs, column)
            if slot == 3:
                for copy in x_copies(g):
                    copy.start()

    def x_stage(g):
        b = g % 2
        for copy in self_copies(g):
            copy.wait()
        packed = jnp.where(is_max, NEG_BIG, 0.0)
        causal = lax.broadcasted_iota(jnp.int32, (PAIR, CHUNK), 0) % CHUNK >= lax.broadcasted_iota(jnp.int32, (PAIR, CHUNK), 1)
        own = {}
        for slot in range(2):
            for pair in range(HEADS // 2):
                cols = slice(pair * PAIR, (pair + 1) * PAIR)
                q2 = stacked_heads(self_buf[b, slot, 0, :, cols])
                scores = lax.dot_general(q2, self_buf[b, slot, 1, :, cols], (((1,), (1,)), ((), ())), preferred_element_type=F32)
                scores = jnp.where(causal, scores, NEG_BIG)
                top = jnp.max(scores, axis=1, keepdims=True)
                probs = jnp.where(causal, jnp.exp(scores - top), 0.0)
                total = jnp.sum(probs, axis=1, keepdims=True)
                both = jnp.dot(probs.astype(BF16), self_buf[b, slot, 2, :, cols], preferred_element_type=F32)
                own[slot, pair] = jnp.where(low_half, both[:CHUNK], both[CHUNK:])
                for sub in range(2):
                    column = slot * 16 + 2 * pair + sub
                    rows = slice(sub * CHUNK, (sub + 1) * CHUNK)
                    packed = jnp.where(lane == column, top[rows], packed)
                    packed = jnp.where(lane == column + 8, total[rows], packed)
        x_both = x_buf[b].reshape(2 * CHUNK, D_MODEL).astype(F32)
        normed = normalize(x_both, gain_ref[...], bias_ref[...])
        up = jnp.dot(normed, wu[...], preferred_element_type=F32) + bu_ref[...]
        hidden = (0.5 * up * (1.0 + lax.erf(up * (0.5 ** 0.5)))).astype(BF16)
        for copy in x_copies(g):
            copy.wait_recv()
        mine = cx_stat[g]
        theirs = pltpu.roll(x_stat[g], 96, 1)
        top = jnp.maximum(jnp.maximum(mine, theirs), packed)
        w_mine = jnp.exp(mine - top)
        w_theirs = jnp.exp(theirs - top)
        w_own = jnp.exp(packed - top)
        total = mine * pltpu.roll(w_mine, 8, 1) + theirs * pltpu.roll(w_theirs, 8, 1) + packed * pltpu.roll(w_own, 8, 1)
        inverse = pltpu.roll(1.0 / jnp.where(is_max, 1.0, total), 120, 1)
        w_mine = w_mine * inverse
        w_theirs = w_theirs * inverse
        w_own = w_own * inverse
        for slot in range(2):
            for pair in range(HEADS // 2):
                cols = slice(pair * PAIR, (pair + 1) * PAIR)
                column = slot * 16 + 2 * pair
                value = o_buf[g, slot, :, cols] * spread(w_mine, column) + x_recv[g, slot, :, cols] * spread(w_theirs, column) + own[slot, pair] * spread(w_own, column)
                ctx[slot * CHUNK:(slot + 1) * CHUNK, cols] = value.astype(BF16)
        branch = jnp.dot(ctx[...], wo[...], preferred_element_type=F32) + jnp.dot(hidden, wd[...], preferred_element_type=F32)
        y_send[g] = branch[CHUNK:]
        y_copy(g).start()
        y_keep[b] = branch[:CHUNK] + x_both[:CHUNK] + bo_ref[...] + bd_ref[...]

    def y_stage(g):
        y_copy(g).wait_recv()
        fin[g, 0] = y_keep[g % 2] + y_recv[g]
        f_copy(g, 0, 2, 0, to_x).start()
        f_copy(g, 0, 1, 1, to_y).start()
        f_copy(g, 0, 4, 2, to_core).start()

    def forward_stage(g):
        f_copy(g, 0, 1, 1, to_y).wait_recv()
        f_copy(g, 0, 2, 0, to_x).wait_recv()

        @pl.when(g % 2 == 0)
        def _():
            f_copy(g, 1, 3, 3, to_x).start()

        @pl.when(g % 2 == 1)
        def _():
            f_copy(g, 2, 3, 3, to_y).start()

        f_copy(g, 1, 5, 4, to_core).start()
        f_copy(g, 2, 6, 5, to_core).start()

    def diagonal_stage(g):
        f_copy(g, 1, 3, 3, to_x).wait_recv()
        f_copy(g, 3, 7, 6, to_core).start()

    def out_stage(g):
        f_copy(g, 0, 4, 2, to_core).wait_recv()
        f_copy(g, 1, 5, 4, to_core).wait_recv()
        f_copy(g, 2, 6, 5, to_core).wait_recv()
        f_copy(g, 3, 7, 6, to_core).wait_recv()

        @pl.when(g >= 2)
        def _():
            for slot in range(GROUP):
                out_copy(g - 2, slot).wait()

        for slot in range(GROUP):
            stage[g % 2, slot] = fin[g, slot].astype(BF16)
            out_copy(g, slot).start()

    for n in range(KV_BUFS - 1):
        for copy in kv_copies(n):
            copy.start()
    for copy in w_copies:
        copy.start()
    barrier = pltpu.get_barrier_semaphore()
    for device in (to_core, to_x, to_y):
        pl.semaphore_signal(barrier, inc=1, device_id=device, device_id_type=pl.DeviceIdType.MESH)
    pl.semaphore_wait(barrier, 3)

    def iteration(i, carry):
        @pl.when(i < GROUPS)
        def _():
            for copy in self_copies(i):
                copy.start()
            stat[i, 0] = jnp.zeros((CHUNK, PAIR), F32)
            stat[i, 1] = jnp.zeros((CHUNK, PAIR), F32)

            def attend_half(half, outer):
                def one(j, inner):
                    attend(i, half * 4 + j)
                    return inner

                lax.fori_loop(0, GROUP // 2, one, 0)

                @pl.when(half == 0)
                def _():
                    for copy in c_copies(i):
                        copy.start()

                return outer

            lax.fori_loop(0, 2, attend_half, 0)
            core_stage(i)

        for depth, work in ((1, x_stage), (2, y_stage), (3, forward_stage), (4, diagonal_stage), (5, out_stage)):
            @pl.when(jnp.logical_and(i >= depth, i < GROUPS + depth))
            def _(depth=depth, work=work):
                if depth == 1:
                    @pl.when(i == 1)
                    def _():
                        for copy in w_copies:
                            copy.wait()

                work(i - depth)

        return carry

    lax.fori_loop(0, GROUPS + 5, iteration, 0)
    for g in (GROUPS - 2, GROUPS - 1):
        for slot in range(GROUP):
            out_copy(g, slot).wait()

    def finish(g, carry):
        for copy in c_copies(g) + x_copies(g) + (y_copy(g),):
            copy.wait_send()
        for src, dst, k, device in ((0, 2, 0, to_x), (0, 1, 1, to_y), (0, 4, 2, to_core), (1, 3, 3, to_x), (1, 5, 4, to_core), (2, 6, 5, to_core), (3, 7, 6, to_core)):
            f_copy(g, src, dst, k, device).wait_send()
        return carry

    lax.fori_loop(0, GROUPS, finish, 0)


def layer_call(lengths, q, kd, vd, k_cache, v_cache, x, gain, bias, w_out, w_up, b_up, w_down, b_out, b_down):
    vmem = pl.BlockSpec(memory_space=pltpu.VMEM)
    dma = pltpu.SemaphoreType.DMA
    return pl.pallas_call(
        layer_kernel,
        in_specs=[pl.BlockSpec(memory_space=pltpu.SMEM), ANY, ANY, ANY, ANY, ANY, ANY, vmem, vmem, ANY, ANY, vmem, ANY, vmem, vmem],
        out_specs=ANY,
        out_shape=jax.ShapeDtypeStruct((ROWS, CHUNK, D_MODEL), BF16),
        scratch_shapes=[
            pltpu.VMEM((WIDTH, D_MODEL), BF16),
            pltpu.VMEM((D_MODEL, FF), BF16),
            pltpu.VMEM((FF, D_MODEL), BF16),
            pltpu.VMEM((KV_BUFS, WIDTH, SLOTS), BF16),
            pltpu.VMEM((KV_BUFS, WIDTH, SLOTS), BF16),
            pltpu.VMEM((KV_BUFS, CHUNK, WIDTH), BF16),
            pltpu.VMEM((2, 2, 3, CHUNK, WIDTH), BF16),
            pltpu.VMEM((2, 2, CHUNK, D_MODEL), BF16),
            pltpu.VMEM((GROUPS, GROUP, CHUNK, WIDTH), F32),
            pltpu.VMEM((GROUPS, 2, CHUNK, PAIR), F32),
            pltpu.VMEM((GROUPS, 4, CHUNK, WIDTH), F32),
            pltpu.VMEM((GROUPS, CHUNK, PAIR), F32),
            pltpu.VMEM((GROUPS, CHUNK, PAIR), F32),
            pltpu.VMEM((GROUPS, 2, CHUNK, WIDTH), F32),
            pltpu.VMEM((GROUPS, CHUNK, PAIR), F32),
            pltpu.VMEM((2 * CHUNK, WIDTH), BF16),
            pltpu.VMEM((GROUPS, CHUNK, D_MODEL), F32),
            pltpu.VMEM((2, CHUNK, D_MODEL), F32),
            pltpu.VMEM((GROUPS, CHUNK, D_MODEL), F32),
            pltpu.VMEM((GROUPS, GROUP, CHUNK, D_MODEL), F32),
            pltpu.VMEM((2, GROUP, CHUNK, D_MODEL), BF16),
            dma((3,)), dma((KV_BUFS, 3)), dma((2, 8)),
            dma((GROUPS, 2)), dma((GROUPS, 2)), dma((GROUPS, 2)), dma((GROUPS, 2)),
            dma((GROUPS,)), dma((GROUPS,)), dma((GROUPS, 7)), dma((GROUPS, GROUP)), dma((2, GROUP)),
        ],
        compiler_params=pltpu.CompilerParams(collective_id=0, has_side_effects=True, vmem_limit_bytes=66_000_000),
        cost_estimate=pl.CostEstimate(flops=30 * 10 ** 9, bytes_accessed=100 << 20, transcendentals=0),
        name="layer",
    )(lengths, q, kd, vd, k_cache, v_cache, x, gain, bias, w_out, w_up, b_up, w_down, b_out, b_down)


def solution(mesh):
    in_specs = (P("dp", None, None), P("dp"), P("dp", "tp", "cp", None), P("dp", "tp", "cp", None), P(), P(), P(), P(), P(None, "tp"), P("tp"), P("tp", None), P(), P(None, "tp"), P("tp"), P("tp", None), P())
    out_specs = (P("dp", None, None), P("dp", "tp", None, None), P("dp", "tp", None, None))
    half = ROT_DIM // 2
    freq = np.broadcast_to((ROPE_BASE ** (-2.0 * np.arange(half) / ROT_DIM)).astype(np.float32)[:, None], (half, 128))

    def local_layer(hidden_in, lengths, k_block, v_block, ln1_gain, ln1_bias, ln2_gain, ln2_bias, w_qkv, b_qkv, w_out, b_out, w_up, b_up, w_down, b_down):
        row = lambda vec: vec.reshape(1, -1).astype(F32)
        b_perm = row(jnp.swapaxes(b_qkv.reshape(HEADS, 3, HEAD_DIM), 0, 1))
        q, k_new, v_new, kd, vd = qkv_call(lengths, hidden_in.reshape(ROWS * CHUNK, D_MODEL), row(ln1_gain), row(ln1_bias), w_qkv, b_perm, jnp.asarray(freq), jnp.asarray(rotate_matrix(), BF16))
        by_row = lambda values: values.reshape(ROWS, CHUNK, WIDTH)
        slot_minor = lambda cache: jnp.swapaxes(cache, 2, 3).reshape(ROWS, WIDTH, SLOTS)
        out = layer_call(lengths, by_row(q), by_row(kd), by_row(vd), slot_minor(k_block), slot_minor(v_block), hidden_in, row(ln2_gain), row(ln2_bias), w_out, w_up, row(b_up), w_down, row(b_out), row(b_down))
        return out, k_new, v_new

    return jax.shard_map(local_layer, mesh=mesh, in_specs=in_specs, out_specs=out_specs, check_vma=False)
```

```python
import functools
import numpy as np
import jax
import jax.numpy as jnp
from jax import lax
from jax.experimental import pallas as pl
from jax.experimental.pallas import tpu as pltpu
from jax.sharding import PartitionSpec as P

EPSILON = 1e-5
NEG_BIG = -1e30
MAX_FLOOR = -1e29
ROPE_BASE = 10000.0
HEAD_DIM = 64
ROT_DIM = 16
PAIR = 2 * HEAD_DIM
ROWS = 64
CHUNK = 64
HEADS = 8
WIDTH = HEADS * HEAD_DIM
SLOTS = 512
D_MODEL = 1024
FF = 2048
GROUP = 8
GROUPS = ROWS // GROUP
KV_BUFS = 3
QUAD = 4 * HEAD_DIM
HALF = GROUP // 2
TAIL_ROWS = 4
TAIL_TOKENS = TAIL_ROWS * CHUNK
F32 = jnp.float32
BF16 = jnp.bfloat16
ANY = pl.BlockSpec(memory_space=pl.ANY)


def normalize(x_f32, gain, bias):
    row_mean = jnp.mean(x_f32, axis=-1, keepdims=True)
    centered = x_f32 - row_mean
    variance = jnp.mean(centered * centered, axis=-1, keepdims=True)
    return (centered * lax.rsqrt(variance + EPSILON) * gain + bias).astype(BF16)


def rotate_matrix():
    matrix = np.zeros((PAIR, PAIR), np.float32)
    half = ROT_DIM // 2
    for base in (0, HEAD_DIM):
        for i in range(half):
            matrix[base + half + i, base + i] = -1.0
            matrix[base + i, base + half + i] = 1.0
    return matrix


def swap_halves(pair):
    return jnp.concatenate([pair[:, HEAD_DIM:], pair[:, :HEAD_DIM]], axis=1)


def pick_parts(blocks, low_half):
    first, second, third = blocks
    return jnp.where(low_half, first, second), swap_halves(jnp.where(low_half, third, first)), jnp.where(low_half, second, third)


def bias_parts(bias_row):
    low_half = lax.broadcasted_iota(jnp.int32, (1, PAIR), 1) < HEAD_DIM
    parts = [pick_parts([bias_row[:, (3 * pair + k) * PAIR:(3 * pair + k + 1) * PAIR] for k in range(3)], low_half) for pair in range(HEADS // 2)]
    return [jnp.concatenate([parts[pair][k] for pair in range(HEADS // 2)], axis=1) for k in range(3)]


def row_tables(trig, row):
    cos_len = trig[0, pl.ds(row, 1), :]
    sin_len = trig[1, pl.ds(row, 1), :]
    cos_c = trig[2]
    sin_c = trig[3]
    return cos_len * cos_c - sin_len * sin_c, sin_len * cos_c + cos_len * sin_c


def tail_kernel(a_ref, w_ref, bq_ref, trig_ref, rot_ref, through_ref, out_ref, k_out, v_out):
    step = pl.program_id(0)
    out_ref[...] = through_ref[...]
    _, k_bias, v_bias = bias_parts(bq_ref[...].astype(F32).reshape(1, 3 * WIDTH))
    k_all = (jnp.dot(a_ref[...], w_ref[:, :WIDTH], preferred_element_type=F32) + k_bias).astype(BF16)
    v_all = (jnp.dot(a_ref[...], w_ref[:, WIDTH:], preferred_element_type=F32) + v_bias).astype(BF16)
    tables = [row_tables(trig_ref, step * TAIL_ROWS + row) for row in range(TAIL_ROWS)]
    cos_tab = jnp.concatenate([table[0] for table in tables], axis=0)
    sin_tab = jnp.concatenate([table[1] for table in tables], axis=0)
    for pair in range(HEADS // 2):
        cols = slice(pair * PAIR, (pair + 1) * PAIR)
        x = k_all[:, cols]
        turned = jnp.dot(x, rot_ref[...], preferred_element_type=F32)
        k_pair = (x.astype(F32) * cos_tab + turned * sin_tab).astype(BF16)
        v_pair = v_all[:, cols]
        for row in range(TAIL_ROWS):
            tokens = slice(row * CHUNK, (row + 1) * CHUNK)
            for sub in range(2):
                dims = slice(sub * HEAD_DIM, (sub + 1) * HEAD_DIM)
                k_out[row, 2 * pair + sub] = k_pair[tokens, dims]
                v_out[row, 2 * pair + sub] = v_pair[tokens, dims]


def tail_call(a_flat, w_kv, b_qkv, trig, rot, through):
    tokens = ROWS * CHUNK
    whole = lambda shape: pl.BlockSpec(shape, lambda i: (0,) * len(shape))
    dense = pl.BlockSpec((TAIL_TOKENS, D_MODEL), lambda i: (i, 0))
    heads = pl.BlockSpec((TAIL_ROWS, HEADS, CHUNK, HEAD_DIM), lambda i: (i, 0, 0, 0))
    return pl.pallas_call(
        tail_kernel,
        grid=(ROWS // TAIL_ROWS,),
        in_specs=[dense, whole((D_MODEL, 2 * WIDTH)), whole((3 * WIDTH,)), whole((4, CHUNK, PAIR)), whole((PAIR, PAIR)), dense],
        out_specs=[dense, heads, heads],
        out_shape=[
            jax.ShapeDtypeStruct((tokens, D_MODEL), BF16),
            jax.ShapeDtypeStruct((ROWS, HEADS, CHUNK, HEAD_DIM), BF16),
            jax.ShapeDtypeStruct((ROWS, HEADS, CHUNK, HEAD_DIM), BF16),
        ],
        cost_estimate=pl.CostEstimate(flops=2 * tokens * D_MODEL * 2 * WIDTH, bytes_accessed=42 << 20, transcendentals=0),
        name="tail",
    )(a_flat, w_kv, b_qkv, trig, rot, through)


def layer_kernel(len_ref, kc_hbm, vc_hbm, x_hbm, gain1_ref, bias1_ref, gain2_ref, bias2_ref, wqkv_hbm, bq_ref, rot_ref, wo_hbm, wu_hbm, bu_ref, wd_hbm, bo_ref, bd_ref,
                 out_hbm, a_hbm, wkv_hbm, trig_hbm,
                 wo, wu, wd, wq, wkv, bias_q, bias_kv, trig, kbuf, vbuf, x_buf, a_buf, q_buf, kv_self, own_o, own_stat, mlp_acc,
                 o_buf, stat, c_recv, c_stat, cx_stat, x_recv, x_stat, ctx, y_send, y_keep, y_recv, fin, stage,
                 w_sem, kv_sem, xin_sem, a_sem, side_sem, c_ssem, c_rsem, x_ssem, x_rsem, y_ssem, y_rsem, f_ssem, f_rsem, out_sem):
    tp_id = lax.axis_index("tp")
    cp_id = lax.axis_index("cp")
    chip_x = cp_id // 2
    core = cp_id % 2
    to_core = {"cp": 2 * chip_x + 1 - core}
    to_x = {"cp": 2 * (1 - chip_x) + core}
    to_y = {"tp": 1 - tp_id}

    def flip(bit, mine):
        return bit + mine - 2 * bit * mine

    def row_of(group, slot):
        return group * GROUP + 4 * flip(slot // 4, core) + 2 * flip((slot // 2) % 2, chip_x) + flip(slot % 2, tp_id)

    def remote(src, dst, ssem, rsem, device):
        return pltpu.make_async_remote_copy(src_ref=src, dst_ref=dst, send_sem=ssem, recv_sem=rsem, device_id=device, device_id_type=pl.DeviceIdType.MESH)

    def kv_copies(n):
        b = n % KV_BUFS
        row = row_of(n // GROUP, (n % GROUP + 4) % GROUP)
        return (pltpu.make_async_copy(kc_hbm.at[row], kbuf.at[b], kv_sem.at[b, 0]), pltpu.make_async_copy(vc_hbm.at[row], vbuf.at[b], kv_sem.at[b, 1]))

    def x_in(g):
        return [pltpu.make_async_copy(x_hbm.at[row_of(g, slot)], x_buf.at[g % 2, slot], xin_sem.at[g % 2, slot]) for slot in range(GROUP)]

    def a_copies(g, half):
        first = 4 - 4 * half
        return [pltpu.make_async_copy(a_buf.at[half, pl.ds(k * CHUNK, CHUNK)], a_hbm.at[row_of(g, first + k)], a_sem.at[half, k]) for k in range(HALF)]

    wqkv_copy = pltpu.make_async_copy(wqkv_hbm, wu.at[:, pl.ds(0, 3 * WIDTH)], w_sem.at[0])
    w_copies = [pltpu.make_async_copy(wu_hbm, wu, w_sem.at[1]), pltpu.make_async_copy(wd_hbm, wd, w_sem.at[2])]
    for head in range(HEADS):
        w_copies.append(pltpu.make_async_copy(wo_hbm.at[pl.ds(head * HEAD_DIM, HEAD_DIM)], wo.at[pl.ds((head % 2) * QUAD + (head // 2) * HEAD_DIM, HEAD_DIM)], w_sem.at[3 + head]))
    side_copies = (pltpu.make_async_copy(wkv, wkv_hbm, side_sem.at[0]), pltpu.make_async_copy(trig, trig_hbm, side_sem.at[1]))

    def c_copies(g):
        return (remote(o_buf.at[g, pl.ds(4, 4)], c_recv.at[g], c_ssem.at[g, 0], c_rsem.at[g, 0], to_core), remote(stat.at[g, 0], c_stat.at[g], c_ssem.at[g, 1], c_rsem.at[g, 1], to_core))

    def x_copies(g):
        return (remote(o_buf.at[g, pl.ds(2, 2)], x_recv.at[g], x_ssem.at[g, 0], x_rsem.at[g, 0], to_x), remote(cx_stat.at[g, pl.ds(2, 2)], x_stat.at[g], x_ssem.at[g, 1], x_rsem.at[g, 1], to_x))

    def y_copy(g):
        return remote(y_send.at[g], y_recv.at[g], y_ssem.at[g], y_rsem.at[g], to_y)

    def f_copy(g, src, dst, k, device):
        return remote(fin.at[g, src], fin.at[g, dst], f_ssem.at[g, k], f_rsem.at[g, dst], device)

    def out_copy(g, slot):
        return pltpu.make_async_copy(stage.at[g % 2, slot], out_hbm.at[row_of(g, slot)], out_sem.at[g % 2, slot])

    lane = lax.broadcasted_iota(jnp.int32, (CHUNK, PAIR), 1)
    low_half = lane < HEAD_DIM
    is_max = lax.broadcasted_iota(jnp.int32, (8, PAIR), 0) < HEADS // 2
    quad_lane = lax.broadcasted_iota(jnp.int32, (CHUNK, QUAD), 1)

    def block_diagonal(q_quad):
        zero = jnp.zeros_like(q_quad)
        return jnp.concatenate([jnp.where(quad_lane // HEAD_DIM == k, q_quad, zero) for k in range(4)], axis=0)

    def rotate(values, turned, tables, scale):
        return ((values.astype(F32) * tables[0] + turned * tables[1]) * scale).astype(BF16)

    def project(g, half):
        first = 4 - 4 * half

        @pl.when(g >= 1)
        def _():
            for copy in a_copies(g - 1, half):
                copy.wait()

        x = x_buf[g % 2, first:first + HALF].reshape(HALF * CHUNK, D_MODEL).astype(F32)
        normed = normalize(x, gain1_ref[...].reshape(1, D_MODEL), bias1_ref[...].reshape(1, D_MODEL))
        a_buf[half] = normed
        for copy in a_copies(g, half):
            copy.start()
        q_all = (jnp.dot(normed, wq[...], preferred_element_type=F32) + bias_q[...]).astype(BF16)
        tables = [row_tables(trig, row_of(g, first + k)) for k in range(HALF)]
        for pair in range(HEADS // 2):
            cols = slice(pair * PAIR, (pair + 1) * PAIR)
            turned = jnp.dot(q_all[:, cols], rot_ref[...], preferred_element_type=F32)
            for k in range(HALF):
                tokens = slice(k * CHUNK, (k + 1) * CHUNK)
                q_buf[first + k, :, cols] = rotate(q_all[tokens, cols], turned[tokens], tables[k], HEAD_DIM ** -0.5)

    def attend(g, half, j):
        n = g * GROUP + half * HALF + j
        slot = 4 - 4 * half + j
        b = n % KV_BUFS
        for copy in kv_copies(n):
            copy.wait()

        @pl.when(n + KV_BUFS - 1 < ROWS)
        def _():
            for copy in kv_copies(n + KV_BUFS - 1):
                copy.start()

        row_len = len_ref[row_of(g, slot)]
        valid = cp_id * SLOTS + lax.broadcasted_iota(jnp.int32, (SLOTS, QUAD), 0) < row_len
        for quad in range(2):
            dims = slice(quad * QUAD, (quad + 1) * QUAD)
            q4 = block_diagonal(q_buf[slot, :, dims])
            scores = lax.dot_general(kbuf[b, dims, :], q4, (((0,), (1,)), ((), ())), preferred_element_type=F32)
            scores = jnp.where(valid, scores, NEG_BIG)
            top = jnp.maximum(jnp.max(scores, axis=0, keepdims=True), MAX_FLOOR)
            probs = jnp.exp(scores - top)
            total = jnp.sum(probs, axis=0, keepdims=True)
            packed = probs.astype(BF16)
            for sub in range(2):
                pair = 2 * quad + sub
                cols = slice(sub * PAIR, (sub + 1) * PAIR)
                both = jnp.dot(vbuf[b, pair * PAIR:(pair + 1) * PAIR, :], packed[:, cols], preferred_element_type=F32)
                o_buf[g, slot, pair * HEAD_DIM:(pair + 1) * HEAD_DIM, :] = jnp.where(low_half, both[:HEAD_DIM], both[HEAD_DIM:])
                stat[g, half, j, pair:pair + 1, :] = top[:, cols]
                stat[g, half, j, 4 + pair:5 + pair, :] = total[:, cols]

    def core_stage(g):
        for copy in c_copies(g):
            copy.wait_recv()
        for slot in (2, 3, 0, 1):
            mine = stat[g, 1, slot]
            theirs = c_stat[g, slot]
            top = jnp.maximum(mine, theirs)
            w_mine = jnp.exp(mine - top)
            w_theirs = jnp.exp(theirs - top)
            total = mine * pltpu.roll(w_mine, 4, 0) + theirs * pltpu.roll(w_theirs, 4, 0)
            cx_stat[g, slot] = jnp.where(is_max, top, total)
            for pair in range(HEADS // 2):
                dims = slice(pair * HEAD_DIM, (pair + 1) * HEAD_DIM)
                o_buf[g, slot, dims, :] = o_buf[g, slot, dims, :] * w_mine[pair:pair + 1] + c_recv[g, slot, dims, :] * w_theirs[pair:pair + 1]
            if slot == 3:
                for copy in x_copies(g):
                    copy.start()

    def prepare(g):
        kv = (jnp.dot(a_buf[1, :2 * CHUNK], wkv[...], preferred_element_type=F32) + bias_kv[...]).astype(BF16)
        tables = [row_tables(trig, row_of(g, slot)) for slot in range(2)]
        for pair in range(HEADS // 2):
            cols = slice(pair * PAIR, (pair + 1) * PAIR)
            turned = jnp.dot(kv[:, cols], rot_ref[...], preferred_element_type=F32)
            for slot in range(2):
                tokens = slice(slot * CHUNK, (slot + 1) * CHUNK)
                kv_self[slot, :, cols] = rotate(kv[tokens, cols], turned[tokens], tables[slot], 1.0)
        for slot in range(2):
            kv_self[slot, :, WIDTH:] = kv[slot * CHUNK:(slot + 1) * CHUNK, WIDTH:]
        causal = lax.broadcasted_iota(jnp.int32, (CHUNK, QUAD), 0) <= quad_lane % CHUNK
        for slot in range(2):
            for quad in range(2):
                dims = slice(quad * QUAD, (quad + 1) * QUAD)
                q4 = block_diagonal(q_buf[slot, :, dims])
                scores = lax.dot_general(kv_self[slot, :, dims], q4, (((1,), (1,)), ((), ())), preferred_element_type=F32)
                scores = jnp.where(causal, scores, NEG_BIG)
                top = jnp.max(scores, axis=0, keepdims=True)
                probs = jnp.where(causal, jnp.exp(scores - top), 0.0)
                total = jnp.sum(probs, axis=0, keepdims=True)
                packed = probs.astype(BF16)
                for sub in range(2):
                    pair = 2 * quad + sub
                    cols = slice(sub * PAIR, (sub + 1) * PAIR)
                    both = lax.dot_general(kv_self[slot, :, WIDTH + pair * PAIR:WIDTH + (pair + 1) * PAIR], packed[:, cols], (((0,), (0,)), ((), ())), preferred_element_type=F32)
                    own_o[slot, pair * HEAD_DIM:(pair + 1) * HEAD_DIM, :] = jnp.where(low_half, both[:HEAD_DIM], both[HEAD_DIM:])
                    own_stat[slot, pair:pair + 1, :] = top[:, cols]
                    own_stat[slot, 4 + pair:5 + pair, :] = total[:, cols]
        x_both = x_buf[g % 2, :2].reshape(2 * CHUNK, D_MODEL).astype(F32)
        normed = normalize(x_both, gain2_ref[...].reshape(1, D_MODEL), bias2_ref[...].reshape(1, D_MODEL))
        up = jnp.dot(normed, wu[...], preferred_element_type=F32) + bu_ref[...].astype(F32).reshape(1, FF)
        hidden = (0.5 * up * (1.0 + lax.erf(up * (0.5 ** 0.5)))).astype(BF16)
        mlp_acc[...] = jnp.dot(hidden, wd[...], preferred_element_type=F32)
        y_keep[g % 2] = x_both[:CHUNK] + bo_ref[...].astype(F32).reshape(1, D_MODEL) + bd_ref[...].astype(F32).reshape(1, D_MODEL)

    def x_stage(g):
        for copy in x_copies(g):
            copy.wait_recv()
        for slot in range(2):
            mine = cx_stat[g, slot]
            theirs = x_stat[g, slot]
            own = own_stat[slot]
            top = jnp.maximum(jnp.maximum(mine, theirs), own)
            w_mine = jnp.exp(mine - top)
            w_theirs = jnp.exp(theirs - top)
            w_own = jnp.exp(own - top)
            total = mine * pltpu.roll(w_mine, 4, 0) + theirs * pltpu.roll(w_theirs, 4, 0) + own * pltpu.roll(w_own, 4, 0)
            inverse = pltpu.roll(1.0 / jnp.where(is_max, 1.0, total), 4, 0)
            w_mine = w_mine * inverse
            w_theirs = w_theirs * inverse
            w_own = w_own * inverse
            values = []
            for pair in range(HEADS // 2):
                dims = slice(pair * HEAD_DIM, (pair + 1) * HEAD_DIM)
                one = slice(pair, pair + 1)
                values.append(o_buf[g, slot, dims, :] * w_mine[one] + x_recv[g, slot, dims, :] * w_theirs[one] + own_o[slot, dims, :] * w_own[one])
            turned = jnp.concatenate(values, axis=0).T
            for half in range(2):
                ctx[slot * CHUNK:(slot + 1) * CHUNK, half * QUAD:(half + 1) * QUAD] = turned[half * CHUNK:(half + 1) * CHUNK].astype(BF16)
        branch = jnp.dot(ctx[...], wo[...], preferred_element_type=F32) + mlp_acc[...]
        y_send[g] = branch[CHUNK:]
        y_copy(g).start()
        y_keep[g % 2] = y_keep[g % 2] + branch[:CHUNK]

    def y_stage(g):
        y_copy(g).wait_recv()
        fin[g, 0] = y_keep[g % 2] + y_recv[g]
        f_copy(g, 0, 2, 0, to_x).start()
        f_copy(g, 0, 1, 1, to_y).start()
        f_copy(g, 0, 4, 2, to_core).start()

    def forward_stage(g):
        f_copy(g, 0, 1, 1, to_y).wait_recv()
        f_copy(g, 0, 2, 0, to_x).wait_recv()

        @pl.when(g % 2 == 0)
        def _():
            f_copy(g, 1, 3, 3, to_x).start()

        @pl.when(g % 2 == 1)
        def _():
            f_copy(g, 2, 3, 3, to_y).start()

        f_copy(g, 1, 5, 4, to_core).start()
        f_copy(g, 2, 6, 5, to_core).start()

    def diagonal_stage(g):
        f_copy(g, 1, 3, 3, to_x).wait_recv()
        f_copy(g, 3, 7, 6, to_core).start()

    def out_stage(g):
        f_copy(g, 0, 4, 2, to_core).wait_recv()
        f_copy(g, 1, 5, 4, to_core).wait_recv()
        f_copy(g, 2, 6, 5, to_core).wait_recv()
        f_copy(g, 3, 7, 6, to_core).wait_recv()

        @pl.when(g >= 2)
        def _():
            for slot in range(GROUP):
                out_copy(g - 2, slot).wait()

        for slot in range(GROUP):
            stage[g % 2, slot] = fin[g, slot].astype(BF16)
            out_copy(g, slot).start()

    def when_group(g, work):
        @pl.when(jnp.logical_and(g >= 0, g < GROUPS))
        def _():
            work(g)

    wqkv_copy.start()
    for copy in x_in(0):
        copy.start()
    for n in range(KV_BUFS - 1):
        for copy in kv_copies(n):
            copy.start()
    barrier = pltpu.get_barrier_semaphore()
    for device in (to_core, to_x, to_y):
        pl.semaphore_signal(barrier, inc=1, device_id=device, device_id_type=pl.DeviceIdType.MESH)

    dim = lane % HEAD_DIM
    freq = jnp.zeros((CHUNK, PAIR), F32)
    for k in range(ROT_DIM // 2):
        here = jnp.logical_and(dim % (ROT_DIM // 2) == k, dim < ROT_DIM)
        freq = jnp.where(here, float(np.float32(ROPE_BASE ** (-2.0 * k / ROT_DIM))), freq)

    def one_angle(r, carry):
        trig[0, pl.ds(r, 1), :] = len_ref[r].astype(F32) * freq[:1]
        return carry

    lax.fori_loop(0, ROWS, one_angle, 0)
    angles = trig[0]
    trig[1] = jnp.sin(angles)
    trig[0] = jnp.cos(angles)
    angles = lax.broadcasted_iota(jnp.int32, (CHUNK, PAIR), 0).astype(F32) * freq
    trig[2] = jnp.cos(angles)
    trig[3] = jnp.sin(angles)
    q_bias, k_bias, v_bias = bias_parts(bq_ref[...].astype(F32).reshape(1, 3 * WIDTH))
    bias_q[...] = q_bias
    bias_kv[:, :WIDTH] = k_bias
    bias_kv[:, WIDTH:] = v_bias
    wqkv_copy.wait()

    def arrange(r, carry):
        rows = pl.ds(pl.multiple_of(r * PAIR, PAIR), PAIR)
        low = lax.broadcasted_iota(jnp.int32, (PAIR, PAIR), 1) < HEAD_DIM
        for pair in range(HEADS // 2):
            q_part, k_part, v_part = pick_parts([wu[rows, (3 * pair + k) * PAIR:(3 * pair + k + 1) * PAIR] for k in range(3)], low)
            wq[rows, pair * PAIR:(pair + 1) * PAIR] = q_part
            wkv[rows, pair * PAIR:(pair + 1) * PAIR] = k_part
            wkv[rows, WIDTH + pair * PAIR:WIDTH + (pair + 1) * PAIR] = v_part
        return carry

    lax.fori_loop(0, D_MODEL // PAIR, arrange, 0)
    for copy in w_copies:
        copy.start()
    for copy in side_copies:
        copy.start()
    pl.semaphore_wait(barrier, 3)

    def iteration(i, carry):
        @pl.when(i + 1 < GROUPS)
        def _():
            for copy in x_in(i + 1):
                copy.start()

        for half in range(2):
            @pl.when(i < GROUPS)
            def _(half=half):
                if half == 0:
                    for copy in x_in(i):
                        copy.wait()
                project(i, half)
                lax.fori_loop(0, HALF, lambda j, inner: (attend(i, half, j), inner)[1], 0)
                if half == 0:
                    for copy in c_copies(i):
                        copy.start()
                else:
                    core_stage(i)

            if half == 0:
                when_group(i - 1, x_stage)
                when_group(i - 2, forward_stage)

        @pl.when(i == 0)
        def _():
            for copy in w_copies:
                copy.wait()

        when_group(i, prepare)
        when_group(i - 1, y_stage)
        when_group(i - 2, diagonal_stage)
        when_group(i - 3, out_stage)
        return carry

    lax.fori_loop(0, GROUPS + 3, iteration, 0)
    for copy in side_copies:
        copy.wait()
    for half in range(2):
        for copy in a_copies(GROUPS - 1, half):
            copy.wait()
    for g in (GROUPS - 2, GROUPS - 1):
        for slot in range(GROUP):
            out_copy(g, slot).wait()

    def finish(g, carry):
        for copy in c_copies(g) + x_copies(g) + (y_copy(g),):
            copy.wait_send()
        for src, dst, k, device in ((0, 2, 0, to_x), (0, 1, 1, to_y), (0, 4, 2, to_core), (1, 3, 3, to_x), (1, 5, 4, to_core), (2, 6, 5, to_core), (3, 7, 6, to_core)):
            f_copy(g, src, dst, k, device).wait_send()
        return carry

    lax.fori_loop(0, GROUPS, finish, 0)


def layer_call(lengths, k_cache, v_cache, x, gain1, bias1, gain2, bias2, w_qkv, b_qkv, rot, w_out, w_up, b_up, w_down, b_out, b_down):
    vmem = pl.BlockSpec(memory_space=pltpu.VMEM)
    dma = pltpu.SemaphoreType.DMA
    return pl.pallas_call(
        layer_kernel,
        in_specs=[pl.BlockSpec(memory_space=pltpu.SMEM), ANY, ANY, ANY, vmem, vmem, vmem, vmem, ANY, vmem, vmem, ANY, ANY, vmem, ANY, vmem, vmem],
        out_specs=[ANY, ANY, ANY, ANY],
        out_shape=[
            jax.ShapeDtypeStruct((ROWS, CHUNK, D_MODEL), BF16),
            jax.ShapeDtypeStruct((ROWS, CHUNK, D_MODEL), BF16),
            jax.ShapeDtypeStruct((D_MODEL, 2 * WIDTH), BF16),
            jax.ShapeDtypeStruct((4, CHUNK, PAIR), F32),
        ],
        scratch_shapes=[
            pltpu.VMEM((WIDTH, D_MODEL), BF16),
            pltpu.VMEM((D_MODEL, FF), BF16),
            pltpu.VMEM((FF, D_MODEL), BF16),
            pltpu.VMEM((D_MODEL, WIDTH), BF16),
            pltpu.VMEM((D_MODEL, 2 * WIDTH), BF16),
            pltpu.VMEM((1, WIDTH), F32),
            pltpu.VMEM((1, 2 * WIDTH), F32),
            pltpu.VMEM((4, CHUNK, PAIR), F32),
            pltpu.VMEM((KV_BUFS, WIDTH, SLOTS), BF16),
            pltpu.VMEM((KV_BUFS, WIDTH, SLOTS), BF16),
            pltpu.VMEM((2, GROUP, CHUNK, D_MODEL), BF16),
            pltpu.VMEM((2, HALF * CHUNK, D_MODEL), BF16),
            pltpu.VMEM((GROUP, CHUNK, WIDTH), BF16),
            pltpu.VMEM((2, CHUNK, 2 * WIDTH), BF16),
            pltpu.VMEM((2, QUAD, PAIR), F32),
            pltpu.VMEM((2, 8, PAIR), F32),
            pltpu.VMEM((2 * CHUNK, D_MODEL), F32),
            pltpu.VMEM((GROUPS, GROUP, QUAD, PAIR), F32),
            pltpu.VMEM((GROUPS, 2, HALF, 8, PAIR), F32),
            pltpu.VMEM((GROUPS, HALF, QUAD, PAIR), F32),
            pltpu.VMEM((GROUPS, HALF, 8, PAIR), F32),
            pltpu.VMEM((GROUPS, HALF, 8, PAIR), F32),
            pltpu.VMEM((GROUPS, 2, QUAD, PAIR), F32),
            pltpu.VMEM((GROUPS, 2, 8, PAIR), F32),
            pltpu.VMEM((2 * CHUNK, WIDTH), BF16),
            pltpu.VMEM((GROUPS, CHUNK, D_MODEL), F32),
            pltpu.VMEM((2, CHUNK, D_MODEL), F32),
            pltpu.VMEM((GROUPS, CHUNK, D_MODEL), F32),
            pltpu.VMEM((GROUPS, GROUP, CHUNK, D_MODEL), F32),
            pltpu.VMEM((2, GROUP, CHUNK, D_MODEL), BF16),
            dma((3 + HEADS,)), dma((KV_BUFS, 2)), dma((2, GROUP)), dma((2, HALF)), dma((2,)),
            dma((GROUPS, 2)), dma((GROUPS, 2)), dma((GROUPS, 2)), dma((GROUPS, 2)),
            dma((GROUPS,)), dma((GROUPS,)), dma((GROUPS, 7)), dma((GROUPS, GROUP)), dma((2, GROUP)),
        ],
        compiler_params=pltpu.CompilerParams(collective_id=0, has_side_effects=True, vmem_limit_bytes=67_000_000),
        cost_estimate=pl.CostEstimate(flops=30 * 10 ** 9, bytes_accessed=100 << 20, transcendentals=0),
        name="layer",
    )(lengths, k_cache, v_cache, x, gain1, bias1, gain2, bias2, w_qkv, b_qkv, rot, w_out, w_up, b_up, w_down, b_out, b_down)


def solution(mesh):
    in_specs = (P("dp", None, None), P("dp"), P("dp", "tp", "cp", None), P("dp", "tp", "cp", None), P(), P(), P(), P(), P(None, "tp"), P("tp"), P("tp", None), P(), P(None, "tp"), P("tp"), P("tp", None), P())
    out_specs = (P("dp", None, None), P("dp", "tp", None, None), P("dp", "tp", None, None))

    def local_layer(hidden_in, lengths, k_block, v_block, ln1_gain, ln1_bias, ln2_gain, ln2_bias, w_qkv, b_qkv, w_out, b_out, w_up, b_up, w_down, b_down):
        slot_minor = lambda cache: jnp.swapaxes(cache, 2, 3).reshape(ROWS, WIDTH, SLOTS)
        rot = jnp.asarray(rotate_matrix(), BF16)
        through, normed, w_kv, trig = layer_call(lengths, slot_minor(k_block), slot_minor(v_block), hidden_in, ln1_gain, ln1_bias, ln2_gain, ln2_bias, w_qkv, b_qkv, rot, w_out, w_up, b_up, w_down, b_out, b_down)
        flat = lambda values: values.reshape(ROWS * CHUNK, D_MODEL)
        out, k_new, v_new = tail_call(flat(normed), w_kv, b_qkv, trig, rot, flat(through))
        return out.reshape(ROWS, CHUNK, D_MODEL), k_new, v_new

    return jax.shard_map(local_layer, mesh=mesh, in_specs=in_specs, out_specs=out_specs, check_vma=False)
```

```python
import functools
import numpy as np
import jax
import jax.numpy as jnp
from jax import lax
from jax.experimental import pallas as pl
from jax.experimental.pallas import tpu as pltpu
from jax.sharding import PartitionSpec as P

EPSILON = 1e-5
NEG_BIG = -1e30
MAX_FLOOR = -1e29
ROPE_BASE = 10000.0
HEAD_DIM = 64
ROT_DIM = 16
PAIR = 2 * HEAD_DIM
ROWS = 64
CHUNK = 64
HEADS = 8
WIDTH = HEADS * HEAD_DIM
SLOTS = 512
D_MODEL = 1024
FF = 2048
GROUP = 8
GROUPS = ROWS // GROUP
K_BUFS = 3
V_BUFS = 5
AHEAD = 2
STRIP = 64
FORWARD_LAG = 5
DIAGONAL_LAG = 8
QUAD = 4 * HEAD_DIM
HALF = GROUP // 2
TAIL_ROWS = 16
TAIL_TOKENS = TAIL_ROWS * CHUNK
TAIL_SLOTS = 2
PASS_STEPS = 2
F32 = jnp.float32
BF16 = jnp.bfloat16
ANY = pl.BlockSpec(memory_space=pl.ANY)


def normalize(x_f32, gain, bias):
    row_mean = jnp.mean(x_f32, axis=-1, keepdims=True)
    centered = x_f32 - row_mean
    variance = jnp.mean(centered * centered, axis=-1, keepdims=True)
    return (centered * lax.rsqrt(variance + EPSILON) * gain + bias).astype(BF16)


def rotate_matrix():
    matrix = np.zeros((PAIR, PAIR), np.float32)
    half = ROT_DIM // 2
    for base in (0, HEAD_DIM):
        for i in range(half):
            matrix[base + half + i, base + i] = -1.0
            matrix[base + i, base + half + i] = 1.0
    return matrix


def swap_halves(pair):
    return jnp.concatenate([pair[:, HEAD_DIM:], pair[:, :HEAD_DIM]], axis=1)


def pick_parts(blocks, low_half):
    first, second, third = blocks
    return jnp.where(low_half, first, second), swap_halves(jnp.where(low_half, third, first)), jnp.where(low_half, second, third)


def bias_parts(bias_row):
    low_half = lax.broadcasted_iota(jnp.int32, (1, PAIR), 1) < HEAD_DIM
    parts = [pick_parts([bias_row[:, (3 * pair + k) * PAIR:(3 * pair + k + 1) * PAIR] for k in range(3)], low_half) for pair in range(HEADS // 2)]
    return [jnp.concatenate([parts[pair][k] for pair in range(HEADS // 2)], axis=1) for k in range(3)]


def row_tables(trig, row):
    cos_len = trig[0, pl.ds(row, 1), :]
    sin_len = trig[1, pl.ds(row, 1), :]
    cos_c = trig[2]
    sin_c = trig[3]
    return cos_len * cos_c - sin_len * sin_c, sin_len * cos_c + cos_len * sin_c


def tail_kernel(a_hbm, w_hbm, bq_ref, trig_ref, rot_ref, through_hbm, out_hbm, k_hbm, v_hbm, w_ref, a_all, passing, raw, bias, k_stage, v_stage, w_sem, a_sem, in_sem, out_sem, k_sem, v_sem):
    blocks = ROWS // TAIL_ROWS

    def tokens(i):
        return pl.ds(i * TAIL_TOKENS, TAIL_TOKENS)

    def rows(i):
        return pl.ds(i * TAIL_ROWS, TAIL_ROWS)

    w_copy = pltpu.make_async_copy(w_hbm, w_ref, w_sem)
    a_in = lambda i: pltpu.make_async_copy(a_hbm.at[tokens(i)], a_all.at[i], a_sem.at[i])
    pass_in = lambda i: pltpu.make_async_copy(through_hbm.at[tokens(i)], passing.at[i], in_sem.at[i])
    pass_out = lambda i: pltpu.make_async_copy(passing.at[i], out_hbm.at[tokens(i)], out_sem.at[i])
    k_put = lambda i: pltpu.make_async_copy(k_stage.at[i % TAIL_SLOTS], k_hbm.at[rows(i)], k_sem.at[i % TAIL_SLOTS])
    v_put = lambda i: pltpu.make_async_copy(v_stage.at[i % TAIL_SLOTS], v_hbm.at[rows(i)], v_sem.at[i % TAIL_SLOTS])

    w_copy.start()
    for i in range(blocks):
        a_in(i).start()
        if i >= 2:
            pass_in(i - 2).start()
    for i in range(blocks - 2, blocks):
        pass_in(i).start()
    _, k_bias, v_bias = bias_parts(bq_ref[...].astype(F32).reshape(1, 3 * WIDTH))
    bias[:, :WIDTH] = k_bias
    bias[:, WIDTH:] = v_bias
    w_copy.wait()

    def multiply(i):
        raw[...] = (jnp.dot(a_all[i], w_ref[...], preferred_element_type=F32) + bias[...]).astype(BF16)

    def place(i):
        slot = i % TAIL_SLOTS
        for row in range(TAIL_ROWS):
            tables = row_tables(trig_ref, i * TAIL_ROWS + row)
            here = slice(row * CHUNK, (row + 1) * CHUNK)
            for pair in range(HEADS // 2):
                x = raw[here, pair * PAIR:(pair + 1) * PAIR]
                turned = jnp.dot(x, rot_ref[...], preferred_element_type=F32)
                k_pair = (x.astype(F32) * tables[0] + turned * tables[1]).astype(BF16)
                v_pair = raw[here, WIDTH + pair * PAIR:WIDTH + (pair + 1) * PAIR]
                for sub in range(2):
                    dims = slice(sub * HEAD_DIM, (sub + 1) * HEAD_DIM)
                    k_stage[slot, row, 2 * pair + sub] = k_pair[:, dims]
                    v_stage[slot, row, 2 * pair + sub] = v_pair[:, dims]

    def step(i, carry):
        @pl.when(i < blocks)
        def _():
            a_in(i).wait()

        @pl.when(i >= 1 + TAIL_SLOTS)
        def _():
            k_put(i - 1 - TAIL_SLOTS).wait()
            v_put(i - 1 - TAIL_SLOTS).wait()

        place(jnp.maximum(i - 1, 0))
        multiply(jnp.minimum(i, blocks - 1))

        @pl.when(i >= 1)
        def _():
            k_put(i - 1).start()
            v_put(i - 1).start()

        for early in range(PASS_STEPS):
            @pl.when(i == early + 1)
            def _(early=early):
                for block in range(early * blocks // PASS_STEPS, (early + 1) * blocks // PASS_STEPS):
                    pass_in(block).wait()
                    pass_out(block).start()

        return carry

    lax.fori_loop(0, blocks + 1, step, 0)
    for i in range(blocks - TAIL_SLOTS, blocks):
        k_put(i).wait()
        v_put(i).wait()
    for i in range(blocks):
        pass_out(i).wait()


def tail_call(a_flat, w_kv, b_qkv, trig, rot, through):
    tokens = ROWS * CHUNK
    blocks = ROWS // TAIL_ROWS
    vmem = pl.BlockSpec(memory_space=pltpu.VMEM)
    dma = pltpu.SemaphoreType.DMA
    return pl.pallas_call(
        tail_kernel,
        in_specs=[ANY, ANY, vmem, vmem, vmem, ANY],
        out_specs=[ANY, ANY, ANY],
        out_shape=[
            jax.ShapeDtypeStruct((tokens, D_MODEL), BF16),
            jax.ShapeDtypeStruct((ROWS, HEADS, CHUNK, HEAD_DIM), BF16),
            jax.ShapeDtypeStruct((ROWS, HEADS, CHUNK, HEAD_DIM), BF16),
        ],
        scratch_shapes=[
            pltpu.VMEM((D_MODEL, 2 * WIDTH), BF16),
            pltpu.VMEM((blocks, TAIL_TOKENS, D_MODEL), BF16),
            pltpu.VMEM((blocks, TAIL_TOKENS, D_MODEL), BF16),
            pltpu.VMEM((TAIL_TOKENS, 2 * WIDTH), BF16),
            pltpu.VMEM((1, 2 * WIDTH), F32),
            pltpu.VMEM((TAIL_SLOTS, TAIL_ROWS, HEADS, CHUNK, HEAD_DIM), BF16),
            pltpu.VMEM((TAIL_SLOTS, TAIL_ROWS, HEADS, CHUNK, HEAD_DIM), BF16),
            dma(()), dma((blocks,)), dma((blocks,)), dma((blocks,)), dma((TAIL_SLOTS,)), dma((TAIL_SLOTS,)),
        ],
        cost_estimate=pl.CostEstimate(flops=2 * tokens * D_MODEL * 2 * WIDTH, bytes_accessed=42 << 20, transcendentals=0),
        compiler_params=pltpu.CompilerParams(vmem_limit_bytes=60_000_000),
        name="tail",
    )(a_flat, w_kv, b_qkv, trig, rot, through)


def layer_kernel(len_ref, kc_hbm, vc_hbm, x_hbm, gain1_ref, bias1_ref, gain2_ref, bias2_ref, wqkv_hbm, bq_ref, rot_ref, wo_hbm, wu_hbm, bu_ref, wd_hbm, bo_ref, bd_ref,
                 out_hbm, a_hbm, wkv_hbm, trig_hbm,
                 wo, wu, wd, wq, wkv, bias_q, bias_kv, trig, kbuf, vbuf, s0, s1, p0, p1, x_buf, a_buf, q_buf, kv_self, own_o, own_stat, mlp_acc,
                 o_buf, stat, c_recv, c_stat, cx_stat, x_recv, x_stat, ctx, y_send, y_keep, y_recv, fin, stage,
                 w_sem, k_sem, v_sem, xin_sem, a_sem, side_sem, c_ssem, c_rsem, x_ssem, x_rsem, y_ssem, y_rsem, f_ssem, f_rsem, out_sem):
    tp_id = lax.axis_index("tp")
    cp_id = lax.axis_index("cp")
    chip_x = cp_id // 2
    core = cp_id % 2
    to_core = {"cp": 2 * chip_x + 1 - core}
    to_x = {"cp": 2 * (1 - chip_x) + core}
    to_y = {"tp": 1 - tp_id}

    def flip(bit, mine):
        return bit + mine - 2 * bit * mine

    def row_of(group, slot):
        return group * GROUP + 4 * flip(slot // 4, core) + 2 * flip((slot // 2) % 2, chip_x) + flip(slot % 2, tp_id)

    def remote(src, dst, ssem, rsem, device):
        return pltpu.make_async_remote_copy(src_ref=src, dst_ref=dst, send_sem=ssem, recv_sem=rsem, device_id=device, device_id_type=pl.DeviceIdType.MESH)

    def kv_copies(n):
        kb = n % K_BUFS
        vb = n % V_BUFS
        row = row_of(n // GROUP, (n % GROUP + 4) % GROUP)
        return (pltpu.make_async_copy(kc_hbm.at[row], kbuf.at[kb], k_sem.at[kb]), pltpu.make_async_copy(vc_hbm.at[row], vbuf.at[vb], v_sem.at[vb]))

    def x_in(g):
        return [pltpu.make_async_copy(x_hbm.at[row_of(g, slot)], x_buf.at[g % 2, slot], xin_sem.at[g % 2, slot]) for slot in range(GROUP)]

    def a_copies(g, half):
        first = 4 - 4 * half
        return [pltpu.make_async_copy(a_buf.at[half, pl.ds(k * CHUNK, CHUNK)], a_hbm.at[row_of(g, first + k)], a_sem.at[half, k]) for k in range(HALF)]

    wqkv_copy = pltpu.make_async_copy(wqkv_hbm, wu.at[:, pl.ds(0, 3 * WIDTH)], w_sem.at[0])
    w_copies = [pltpu.make_async_copy(wu_hbm, wu, w_sem.at[1]), pltpu.make_async_copy(wd_hbm, wd, w_sem.at[2])]
    for head in range(HEADS):
        w_copies.append(pltpu.make_async_copy(wo_hbm.at[pl.ds(head * HEAD_DIM, HEAD_DIM)], wo.at[pl.ds((head % 2) * QUAD + (head // 2) * HEAD_DIM, HEAD_DIM)], w_sem.at[3 + head]))
    side_copies = (pltpu.make_async_copy(wkv, wkv_hbm, side_sem.at[0]), pltpu.make_async_copy(trig, trig_hbm, side_sem.at[1]))

    def c_copies(g):
        return (remote(o_buf.at[g, pl.ds(4, 4)], c_recv.at[g], c_ssem.at[g, 0], c_rsem.at[g, 0], to_core), remote(stat.at[g, 0], c_stat.at[g], c_ssem.at[g, 1], c_rsem.at[g, 1], to_core))

    def x_copies(g):
        return (remote(o_buf.at[g, pl.ds(2, 2)], x_recv.at[g], x_ssem.at[g, 0], x_rsem.at[g, 0], to_x), remote(cx_stat.at[g, pl.ds(2, 2)], x_stat.at[g], x_ssem.at[g, 1], x_rsem.at[g, 1], to_x))

    def y_copy(g):
        return remote(y_send.at[g], y_recv.at[g], y_ssem.at[g], y_rsem.at[g], to_y)

    def f_copy(g, src, dst, k, device):
        return remote(fin.at[g, src], fin.at[g, dst], f_ssem.at[g, k], f_rsem.at[g, dst], device)

    def out_copy(g, slot):
        return pltpu.make_async_copy(stage.at[g % 2, slot], out_hbm.at[row_of(g, slot)], out_sem.at[g % 2, slot])

    lane = lax.broadcasted_iota(jnp.int32, (CHUNK, PAIR), 1)
    low_half = lane < HEAD_DIM
    is_max = lax.broadcasted_iota(jnp.int32, (8, PAIR), 0) < HEADS // 2
    quad_lane = lax.broadcasted_iota(jnp.int32, (CHUNK, QUAD), 1)

    def block_diagonal(q_quad):
        zero = jnp.zeros_like(q_quad)
        return jnp.concatenate([jnp.where(quad_lane // HEAD_DIM == k, q_quad, zero) for k in range(4)], axis=0)

    def rotate(values, turned, tables, scale):
        return ((values.astype(F32) * tables[0] + turned * tables[1]) * scale).astype(BF16)

    def project(g, half):
        first = 4 - 4 * half

        @pl.when(g >= 1)
        def _():
            for copy in a_copies(g - 1, half):
                copy.wait()

        x = x_buf[g % 2, first:first + HALF].reshape(HALF * CHUNK, D_MODEL).astype(F32)
        normed = normalize(x, gain1_ref[...].reshape(1, D_MODEL), bias1_ref[...].reshape(1, D_MODEL))
        a_buf[half] = normed
        for copy in a_copies(g, half):
            copy.start()
        q_all = (jnp.dot(normed, wq[...], preferred_element_type=F32) + bias_q[...]).astype(BF16)
        tables = [row_tables(trig, row_of(g, first + k)) for k in range(HALF)]
        for pair in range(HEADS // 2):
            cols = slice(pair * PAIR, (pair + 1) * PAIR)
            turned = jnp.dot(q_all[:, cols], rot_ref[...], preferred_element_type=F32)
            for k in range(HALF):
                tokens = slice(k * CHUNK, (k + 1) * CHUNK)
                q_buf[first + k, :, cols] = rotate(q_all[tokens, cols], turned[tokens], tables[k], HEAD_DIM ** -0.5)

    def slot_at(j):
        return (j + HALF) % GROUP

    def score_unit(g, j, quad, s_buf):
        slot = slot_at(j)
        dims = slice(quad * QUAD, (quad + 1) * QUAD)
        row_len = len_ref[row_of(g, slot)]
        valid = cp_id * SLOTS + lax.broadcasted_iota(jnp.int32, (SLOTS, QUAD), 0) < row_len
        q4 = block_diagonal(q_buf[slot, :, dims])
        scores = lax.dot_general(kbuf[(g * GROUP + j) % K_BUFS, dims, :], q4, (((0,), (1,)), ((), ())), preferred_element_type=F32)
        s_buf[...] = jnp.where(valid, scores, NEG_BIG)

    def soft_unit(g, j, quad, s_buf, p_buf):
        top = jnp.full((8, QUAD), MAX_FLOOR, F32)
        for k in range(SLOTS // STRIP):
            top = jnp.maximum(top, jnp.max(s_buf[k * STRIP:(k + 1) * STRIP, :].reshape(STRIP // 8, 8, QUAD), axis=0))
        top = jnp.max(top, axis=0, keepdims=True)
        total = jnp.zeros((8, QUAD), F32)
        for k in range(SLOTS // STRIP):
            slots = slice(k * STRIP, (k + 1) * STRIP)
            probs = jnp.exp(s_buf[slots, :] - top)
            total = total + jnp.sum(probs.reshape(STRIP // 8, 8, QUAD), axis=0)
            p_buf[slots, :] = probs.astype(BF16)
        total = jnp.sum(total, axis=0, keepdims=True)
        for sub in range(2):
            pair = 2 * quad + sub
            cols = slice(sub * PAIR, (sub + 1) * PAIR)
            stat[g, j // HALF, j % HALF, pair:pair + 1, :] = top[:, cols]
            stat[g, j // HALF, j % HALF, 4 + pair:5 + pair, :] = total[:, cols]

    def value_unit(g, j, quad, p_buf):
        slot = slot_at(j)
        for sub in range(2):
            pair = 2 * quad + sub
            both = jnp.dot(vbuf[(g * GROUP + j) % V_BUFS, pair * PAIR:(pair + 1) * PAIR, :], p_buf[:, sub * PAIR:(sub + 1) * PAIR], preferred_element_type=F32)
            o_buf[g, slot, pair * HEAD_DIM:(pair + 1) * HEAD_DIM, :] = jnp.where(low_half, both[:HEAD_DIM], both[HEAD_DIM:])

    def attend_group(g):
        first = g * GROUP

        def fetch(j):
            for copy in kv_copies(first + j):
                copy.wait()

            @pl.when(first + j + AHEAD < ROWS)
            def _():
                for copy in kv_copies(first + j + AHEAD):
                    copy.start()

        def scores_of(j):
            score_unit(g, j, 0, s0)
            score_unit(g, j, 1, s1)

        def soft_of(j):
            soft_unit(g, j, 0, s0, p0)
            soft_unit(g, j, 1, s1, p1)

        def values_of(j):
            value_unit(g, j, 0, p0)
            value_unit(g, j, 1, p1)

        fetch(0)
        scores_of(0)
        fetch(1)
        soft_of(0)
        scores_of(1)

        def step(j, carry):
            fetch(j)
            values_of(j - 2)
            soft_of(j - 1)
            scores_of(j)

            @pl.when(j == HALF + 1)
            def _():
                for copy in c_copies(g):
                    copy.start()

            return carry

        lax.fori_loop(2, GROUP, step, 0)
        values_of(GROUP - 2)
        soft_of(GROUP - 1)
        values_of(GROUP - 1)

    def core_stage(g):
        for copy in c_copies(g):
            copy.wait_recv()
        for slot in (2, 3, 0, 1):
            mine = stat[g, 1, slot]
            theirs = c_stat[g, slot]
            top = jnp.maximum(mine, theirs)
            w_mine = jnp.exp(mine - top)
            w_theirs = jnp.exp(theirs - top)
            total = mine * pltpu.roll(w_mine, 4, 0) + theirs * pltpu.roll(w_theirs, 4, 0)
            cx_stat[g, slot] = jnp.where(is_max, top, total)
            for pair in range(HEADS // 2):
                dims = slice(pair * HEAD_DIM, (pair + 1) * HEAD_DIM)
                o_buf[g, slot, dims, :] = o_buf[g, slot, dims, :] * w_mine[pair:pair + 1] + c_recv[g, slot, dims, :] * w_theirs[pair:pair + 1]
            if slot == 3:
                for copy in x_copies(g):
                    copy.start()

    def prepare(g):
        kv = (jnp.dot(a_buf[1, :2 * CHUNK], wkv[...], preferred_element_type=F32) + bias_kv[...]).astype(BF16)
        tables = [row_tables(trig, row_of(g, slot)) for slot in range(2)]
        for pair in range(HEADS // 2):
            cols = slice(pair * PAIR, (pair + 1) * PAIR)
            turned = jnp.dot(kv[:, cols], rot_ref[...], preferred_element_type=F32)
            for slot in range(2):
                tokens = slice(slot * CHUNK, (slot + 1) * CHUNK)
                kv_self[slot, :, cols] = rotate(kv[tokens, cols], turned[tokens], tables[slot], 1.0)
        for slot in range(2):
            kv_self[slot, :, WIDTH:] = kv[slot * CHUNK:(slot + 1) * CHUNK, WIDTH:]
        causal = lax.broadcasted_iota(jnp.int32, (CHUNK, QUAD), 0) <= quad_lane % CHUNK
        for slot in range(2):
            for quad in range(2):
                dims = slice(quad * QUAD, (quad + 1) * QUAD)
                q4 = block_diagonal(q_buf[slot, :, dims])
                scores = lax.dot_general(kv_self[slot, :, dims], q4, (((1,), (1,)), ((), ())), preferred_element_type=F32)
                scores = jnp.where(causal, scores, NEG_BIG)
                top = jnp.max(scores, axis=0, keepdims=True)
                probs = jnp.where(causal, jnp.exp(scores - top), 0.0)
                total = jnp.sum(probs, axis=0, keepdims=True)
                packed = probs.astype(BF16)
                for sub in range(2):
                    pair = 2 * quad + sub
                    cols = slice(sub * PAIR, (sub + 1) * PAIR)
                    both = lax.dot_general(kv_self[slot, :, WIDTH + pair * PAIR:WIDTH + (pair + 1) * PAIR], packed[:, cols], (((0,), (0,)), ((), ())), preferred_element_type=F32)
                    own_o[slot, pair * HEAD_DIM:(pair + 1) * HEAD_DIM, :] = jnp.where(low_half, both[:HEAD_DIM], both[HEAD_DIM:])
                    own_stat[slot, pair:pair + 1, :] = top[:, cols]
                    own_stat[slot, 4 + pair:5 + pair, :] = total[:, cols]
        x_both = x_buf[g % 2, :2].reshape(2 * CHUNK, D_MODEL).astype(F32)
        normed = normalize(x_both, gain2_ref[...].reshape(1, D_MODEL), bias2_ref[...].reshape(1, D_MODEL))
        up = jnp.dot(normed, wu[...], preferred_element_type=F32) + bu_ref[...].astype(F32).reshape(1, FF)
        hidden = (0.5 * up * (1.0 + lax.erf(up * (0.5 ** 0.5)))).astype(BF16)
        mlp_acc[...] = jnp.dot(hidden, wd[...], preferred_element_type=F32)
        y_keep[g % 3] = x_both[:CHUNK] + bo_ref[...].astype(F32).reshape(1, D_MODEL) + bd_ref[...].astype(F32).reshape(1, D_MODEL)

    def x_stage(g):
        for copy in x_copies(g):
            copy.wait_recv()
        for slot in range(2):
            mine = cx_stat[g, slot]
            theirs = x_stat[g, slot]
            own = own_stat[slot]
            top = jnp.maximum(jnp.maximum(mine, theirs), own)
            w_mine = jnp.exp(mine - top)
            w_theirs = jnp.exp(theirs - top)
            w_own = jnp.exp(own - top)
            total = mine * pltpu.roll(w_mine, 4, 0) + theirs * pltpu.roll(w_theirs, 4, 0) + own * pltpu.roll(w_own, 4, 0)
            inverse = pltpu.roll(1.0 / jnp.where(is_max, 1.0, total), 4, 0)
            w_mine = w_mine * inverse
            w_theirs = w_theirs * inverse
            w_own = w_own * inverse
            values = []
            for pair in range(HEADS // 2):
                dims = slice(pair * HEAD_DIM, (pair + 1) * HEAD_DIM)
                one = slice(pair, pair + 1)
                values.append(o_buf[g, slot, dims, :] * w_mine[one] + x_recv[g, slot, dims, :] * w_theirs[one] + own_o[slot, dims, :] * w_own[one])
            turned = jnp.concatenate(values, axis=0).T
            for half in range(2):
                ctx[slot * CHUNK:(slot + 1) * CHUNK, half * QUAD:(half + 1) * QUAD] = turned[half * CHUNK:(half + 1) * CHUNK].astype(BF16)
        branch = jnp.dot(ctx[...], wo[...], preferred_element_type=F32) + mlp_acc[...]
        y_send[g] = branch[CHUNK:]
        y_copy(g).start()
        y_keep[g % 3] = y_keep[g % 3] + branch[:CHUNK]

    def y_stage(g):
        y_copy(g).wait_recv()
        fin[g, 0] = y_keep[g % 3] + y_recv[g]
        f_copy(g, 0, 2, 0, to_x).start()
        f_copy(g, 0, 1, 1, to_y).start()
        f_copy(g, 0, 4, 2, to_core).start()

    def forward_stage(g):
        f_copy(g, 0, 1, 1, to_y).wait_recv()
        f_copy(g, 0, 2, 0, to_x).wait_recv()

        @pl.when(g % 2 == 0)
        def _():
            f_copy(g, 1, 3, 3, to_x).start()

        @pl.when(g % 2 == 1)
        def _():
            f_copy(g, 2, 3, 3, to_y).start()

        f_copy(g, 1, 5, 4, to_core).start()
        f_copy(g, 2, 6, 5, to_core).start()

    def diagonal_stage(g):
        f_copy(g, 1, 3, 3, to_x).wait_recv()
        f_copy(g, 3, 7, 6, to_core).start()

    def out_stage(g):
        f_copy(g, 0, 4, 2, to_core).wait_recv()
        f_copy(g, 1, 5, 4, to_core).wait_recv()
        f_copy(g, 2, 6, 5, to_core).wait_recv()
        f_copy(g, 3, 7, 6, to_core).wait_recv()

        @pl.when(g >= 2)
        def _():
            for slot in range(GROUP):
                out_copy(g - 2, slot).wait()

        for slot in range(GROUP):
            stage[g % 2, slot] = fin[g, slot].astype(BF16)
            out_copy(g, slot).start()

    def when_group(g, work):
        @pl.when(jnp.logical_and(g >= 0, g < GROUPS))
        def _():
            work(g)

    wqkv_copy.start()
    for copy in x_in(0):
        copy.start()
    for n in range(AHEAD):
        for copy in kv_copies(n):
            copy.start()
    barrier = pltpu.get_barrier_semaphore()
    for device in (to_core, to_x, to_y):
        pl.semaphore_signal(barrier, inc=1, device_id=device, device_id_type=pl.DeviceIdType.MESH)

    dim = lane % HEAD_DIM
    freq = jnp.zeros((CHUNK, PAIR), F32)
    for k in range(ROT_DIM // 2):
        here = jnp.logical_and(dim % (ROT_DIM // 2) == k, dim < ROT_DIM)
        freq = jnp.where(here, float(np.float32(ROPE_BASE ** (-2.0 * k / ROT_DIM))), freq)

    def one_angle(r, carry):
        trig[0, pl.ds(r, 1), :] = len_ref[r].astype(F32) * freq[:1]
        return carry

    lax.fori_loop(0, ROWS, one_angle, 0)
    angles = trig[0]
    trig[1] = jnp.sin(angles)
    trig[0] = jnp.cos(angles)
    angles = lax.broadcasted_iota(jnp.int32, (CHUNK, PAIR), 0).astype(F32) * freq
    trig[2] = jnp.cos(angles)
    trig[3] = jnp.sin(angles)
    q_bias, k_bias, v_bias = bias_parts(bq_ref[...].astype(F32).reshape(1, 3 * WIDTH))
    bias_q[...] = q_bias
    bias_kv[:, :WIDTH] = k_bias
    bias_kv[:, WIDTH:] = v_bias
    wqkv_copy.wait()

    def arrange(r, carry):
        rows = pl.ds(pl.multiple_of(r * PAIR, PAIR), PAIR)
        low = lax.broadcasted_iota(jnp.int32, (PAIR, PAIR), 1) < HEAD_DIM
        for pair in range(HEADS // 2):
            q_part, k_part, v_part = pick_parts([wu[rows, (3 * pair + k) * PAIR:(3 * pair + k + 1) * PAIR] for k in range(3)], low)
            wq[rows, pair * PAIR:(pair + 1) * PAIR] = q_part
            wkv[rows, pair * PAIR:(pair + 1) * PAIR] = k_part
            wkv[rows, WIDTH + pair * PAIR:WIDTH + (pair + 1) * PAIR] = v_part
        return carry

    lax.fori_loop(0, D_MODEL // PAIR, arrange, 0)
    for copy in w_copies:
        copy.start()
    for copy in side_copies:
        copy.start()
    pl.semaphore_wait(barrier, 3)

    def iteration(i, carry):
        @pl.when(i + 1 < GROUPS)
        def _():
            for copy in x_in(i + 1):
                copy.start()

        when_group(i - DIAGONAL_LAG, diagonal_stage)

        @pl.when(i < GROUPS)
        def _():
            for copy in x_in(i):
                copy.wait()
            project(i, 0)
            project(i, 1)
            attend_group(i)
            core_stage(i)

        when_group(i - 1, x_stage)
        when_group(i - FORWARD_LAG, forward_stage)
        when_group(i - DIAGONAL_LAG, out_stage)
        when_group(i - 2, y_stage)

        @pl.when(i == 0)
        def _():
            for copy in w_copies:
                copy.wait()

        when_group(i, prepare)
        return carry

    lax.fori_loop(0, GROUPS + DIAGONAL_LAG, iteration, 0)
    for copy in side_copies:
        copy.wait()
    for half in range(2):
        for copy in a_copies(GROUPS - 1, half):
            copy.wait()
    for g in (GROUPS - 2, GROUPS - 1):
        for slot in range(GROUP):
            out_copy(g, slot).wait()

    def finish(g, carry):
        for copy in c_copies(g) + x_copies(g) + (y_copy(g),):
            copy.wait_send()
        for src, dst, k, device in ((0, 2, 0, to_x), (0, 1, 1, to_y), (0, 4, 2, to_core), (1, 3, 3, to_x), (1, 5, 4, to_core), (2, 6, 5, to_core), (3, 7, 6, to_core)):
            f_copy(g, src, dst, k, device).wait_send()
        return carry

    lax.fori_loop(0, GROUPS, finish, 0)


def layer_call(lengths, k_cache, v_cache, x, gain1, bias1, gain2, bias2, w_qkv, b_qkv, rot, w_out, w_up, b_up, w_down, b_out, b_down):
    vmem = pl.BlockSpec(memory_space=pltpu.VMEM)
    dma = pltpu.SemaphoreType.DMA
    return pl.pallas_call(
        layer_kernel,
        in_specs=[pl.BlockSpec(memory_space=pltpu.SMEM), ANY, ANY, ANY, vmem, vmem, vmem, vmem, ANY, vmem, vmem, ANY, ANY, vmem, ANY, vmem, vmem],
        out_specs=[ANY, ANY, ANY, ANY],
        out_shape=[
            jax.ShapeDtypeStruct((ROWS, CHUNK, D_MODEL), BF16),
            jax.ShapeDtypeStruct((ROWS, CHUNK, D_MODEL), BF16),
            jax.ShapeDtypeStruct((D_MODEL, 2 * WIDTH), BF16),
            jax.ShapeDtypeStruct((4, CHUNK, PAIR), F32),
        ],
        scratch_shapes=[
            pltpu.VMEM((WIDTH, D_MODEL), BF16),
            pltpu.VMEM((D_MODEL, FF), BF16),
            pltpu.VMEM((FF, D_MODEL), BF16),
            pltpu.VMEM((D_MODEL, WIDTH), BF16),
            pltpu.VMEM((D_MODEL, 2 * WIDTH), BF16),
            pltpu.VMEM((1, WIDTH), F32),
            pltpu.VMEM((1, 2 * WIDTH), F32),
            pltpu.VMEM((4, CHUNK, PAIR), F32),
            pltpu.VMEM((K_BUFS, WIDTH, SLOTS), BF16),
            pltpu.VMEM((V_BUFS, WIDTH, SLOTS), BF16),
            pltpu.VMEM((SLOTS, QUAD), F32),
            pltpu.VMEM((SLOTS, QUAD), F32),
            pltpu.VMEM((SLOTS, QUAD), BF16),
            pltpu.VMEM((SLOTS, QUAD), BF16),
            pltpu.VMEM((2, GROUP, CHUNK, D_MODEL), BF16),
            pltpu.VMEM((2, HALF * CHUNK, D_MODEL), BF16),
            pltpu.VMEM((GROUP, CHUNK, WIDTH), BF16),
            pltpu.VMEM((2, CHUNK, 2 * WIDTH), BF16),
            pltpu.VMEM((2, QUAD, PAIR), F32),
            pltpu.VMEM((2, 8, PAIR), F32),
            pltpu.VMEM((2 * CHUNK, D_MODEL), F32),
            pltpu.VMEM((GROUPS, GROUP, QUAD, PAIR), F32),
            pltpu.VMEM((GROUPS, 2, HALF, 8, PAIR), F32),
            pltpu.VMEM((GROUPS, HALF, QUAD, PAIR), F32),
            pltpu.VMEM((GROUPS, HALF, 8, PAIR), F32),
            pltpu.VMEM((GROUPS, HALF, 8, PAIR), F32),
            pltpu.VMEM((GROUPS, 2, QUAD, PAIR), F32),
            pltpu.VMEM((GROUPS, 2, 8, PAIR), F32),
            pltpu.VMEM((2 * CHUNK, WIDTH), BF16),
            pltpu.VMEM((GROUPS, CHUNK, D_MODEL), F32),
            pltpu.VMEM((3, CHUNK, D_MODEL), F32),
            pltpu.VMEM((GROUPS, CHUNK, D_MODEL), F32),
            pltpu.VMEM((GROUPS, GROUP, CHUNK, D_MODEL), F32),
            pltpu.VMEM((2, GROUP, CHUNK, D_MODEL), BF16),
            dma((3 + HEADS,)), dma((K_BUFS,)), dma((V_BUFS,)), dma((2, GROUP)), dma((2, HALF)), dma((2,)),
            dma((GROUPS, 2)), dma((GROUPS, 2)), dma((GROUPS, 2)), dma((GROUPS, 2)),
            dma((GROUPS,)), dma((GROUPS,)), dma((GROUPS, 7)), dma((GROUPS, GROUP)), dma((2, GROUP)),
        ],
        compiler_params=pltpu.CompilerParams(collective_id=0, has_side_effects=True, vmem_limit_bytes=67_000_000),
        cost_estimate=pl.CostEstimate(flops=30 * 10 ** 9, bytes_accessed=100 << 20, transcendentals=0),
        name="layer",
    )(lengths, k_cache, v_cache, x, gain1, bias1, gain2, bias2, w_qkv, b_qkv, rot, w_out, w_up, b_up, w_down, b_out, b_down)


def solution(mesh):
    in_specs = (P("dp", None, None), P("dp"), P("dp", "tp", "cp", None), P("dp", "tp", "cp", None), P(), P(), P(), P(), P(None, "tp"), P("tp"), P("tp", None), P(), P(None, "tp"), P("tp"), P("tp", None), P())
    out_specs = (P("dp", None, None), P("dp", "tp", None, None), P("dp", "tp", None, None))

    def local_layer(hidden_in, lengths, k_block, v_block, ln1_gain, ln1_bias, ln2_gain, ln2_bias, w_qkv, b_qkv, w_out, b_out, w_up, b_up, w_down, b_down):
        slot_minor = lambda cache: jnp.swapaxes(cache, 2, 3).reshape(ROWS, WIDTH, SLOTS)
        rot = jnp.asarray(rotate_matrix(), BF16)
        through, normed, w_kv, trig = layer_call(lengths, slot_minor(k_block), slot_minor(v_block), hidden_in, ln1_gain, ln1_bias, ln2_gain, ln2_bias, w_qkv, b_qkv, rot, w_out, w_up, b_up, w_down, b_out, b_down)
        flat = lambda values: values.reshape(ROWS * CHUNK, D_MODEL)
        out, k_new, v_new = tail_call(flat(normed), w_kv, b_qkv, trig, rot, flat(through))
        return out.reshape(ROWS, CHUNK, D_MODEL), k_new, v_new

    return jax.shard_map(local_layer, mesh=mesh, in_specs=in_specs, out_specs=out_specs, check_vma=False)
```

```python
import functools
import numpy as np
import jax
import jax.numpy as jnp
from jax import lax
from jax.experimental import pallas as pl
from jax.experimental.pallas import tpu as pltpu
from jax.sharding import PartitionSpec as P

EPSILON = 1e-5
NEG_BIG = -1e30
MAX_FLOOR = -1e29
ROPE_BASE = 10000.0
HEAD_DIM = 64
ROT_DIM = 16
PAIR = 2 * HEAD_DIM
ROWS = 64
CHUNK = 64
HEADS = 8
WIDTH = HEADS * HEAD_DIM
SLOTS = 512
D_MODEL = 1024
FF = 2048
GROUP = 8
GROUPS = ROWS // GROUP
K_BUFS = 3
V_BUFS = 5
AHEAD = 2
STRIP = 64
FORWARD_LAG = 5
DIAGONAL_LAG = 8
OUT_LAG = 9
QUAD = 4 * HEAD_DIM
HALF = GROUP // 2
TAIL_ROWS = 4
TAIL_SLOTS = 4
F32 = jnp.float32
BF16 = jnp.bfloat16
ANY = pl.BlockSpec(memory_space=pl.ANY)


def normalize(x_f32, gain, bias):
    row_mean = jnp.mean(x_f32, axis=-1, keepdims=True)
    centered = x_f32 - row_mean
    variance = jnp.mean(centered * centered, axis=-1, keepdims=True)
    return (centered * lax.rsqrt(variance + EPSILON) * gain + bias).astype(BF16)


def rotate_matrix():
    matrix = np.zeros((PAIR, PAIR), np.float32)
    half = ROT_DIM // 2
    for base in (0, HEAD_DIM):
        for i in range(half):
            matrix[base + half + i, base + i] = -1.0
            matrix[base + i, base + half + i] = 1.0
    return matrix


def swap_halves(pair):
    return jnp.concatenate([pair[:, HEAD_DIM:], pair[:, :HEAD_DIM]], axis=1)


def pick_parts(blocks, low_half):
    first, second, third = blocks
    return jnp.where(low_half, first, second), swap_halves(jnp.where(low_half, third, first)), jnp.where(low_half, second, third)


def bias_parts(bias_row):
    low_half = lax.broadcasted_iota(jnp.int32, (1, PAIR), 1) < HEAD_DIM
    parts = [pick_parts([bias_row[:, (3 * pair + k) * PAIR:(3 * pair + k + 1) * PAIR] for k in range(3)], low_half) for pair in range(HEADS // 2)]
    return [jnp.concatenate([parts[pair][k] for pair in range(HEADS // 2)], axis=1) for k in range(3)]


def row_tables(trig, row):
    cos_len = trig[0, pl.ds(row, 1), :]
    sin_len = trig[1, pl.ds(row, 1), :]
    cos_c = trig[2]
    sin_c = trig[3]
    return cos_len * cos_c - sin_len * sin_c, sin_len * cos_c + cos_len * sin_c


def tail_kernel(kv_hbm, through_hbm, out_hbm, k_hbm, v_hbm, kv_all, passing, k_stage, v_stage, kv_sem, in_sem, out_sem, k_sem, v_sem):
    blocks = ROWS // TAIL_ROWS

    def rows(i):
        return pl.ds(i * TAIL_ROWS, TAIL_ROWS)

    kv_in = lambda i: pltpu.make_async_copy(kv_hbm.at[rows(i)], kv_all.at[i], kv_sem.at[i])
    pass_in = lambda i: pltpu.make_async_copy(through_hbm.at[rows(i)], passing.at[i], in_sem.at[i])
    pass_out = lambda i: pltpu.make_async_copy(passing.at[i], out_hbm.at[rows(i)], out_sem.at[i])
    k_put = lambda i: pltpu.make_async_copy(k_stage.at[i % TAIL_SLOTS], k_hbm.at[rows(i)], k_sem.at[i % TAIL_SLOTS])
    v_put = lambda i: pltpu.make_async_copy(v_stage.at[i % TAIL_SLOTS], v_hbm.at[rows(i)], v_sem.at[i % TAIL_SLOTS])

    for i in range(blocks):
        kv_in(i).start()
        pass_in(i).start()

    def step(i, carry):
        @pl.when(i >= TAIL_SLOTS)
        def _():
            k_put(i - TAIL_SLOTS).wait()
            v_put(i - TAIL_SLOTS).wait()

        kv_in(i).wait()
        slot = i % TAIL_SLOTS
        for row in range(TAIL_ROWS):
            for head in range(HEADS):
                dims = slice(head * HEAD_DIM, (head + 1) * HEAD_DIM)
                k_stage[slot, row, head] = kv_all[i, row, :, dims]
                v_stage[slot, row, head] = kv_all[i, row, :, WIDTH + head * HEAD_DIM:WIDTH + (head + 1) * HEAD_DIM]
        k_put(i).start()
        v_put(i).start()
        pass_in(i).wait()
        pass_out(i).start()
        return carry

    lax.fori_loop(0, blocks, step, 0)
    for i in range(blocks - TAIL_SLOTS, blocks):
        k_put(i).wait()
        v_put(i).wait()
    for i in range(blocks):
        pass_out(i).wait()


def tail_call(kv, through):
    blocks = ROWS // TAIL_ROWS
    dma = pltpu.SemaphoreType.DMA
    return pl.pallas_call(
        tail_kernel,
        in_specs=[ANY, ANY],
        out_specs=[ANY, ANY, ANY],
        out_shape=[
            jax.ShapeDtypeStruct((ROWS, CHUNK, D_MODEL), BF16),
            jax.ShapeDtypeStruct((ROWS, HEADS, CHUNK, HEAD_DIM), BF16),
            jax.ShapeDtypeStruct((ROWS, HEADS, CHUNK, HEAD_DIM), BF16),
        ],
        scratch_shapes=[
            pltpu.VMEM((blocks, TAIL_ROWS, CHUNK, D_MODEL), BF16),
            pltpu.VMEM((blocks, TAIL_ROWS, CHUNK, D_MODEL), BF16),
            pltpu.VMEM((TAIL_SLOTS, TAIL_ROWS, HEADS, CHUNK, HEAD_DIM), BF16),
            pltpu.VMEM((TAIL_SLOTS, TAIL_ROWS, HEADS, CHUNK, HEAD_DIM), BF16),
            dma((blocks,)), dma((blocks,)), dma((blocks,)), dma((TAIL_SLOTS,)), dma((TAIL_SLOTS,)),
        ],
        cost_estimate=pl.CostEstimate(flops=1 << 20, bytes_accessed=42 << 20, transcendentals=0),
        compiler_params=pltpu.CompilerParams(vmem_limit_bytes=60_000_000),
        name="tail",
    )(kv, through)


def layer_kernel(len_ref, kc_hbm, vc_hbm, x_hbm, gain1_ref, bias1_ref, gain2_ref, bias2_ref, wqkv_hbm, bq_ref, rot_ref, wo_hbm, wu_hbm, bu_ref, wd_hbm, bo_ref, bd_ref,
                 out_hbm, a_hbm, kv_hbm,
                 wo, wu, wd, wq, wkv, bias_q, bias_kv, trig, kbuf, vbuf, s0, s1, p0, p1, x_buf, a_buf, q_buf, kv_self, own_o, own_stat, mlp_acc,
                 o_buf, stat, c_recv, c_stat, cx_stat, x_recv, x_stat, ctx, y_send, y_keep, y_recv, fin, stage,
                 w_sem, k_sem, v_sem, xin_sem, a_sem, kv_sem, c_ssem, c_rsem, x_ssem, x_rsem, y_ssem, y_rsem, f_ssem, f_rsem, out_sem):
    tp_id = lax.axis_index("tp")
    cp_id = lax.axis_index("cp")
    chip_x = cp_id // 2
    core = cp_id % 2
    to_core = {"cp": 2 * chip_x + 1 - core}
    to_x = {"cp": 2 * (1 - chip_x) + core}
    to_y = {"tp": 1 - tp_id}

    def flip(bit, mine):
        return bit + mine - 2 * bit * mine

    def row_of(group, slot):
        return group * GROUP + 4 * flip(slot // 4, core) + 2 * flip((slot // 2) % 2, chip_x) + flip(slot % 2, tp_id)

    def remote(src, dst, ssem, rsem, device):
        return pltpu.make_async_remote_copy(src_ref=src, dst_ref=dst, send_sem=ssem, recv_sem=rsem, device_id=device, device_id_type=pl.DeviceIdType.MESH)

    def kv_copies(n):
        kb = n % K_BUFS
        vb = n % V_BUFS
        row = row_of(n // GROUP, (n % GROUP + 4) % GROUP)
        return (pltpu.make_async_copy(kc_hbm.at[row], kbuf.at[kb], k_sem.at[kb]), pltpu.make_async_copy(vc_hbm.at[row], vbuf.at[vb], v_sem.at[vb]))

    def x_in(g):
        return [pltpu.make_async_copy(x_hbm.at[row_of(g, slot)], x_buf.at[g % 2, slot], xin_sem.at[g % 2, slot]) for slot in range(GROUP)]

    def a_copies(g, half):
        first = 4 - 4 * half
        return [pltpu.make_async_copy(a_buf.at[half, pl.ds(k * CHUNK, CHUNK)], a_hbm.at[row_of(g, first + k)], a_sem.at[half, k]) for k in range(HALF)]

    wqkv_copy = pltpu.make_async_copy(wqkv_hbm, wu.at[:, pl.ds(0, 3 * WIDTH)], w_sem.at[0])
    w_copies = [pltpu.make_async_copy(wu_hbm, wu, w_sem.at[1]), pltpu.make_async_copy(wd_hbm, wd, w_sem.at[2])]
    for head in range(HEADS):
        w_copies.append(pltpu.make_async_copy(wo_hbm.at[pl.ds(head * HEAD_DIM, HEAD_DIM)], wo.at[pl.ds((head % 2) * QUAD + (head // 2) * HEAD_DIM, HEAD_DIM)], w_sem.at[3 + head]))

    def a_back(g):
        return [pltpu.make_async_copy(a_hbm.at[row_of(g, slot)], x_buf.at[g % 2, slot], xin_sem.at[g % 2, slot]) for slot in range(GROUP)]

    def kv_put(g):
        return [pltpu.make_async_copy(x_buf.at[g % 2, slot], kv_hbm.at[row_of(g, slot)], kv_sem.at[g % 2, slot]) for slot in range(GROUP)]

    def c_copies(g):
        return (remote(o_buf.at[g, pl.ds(4, 4)], c_recv.at[g], c_ssem.at[g, 0], c_rsem.at[g, 0], to_core), remote(stat.at[g, 0], c_stat.at[g], c_ssem.at[g, 1], c_rsem.at[g, 1], to_core))

    def x_copies(g):
        return (remote(o_buf.at[g, pl.ds(2, 2)], x_recv.at[g], x_ssem.at[g, 0], x_rsem.at[g, 0], to_x), remote(cx_stat.at[g, pl.ds(2, 2)], x_stat.at[g], x_ssem.at[g, 1], x_rsem.at[g, 1], to_x))

    def y_copy(g):
        return remote(y_send.at[g], y_recv.at[g], y_ssem.at[g], y_rsem.at[g], to_y)

    def f_copy(g, src, dst, k, device):
        return remote(fin.at[g, src], fin.at[g, dst], f_ssem.at[g, k], f_rsem.at[g, dst], device)

    def out_copy(g, slot):
        return pltpu.make_async_copy(stage.at[g % 2, slot], out_hbm.at[row_of(g, slot)], out_sem.at[g % 2, slot])

    lane = lax.broadcasted_iota(jnp.int32, (CHUNK, PAIR), 1)
    low_half = lane < HEAD_DIM
    is_max = lax.broadcasted_iota(jnp.int32, (8, PAIR), 0) < HEADS // 2
    quad_lane = lax.broadcasted_iota(jnp.int32, (CHUNK, QUAD), 1)

    def block_diagonal(q_quad):
        zero = jnp.zeros_like(q_quad)
        return jnp.concatenate([jnp.where(quad_lane // HEAD_DIM == k, q_quad, zero) for k in range(4)], axis=0)

    def rotate(values, turned, tables, scale):
        return ((values.astype(F32) * tables[0] + turned * tables[1]) * scale).astype(BF16)

    def project(g, half):
        first = 4 - 4 * half

        @pl.when(g >= 1)
        def _():
            for copy in a_copies(g - 1, half):
                copy.wait()

        x = x_buf[g % 2, first:first + HALF].reshape(HALF * CHUNK, D_MODEL).astype(F32)
        normed = normalize(x, gain1_ref[...].reshape(1, D_MODEL), bias1_ref[...].reshape(1, D_MODEL))
        a_buf[half] = normed
        for copy in a_copies(g, half):
            copy.start()
        q_all = (jnp.dot(normed, wq[...], preferred_element_type=F32) + bias_q[...]).astype(BF16)
        tables = [row_tables(trig, row_of(g, first + k)) for k in range(HALF)]
        for pair in range(HEADS // 2):
            cols = slice(pair * PAIR, (pair + 1) * PAIR)
            turned = jnp.dot(q_all[:, cols], rot_ref[...], preferred_element_type=F32)
            for k in range(HALF):
                tokens = slice(k * CHUNK, (k + 1) * CHUNK)
                q_buf[first + k, :, cols] = rotate(q_all[tokens, cols], turned[tokens], tables[k], HEAD_DIM ** -0.5)

    def slot_at(j):
        return (j + HALF) % GROUP

    def score_unit(g, j, quad, s_buf):
        slot = slot_at(j)
        dims = slice(quad * QUAD, (quad + 1) * QUAD)
        row_len = len_ref[row_of(g, slot)]
        valid = cp_id * SLOTS + lax.broadcasted_iota(jnp.int32, (SLOTS, QUAD), 0) < row_len
        q4 = block_diagonal(q_buf[slot, :, dims])
        scores = lax.dot_general(kbuf[(g * GROUP + j) % K_BUFS, dims, :], q4, (((0,), (1,)), ((), ())), preferred_element_type=F32)
        s_buf[...] = jnp.where(valid, scores, NEG_BIG)

    def soft_unit(g, j, quad, s_buf, p_buf):
        top = jnp.full((8, QUAD), MAX_FLOOR, F32)
        for k in range(SLOTS // STRIP):
            top = jnp.maximum(top, jnp.max(s_buf[k * STRIP:(k + 1) * STRIP, :].reshape(STRIP // 8, 8, QUAD), axis=0))
        top = jnp.max(top, axis=0, keepdims=True)
        total = jnp.zeros((8, QUAD), F32)
        for k in range(SLOTS // STRIP):
            slots = slice(k * STRIP, (k + 1) * STRIP)
            probs = jnp.exp(s_buf[slots, :] - top)
            total = total + jnp.sum(probs.reshape(STRIP // 8, 8, QUAD), axis=0)
            p_buf[slots, :] = probs.astype(BF16)
        total = jnp.sum(total, axis=0, keepdims=True)
        for sub in range(2):
            pair = 2 * quad + sub
            cols = slice(sub * PAIR, (sub + 1) * PAIR)
            stat[g, j // HALF, j % HALF, pair:pair + 1, :] = top[:, cols]
            stat[g, j // HALF, j % HALF, 4 + pair:5 + pair, :] = total[:, cols]

    def value_unit(g, j, quad, p_buf):
        slot = slot_at(j)
        for sub in range(2):
            pair = 2 * quad + sub
            both = jnp.dot(vbuf[(g * GROUP + j) % V_BUFS, pair * PAIR:(pair + 1) * PAIR, :], p_buf[:, sub * PAIR:(sub + 1) * PAIR], preferred_element_type=F32)
            o_buf[g, slot, pair * HEAD_DIM:(pair + 1) * HEAD_DIM, :] = jnp.where(low_half, both[:HEAD_DIM], both[HEAD_DIM:])

    def when_group(g, work):
        @pl.when(jnp.logical_and(g >= 0, g < GROUPS))
        def _():
            work(g)

    def attend_group(g):
        first = g * GROUP

        def fetch(j):
            for copy in kv_copies(first + j):
                copy.wait()

            @pl.when(first + j + AHEAD < ROWS)
            def _():
                for copy in kv_copies(first + j + AHEAD):
                    copy.start()

        def scores_of(j):
            score_unit(g, j, 0, s0)
            score_unit(g, j, 1, s1)

        def soft_of(j):
            soft_unit(g, j, 0, s0, p0)
            soft_unit(g, j, 1, s1, p1)

        def values_of(j):
            value_unit(g, j, 0, p0)
            value_unit(g, j, 1, p1)

        fetch(0)
        scores_of(0)
        fetch(1)
        soft_of(0)
        scores_of(1)

        def step(j, carry):
            fetch(j)
            values_of(j - 2)
            soft_of(j - 1)
            scores_of(j)

            @pl.when(j == HALF + 1)
            def _():
                for copy in c_copies(g):
                    copy.start()
                when_group(g - FORWARD_LAG, forward_stage)

            return carry

        lax.fori_loop(2, GROUP, step, 0)
        values_of(GROUP - 2)
        soft_of(GROUP - 1)
        values_of(GROUP - 1)

    def core_stage(g):
        for copy in c_copies(g):
            copy.wait_recv()
        for slot in (2, 3, 0, 1):
            mine = stat[g, 1, slot]
            theirs = c_stat[g, slot]
            top = jnp.maximum(mine, theirs)
            w_mine = jnp.exp(mine - top)
            w_theirs = jnp.exp(theirs - top)
            total = mine * pltpu.roll(w_mine, 4, 0) + theirs * pltpu.roll(w_theirs, 4, 0)
            cx_stat[g, slot] = jnp.where(is_max, top, total)
            for pair in range(HEADS // 2):
                dims = slice(pair * HEAD_DIM, (pair + 1) * HEAD_DIM)
                o_buf[g, slot, dims, :] = o_buf[g, slot, dims, :] * w_mine[pair:pair + 1] + c_recv[g, slot, dims, :] * w_theirs[pair:pair + 1]
            if slot == 3:
                for copy in x_copies(g):
                    copy.start()

    def prepare(g):
        kv = (jnp.dot(a_buf[1, :2 * CHUNK], wkv[...], preferred_element_type=F32) + bias_kv[...]).astype(BF16)
        tables = [row_tables(trig, row_of(g, slot)) for slot in range(2)]
        for pair in range(HEADS // 2):
            cols = slice(pair * PAIR, (pair + 1) * PAIR)
            turned = jnp.dot(kv[:, cols], rot_ref[...], preferred_element_type=F32)
            for slot in range(2):
                tokens = slice(slot * CHUNK, (slot + 1) * CHUNK)
                kv_self[slot, :, cols] = rotate(kv[tokens, cols], turned[tokens], tables[slot], 1.0)
        for slot in range(2):
            kv_self[slot, :, WIDTH:] = kv[slot * CHUNK:(slot + 1) * CHUNK, WIDTH:]
        causal = lax.broadcasted_iota(jnp.int32, (CHUNK, QUAD), 0) <= quad_lane % CHUNK
        for slot in range(2):
            for quad in range(2):
                dims = slice(quad * QUAD, (quad + 1) * QUAD)
                q4 = block_diagonal(q_buf[slot, :, dims])
                scores = lax.dot_general(kv_self[slot, :, dims], q4, (((1,), (1,)), ((), ())), preferred_element_type=F32)
                scores = jnp.where(causal, scores, NEG_BIG)
                top = jnp.max(scores, axis=0, keepdims=True)
                probs = jnp.where(causal, jnp.exp(scores - top), 0.0)
                total = jnp.sum(probs, axis=0, keepdims=True)
                packed = probs.astype(BF16)
                for sub in range(2):
                    pair = 2 * quad + sub
                    cols = slice(sub * PAIR, (sub + 1) * PAIR)
                    both = lax.dot_general(kv_self[slot, :, WIDTH + pair * PAIR:WIDTH + (pair + 1) * PAIR], packed[:, cols], (((0,), (0,)), ((), ())), preferred_element_type=F32)
                    own_o[slot, pair * HEAD_DIM:(pair + 1) * HEAD_DIM, :] = jnp.where(low_half, both[:HEAD_DIM], both[HEAD_DIM:])
                    own_stat[slot, pair:pair + 1, :] = top[:, cols]
                    own_stat[slot, 4 + pair:5 + pair, :] = total[:, cols]
        x_both = x_buf[g % 2, :2].reshape(2 * CHUNK, D_MODEL).astype(F32)
        normed = normalize(x_both, gain2_ref[...].reshape(1, D_MODEL), bias2_ref[...].reshape(1, D_MODEL))
        up = jnp.dot(normed, wu[...], preferred_element_type=F32) + bu_ref[...].astype(F32).reshape(1, FF)
        hidden = (0.5 * up * (1.0 + lax.erf(up * (0.5 ** 0.5)))).astype(BF16)
        mlp_acc[...] = jnp.dot(hidden, wd[...], preferred_element_type=F32)
        y_keep[g % 3] = x_both[:CHUNK] + bo_ref[...].astype(F32).reshape(1, D_MODEL) + bd_ref[...].astype(F32).reshape(1, D_MODEL)

    def keys_values(g):
        b = g % 2
        for copy in a_back(g):
            copy.wait()
        for half in range(2):
            first = half * HALF
            a = x_buf[b, first:first + HALF].reshape(HALF * CHUNK, D_MODEL)
            kv = (jnp.dot(a, wkv[...], preferred_element_type=F32) + bias_kv[...]).astype(BF16)
            for pair in range(HEADS // 2):
                cols = slice(pair * PAIR, (pair + 1) * PAIR)
                turned = jnp.dot(kv[:, cols], rot_ref[...], preferred_element_type=F32)
                for k in range(HALF):
                    tokens = slice(k * CHUNK, (k + 1) * CHUNK)
                    x_buf[b, first + k, :, cols] = rotate(kv[tokens, cols], turned[tokens], row_tables(trig, row_of(g, first + k)), 1.0)
            for k in range(HALF):
                x_buf[b, first + k, :, WIDTH:] = kv[k * CHUNK:(k + 1) * CHUNK, WIDTH:]
        for copy in kv_put(g):
            copy.start()

    def x_stage(g):
        for copy in x_copies(g):
            copy.wait_recv()
        for slot in range(2):
            mine = cx_stat[g, slot]
            theirs = x_stat[g, slot]
            own = own_stat[slot]
            top = jnp.maximum(jnp.maximum(mine, theirs), own)
            w_mine = jnp.exp(mine - top)
            w_theirs = jnp.exp(theirs - top)
            w_own = jnp.exp(own - top)
            total = mine * pltpu.roll(w_mine, 4, 0) + theirs * pltpu.roll(w_theirs, 4, 0) + own * pltpu.roll(w_own, 4, 0)
            inverse = pltpu.roll(1.0 / jnp.where(is_max, 1.0, total), 4, 0)
            w_mine = w_mine * inverse
            w_theirs = w_theirs * inverse
            w_own = w_own * inverse
            values = []
            for pair in range(HEADS // 2):
                dims = slice(pair * HEAD_DIM, (pair + 1) * HEAD_DIM)
                one = slice(pair, pair + 1)
                values.append(o_buf[g, slot, dims, :] * w_mine[one] + x_recv[g, slot, dims, :] * w_theirs[one] + own_o[slot, dims, :] * w_own[one])
            turned = jnp.concatenate(values, axis=0).T
            for half in range(2):
                ctx[slot * CHUNK:(slot + 1) * CHUNK, half * QUAD:(half + 1) * QUAD] = turned[half * CHUNK:(half + 1) * CHUNK].astype(BF16)
        branch = jnp.dot(ctx[...], wo[...], preferred_element_type=F32) + mlp_acc[...]
        y_send[g] = branch[CHUNK:]
        y_copy(g).start()
        y_keep[g % 3] = y_keep[g % 3] + branch[:CHUNK]

    def y_stage(g):
        y_copy(g).wait_recv()
        fin[g, 0] = y_keep[g % 3] + y_recv[g]
        f_copy(g, 0, 2, 0, to_x).start()
        f_copy(g, 0, 1, 1, to_y).start()
        f_copy(g, 0, 4, 2, to_core).start()

    def forward_stage(g):
        f_copy(g, 0, 1, 1, to_y).wait_recv()
        f_copy(g, 0, 2, 0, to_x).wait_recv()

        @pl.when(g % 2 == 0)
        def _():
            f_copy(g, 1, 3, 3, to_x).start()

        @pl.when(g % 2 == 1)
        def _():
            f_copy(g, 2, 3, 3, to_y).start()

        f_copy(g, 1, 5, 4, to_core).start()
        f_copy(g, 2, 6, 5, to_core).start()

    def diagonal_stage(g):
        f_copy(g, 1, 3, 3, to_x).wait_recv()
        f_copy(g, 3, 7, 6, to_core).start()

    def out_stage(g):
        f_copy(g, 0, 4, 2, to_core).wait_recv()
        f_copy(g, 1, 5, 4, to_core).wait_recv()
        f_copy(g, 2, 6, 5, to_core).wait_recv()
        f_copy(g, 3, 7, 6, to_core).wait_recv()

        @pl.when(g >= 2)
        def _():
            for slot in range(GROUP):
                out_copy(g - 2, slot).wait()

        for slot in range(GROUP):
            stage[g % 2, slot] = fin[g, slot].astype(BF16)
            out_copy(g, slot).start()

    wqkv_copy.start()
    for copy in x_in(0):
        copy.start()
    for n in range(AHEAD):
        for copy in kv_copies(n):
            copy.start()
    barrier = pltpu.get_barrier_semaphore()
    for device in (to_core, to_x, to_y):
        pl.semaphore_signal(barrier, inc=1, device_id=device, device_id_type=pl.DeviceIdType.MESH)

    dim = lane % HEAD_DIM
    freq = jnp.zeros((CHUNK, PAIR), F32)
    for k in range(ROT_DIM // 2):
        here = jnp.logical_and(dim % (ROT_DIM // 2) == k, dim < ROT_DIM)
        freq = jnp.where(here, float(np.float32(ROPE_BASE ** (-2.0 * k / ROT_DIM))), freq)

    def one_angle(r, carry):
        trig[0, pl.ds(r, 1), :] = len_ref[r].astype(F32) * freq[:1]
        return carry

    lax.fori_loop(0, ROWS, one_angle, 0)
    angles = trig[0]
    trig[1] = jnp.sin(angles)
    trig[0] = jnp.cos(angles)
    angles = lax.broadcasted_iota(jnp.int32, (CHUNK, PAIR), 0).astype(F32) * freq
    trig[2] = jnp.cos(angles)
    trig[3] = jnp.sin(angles)
    q_bias, k_bias, v_bias = bias_parts(bq_ref[...].astype(F32).reshape(1, 3 * WIDTH))
    bias_q[...] = q_bias
    bias_kv[:, :WIDTH] = k_bias
    bias_kv[:, WIDTH:] = v_bias
    wqkv_copy.wait()

    def arrange(r, carry):
        rows = pl.ds(pl.multiple_of(r * PAIR, PAIR), PAIR)
        low = lax.broadcasted_iota(jnp.int32, (PAIR, PAIR), 1) < HEAD_DIM
        for pair in range(HEADS // 2):
            q_part, k_part, v_part = pick_parts([wu[rows, (3 * pair + k) * PAIR:(3 * pair + k + 1) * PAIR] for k in range(3)], low)
            wq[rows, pair * PAIR:(pair + 1) * PAIR] = q_part
            wkv[rows, pair * PAIR:(pair + 1) * PAIR] = k_part
            wkv[rows, WIDTH + pair * PAIR:WIDTH + (pair + 1) * PAIR] = v_part
        return carry

    lax.fori_loop(0, D_MODEL // PAIR, arrange, 0)
    for copy in w_copies:
        copy.start()
    pl.semaphore_wait(barrier, 3)

    def iteration(i, carry):
        @pl.when(i + 1 < GROUPS)
        def _():
            for copy in x_in(i + 1):
                copy.start()

        @pl.when(i == GROUPS)
        def _():
            for half in range(2):
                for copy in a_copies(GROUPS - 1, half):
                    copy.wait()

        @pl.when(jnp.logical_and(i > GROUPS, i < 2 * GROUPS))
        def _():
            for copy in kv_put(i - 1 - GROUPS):
                copy.wait()

        @pl.when(jnp.logical_and(i + 1 >= GROUPS, i + 1 < 2 * GROUPS))
        def _():
            for copy in a_back(i + 1 - GROUPS):
                copy.start()

        when_group(i - DIAGONAL_LAG, diagonal_stage)
        when_group(i - GROUPS, keys_values)

        @pl.when(i < GROUPS)
        def _():
            for copy in x_in(i):
                copy.wait()
            project(i, 0)
            project(i, 1)
            attend_group(i)
            core_stage(i)

        @pl.when(i >= GROUPS)
        def _():
            when_group(i - FORWARD_LAG, forward_stage)

        when_group(i - OUT_LAG, out_stage)
        when_group(i - 1, x_stage)

        @pl.when(i == 0)
        def _():
            for copy in w_copies:
                copy.wait()

        when_group(i, prepare)
        when_group(i - 2, y_stage)
        return carry

    lax.fori_loop(0, GROUPS + OUT_LAG, iteration, 0)
    for copy in kv_put(GROUPS - 1):
        copy.wait()
    for g in (GROUPS - 2, GROUPS - 1):
        for slot in range(GROUP):
            out_copy(g, slot).wait()

    def finish(g, carry):
        for copy in c_copies(g) + x_copies(g) + (y_copy(g),):
            copy.wait_send()
        for src, dst, k, device in ((0, 2, 0, to_x), (0, 1, 1, to_y), (0, 4, 2, to_core), (1, 3, 3, to_x), (1, 5, 4, to_core), (2, 6, 5, to_core), (3, 7, 6, to_core)):
            f_copy(g, src, dst, k, device).wait_send()
        return carry

    lax.fori_loop(0, GROUPS, finish, 0)


def layer_call(lengths, k_cache, v_cache, x, gain1, bias1, gain2, bias2, w_qkv, b_qkv, rot, w_out, w_up, b_up, w_down, b_out, b_down):
    vmem = pl.BlockSpec(memory_space=pltpu.VMEM)
    dma = pltpu.SemaphoreType.DMA
    return pl.pallas_call(
        layer_kernel,
        in_specs=[pl.BlockSpec(memory_space=pltpu.SMEM), ANY, ANY, ANY, vmem, vmem, vmem, vmem, ANY, vmem, vmem, ANY, ANY, vmem, ANY, vmem, vmem],
        out_specs=[ANY, ANY, ANY],
        out_shape=[
            jax.ShapeDtypeStruct((ROWS, CHUNK, D_MODEL), BF16),
            jax.ShapeDtypeStruct((ROWS, CHUNK, D_MODEL), BF16),
            jax.ShapeDtypeStruct((ROWS, CHUNK, D_MODEL), BF16),
        ],
        scratch_shapes=[
            pltpu.VMEM((WIDTH, D_MODEL), BF16),
            pltpu.VMEM((D_MODEL, FF), BF16),
            pltpu.VMEM((FF, D_MODEL), BF16),
            pltpu.VMEM((D_MODEL, WIDTH), BF16),
            pltpu.VMEM((D_MODEL, 2 * WIDTH), BF16),
            pltpu.VMEM((1, WIDTH), F32),
            pltpu.VMEM((1, 2 * WIDTH), F32),
            pltpu.VMEM((4, CHUNK, PAIR), F32),
            pltpu.VMEM((K_BUFS, WIDTH, SLOTS), BF16),
            pltpu.VMEM((V_BUFS, WIDTH, SLOTS), BF16),
            pltpu.VMEM((SLOTS, QUAD), F32),
            pltpu.VMEM((SLOTS, QUAD), F32),
            pltpu.VMEM((SLOTS, QUAD), BF16),
            pltpu.VMEM((SLOTS, QUAD), BF16),
            pltpu.VMEM((2, GROUP, CHUNK, D_MODEL), BF16),
            pltpu.VMEM((2, HALF * CHUNK, D_MODEL), BF16),
            pltpu.VMEM((GROUP, CHUNK, WIDTH), BF16),
            pltpu.VMEM((2, CHUNK, 2 * WIDTH), BF16),
            pltpu.VMEM((2, QUAD, PAIR), F32),
            pltpu.VMEM((2, 8, PAIR), F32),
            pltpu.VMEM((2 * CHUNK, D_MODEL), F32),
            pltpu.VMEM((GROUPS, GROUP, QUAD, PAIR), F32),
            pltpu.VMEM((GROUPS, 2, HALF, 8, PAIR), F32),
            pltpu.VMEM((GROUPS, HALF, QUAD, PAIR), F32),
            pltpu.VMEM((GROUPS, HALF, 8, PAIR), F32),
            pltpu.VMEM((GROUPS, HALF, 8, PAIR), F32),
            pltpu.VMEM((GROUPS, 2, QUAD, PAIR), F32),
            pltpu.VMEM((GROUPS, 2, 8, PAIR), F32),
            pltpu.VMEM((2 * CHUNK, WIDTH), BF16),
            pltpu.VMEM((GROUPS, CHUNK, D_MODEL), F32),
            pltpu.VMEM((3, CHUNK, D_MODEL), F32),
            pltpu.VMEM((GROUPS, CHUNK, D_MODEL), F32),
            pltpu.VMEM((GROUPS, GROUP, CHUNK, D_MODEL), F32),
            pltpu.VMEM((2, GROUP, CHUNK, D_MODEL), BF16),
            dma((3 + HEADS,)), dma((K_BUFS,)), dma((V_BUFS,)), dma((2, GROUP)), dma((2, HALF)), dma((2, GROUP)),
            dma((GROUPS, 2)), dma((GROUPS, 2)), dma((GROUPS, 2)), dma((GROUPS, 2)),
            dma((GROUPS,)), dma((GROUPS,)), dma((GROUPS, 7)), dma((GROUPS, GROUP)), dma((2, GROUP)),
        ],
        compiler_params=pltpu.CompilerParams(collective_id=0, has_side_effects=True, vmem_limit_bytes=67_000_000),
        cost_estimate=pl.CostEstimate(flops=30 * 10 ** 9, bytes_accessed=100 << 20, transcendentals=0),
        name="layer",
    )(lengths, k_cache, v_cache, x, gain1, bias1, gain2, bias2, w_qkv, b_qkv, rot, w_out, w_up, b_up, w_down, b_out, b_down)


def solution(mesh):
    in_specs = (P("dp", None, None), P("dp"), P("dp", "tp", "cp", None), P("dp", "tp", "cp", None), P(), P(), P(), P(), P(None, "tp"), P("tp"), P("tp", None), P(), P(None, "tp"), P("tp"), P("tp", None), P())
    out_specs = (P("dp", None, None), P("dp", "tp", None, None), P("dp", "tp", None, None))

    def local_layer(hidden_in, lengths, k_block, v_block, ln1_gain, ln1_bias, ln2_gain, ln2_bias, w_qkv, b_qkv, w_out, b_out, w_up, b_up, w_down, b_down):
        slot_minor = lambda cache: jnp.swapaxes(cache, 2, 3).reshape(ROWS, WIDTH, SLOTS)
        rot = jnp.asarray(rotate_matrix(), BF16)
        through, _, kv = layer_call(lengths, slot_minor(k_block), slot_minor(v_block), hidden_in, ln1_gain, ln1_bias, ln2_gain, ln2_bias, w_qkv, b_qkv, rot, w_out, w_up, b_up, w_down, b_out, b_down)
        return tail_call(kv, through)

    return jax.shard_map(local_layer, mesh=mesh, in_specs=in_specs, out_specs=out_specs, check_vma=False)
```

```python
import functools
import numpy as np
import jax
import jax.numpy as jnp
from jax import lax
from jax.experimental import pallas as pl
from jax.experimental.pallas import tpu as pltpu
from jax.sharding import PartitionSpec as P

EPSILON = 1e-5
NEG_BIG = -1e30
MAX_FLOOR = -1e29
ROPE_BASE = 10000.0
HEAD_DIM = 64
ROT_DIM = 16
PAIR = 2 * HEAD_DIM
ROWS = 64
CHUNK = 64
HEADS = 8
WIDTH = HEADS * HEAD_DIM
SLOTS = 512
D_MODEL = 1024
FF = 2048
GROUP = 8
GROUPS = ROWS // GROUP
K_BUFS = 3
V_BUFS = 5
AHEAD = 2
STRIP = 64
FORWARD_LAG = 5
DIAGONAL_LAG = 9
OUT_LAG = 9
QUAD = 4 * HEAD_DIM
HALF = GROUP // 2
TAIL_ROWS = 4
STATS = 4 * HEAD_DIM
SLAB = STATS + 8
TAIL_SLOTS = 4
F32 = jnp.float32
BF16 = jnp.bfloat16
ANY = pl.BlockSpec(memory_space=pl.ANY)


def normalize(x_f32, gain, bias):
    row_mean = jnp.mean(x_f32, axis=-1, keepdims=True)
    centered = x_f32 - row_mean
    variance = jnp.mean(centered * centered, axis=-1, keepdims=True)
    return (centered * lax.rsqrt(variance + EPSILON) * gain + bias).astype(BF16)


def rotate_matrix():
    matrix = np.zeros((PAIR, PAIR), np.float32)
    half = ROT_DIM // 2
    for base in (0, HEAD_DIM):
        for i in range(half):
            matrix[base + half + i, base + i] = -1.0
            matrix[base + i, base + half + i] = 1.0
    return matrix


def swap_halves(pair):
    return jnp.concatenate([pair[:, HEAD_DIM:], pair[:, :HEAD_DIM]], axis=1)


def pick_parts(blocks, low_half):
    first, second, third = blocks
    return jnp.where(low_half, first, second), swap_halves(jnp.where(low_half, third, first)), jnp.where(low_half, second, third)


def bias_parts(bias_row):
    low_half = lax.broadcasted_iota(jnp.int32, (1, PAIR), 1) < HEAD_DIM
    parts = [pick_parts([bias_row[:, (3 * pair + k) * PAIR:(3 * pair + k + 1) * PAIR] for k in range(3)], low_half) for pair in range(HEADS // 2)]
    return [jnp.concatenate([parts[pair][k] for pair in range(HEADS // 2)], axis=1) for k in range(3)]


def row_tables(trig, row):
    cos_len = trig[0, pl.ds(row, 1), :]
    sin_len = trig[1, pl.ds(row, 1), :]
    cos_c = trig[2]
    sin_c = trig[3]
    return cos_len * cos_c - sin_len * sin_c, sin_len * cos_c + cos_len * sin_c


def tail_kernel(kv_hbm, through_hbm, out_hbm, k_hbm, v_hbm, kv_all, passing, k_stage, v_stage, kv_sem, in_sem, out_sem, k_sem, v_sem):
    blocks = ROWS // TAIL_ROWS

    def rows(i):
        return pl.ds(i * TAIL_ROWS, TAIL_ROWS)

    kv_in = lambda i: pltpu.make_async_copy(kv_hbm.at[rows(i)], kv_all.at[i], kv_sem.at[i])
    pass_in = lambda i: pltpu.make_async_copy(through_hbm.at[rows(i)], passing.at[i], in_sem.at[i])
    pass_out = lambda i: pltpu.make_async_copy(passing.at[i], out_hbm.at[rows(i)], out_sem.at[i])
    k_put = lambda i: pltpu.make_async_copy(k_stage.at[i % TAIL_SLOTS], k_hbm.at[rows(i)], k_sem.at[i % TAIL_SLOTS])
    v_put = lambda i: pltpu.make_async_copy(v_stage.at[i % TAIL_SLOTS], v_hbm.at[rows(i)], v_sem.at[i % TAIL_SLOTS])

    for i in range(blocks):
        kv_in(i).start()
        pass_in(i).start()

    def step(i, carry):
        @pl.when(i >= TAIL_SLOTS)
        def _():
            k_put(i - TAIL_SLOTS).wait()
            v_put(i - TAIL_SLOTS).wait()

        kv_in(i).wait()
        slot = i % TAIL_SLOTS
        for row in range(TAIL_ROWS):
            for head in range(HEADS):
                dims = slice(head * HEAD_DIM, (head + 1) * HEAD_DIM)
                k_stage[slot, row, head] = kv_all[i, row, :, dims]
                v_stage[slot, row, head] = kv_all[i, row, :, WIDTH + head * HEAD_DIM:WIDTH + (head + 1) * HEAD_DIM]
        k_put(i).start()
        v_put(i).start()
        pass_in(i).wait()
        pass_out(i).start()
        return carry

    lax.fori_loop(0, blocks, step, 0)
    for i in range(blocks - TAIL_SLOTS, blocks):
        k_put(i).wait()
        v_put(i).wait()
    for i in range(blocks):
        pass_out(i).wait()


def tail_call(kv, through):
    blocks = ROWS // TAIL_ROWS
    dma = pltpu.SemaphoreType.DMA
    return pl.pallas_call(
        tail_kernel,
        in_specs=[ANY, ANY],
        out_specs=[ANY, ANY, ANY],
        out_shape=[
            jax.ShapeDtypeStruct((ROWS, CHUNK, D_MODEL), BF16),
            jax.ShapeDtypeStruct((ROWS, HEADS, CHUNK, HEAD_DIM), BF16),
            jax.ShapeDtypeStruct((ROWS, HEADS, CHUNK, HEAD_DIM), BF16),
        ],
        scratch_shapes=[
            pltpu.VMEM((blocks, TAIL_ROWS, CHUNK, D_MODEL), BF16),
            pltpu.VMEM((blocks, TAIL_ROWS, CHUNK, D_MODEL), BF16),
            pltpu.VMEM((TAIL_SLOTS, TAIL_ROWS, HEADS, CHUNK, HEAD_DIM), BF16),
            pltpu.VMEM((TAIL_SLOTS, TAIL_ROWS, HEADS, CHUNK, HEAD_DIM), BF16),
            dma((blocks,)), dma((blocks,)), dma((blocks,)), dma((TAIL_SLOTS,)), dma((TAIL_SLOTS,)),
        ],
        cost_estimate=pl.CostEstimate(flops=1 << 20, bytes_accessed=42 << 20, transcendentals=0),
        compiler_params=pltpu.CompilerParams(vmem_limit_bytes=60_000_000),
        name="tail",
    )(kv, through)


def layer_kernel(len_ref, kc_hbm, vc_hbm, x_hbm, gain1_ref, bias1_ref, gain2_ref, bias2_ref, wqkv_hbm, bq_ref, rot_ref, wo_hbm, wu_hbm, bu_ref, wd_hbm, bo_ref, bd_ref,
                 out_hbm, a_hbm, kv_hbm,
                 wo, wu, wd, wq, wkv, bias_q, bias_kv, trig, kbuf, vbuf, s0, s1, p0, p1, x_buf, a_buf, q_buf, kv_self, own_o, own_stat, mlp_acc,
                 o_buf, c_recv, x_recv, ctx, y_send, y_keep, y_recv, fin, stage,
                 w_sem, k_sem, v_sem, xin_sem, a_sem, kv_sem, send_sem, c_rsem, x_rsem, y_rsem, f_rsem, out_sem):
    tp_id = lax.axis_index("tp")
    cp_id = lax.axis_index("cp")
    chip_x = cp_id // 2
    core = cp_id % 2
    to_core = {"cp": 2 * chip_x + 1 - core}
    to_x = {"cp": 2 * (1 - chip_x) + core}
    to_y = {"tp": 1 - tp_id}

    def flip(bit, mine):
        return bit + mine - 2 * bit * mine

    def row_of(group, slot):
        return group * GROUP + 4 * flip(slot // 4, core) + 2 * flip((slot // 2) % 2, chip_x) + flip(slot % 2, tp_id)

    def remote(src, dst, ssem, rsem, device):
        return pltpu.make_async_remote_copy(src_ref=src, dst_ref=dst, send_sem=ssem, recv_sem=rsem, device_id=device, device_id_type=pl.DeviceIdType.MESH)

    def kv_copies(n):
        kb = n % K_BUFS
        vb = n % V_BUFS
        row = row_of(n // GROUP, (n % GROUP + 4) % GROUP)
        return (pltpu.make_async_copy(kc_hbm.at[row], kbuf.at[kb], k_sem.at[kb]), pltpu.make_async_copy(vc_hbm.at[row], vbuf.at[vb], v_sem.at[vb]))

    def x_in(g):
        return [pltpu.make_async_copy(x_hbm.at[row_of(g, slot)], x_buf.at[g % 2, slot], xin_sem.at[g % 2]) for slot in range(GROUP)]

    def a_copies(g, half):
        first = 4 - 4 * half
        return [pltpu.make_async_copy(a_buf.at[half, k], a_hbm.at[row_of(g, first + k)], a_sem.at[half]) for k in range(HALF)]

    wqkv_copy = pltpu.make_async_copy(wqkv_hbm, wu.at[:, pl.ds(0, 3 * WIDTH)], w_sem.at[0])
    w_copies = [pltpu.make_async_copy(wu_hbm, wu, w_sem.at[1]), pltpu.make_async_copy(wd_hbm, wd, w_sem.at[2])]
    for head in range(HEADS):
        w_copies.append(pltpu.make_async_copy(wo_hbm.at[pl.ds(head * HEAD_DIM, HEAD_DIM)], wo.at[pl.ds((head % 2) * QUAD + (head // 2) * HEAD_DIM, HEAD_DIM)], w_sem.at[3]))

    def a_back(g):
        return [pltpu.make_async_copy(a_hbm.at[row_of(g, slot)], x_buf.at[g % 2, slot], xin_sem.at[g % 2]) for slot in range(GROUP)]

    def x_arrived(g):
        pltpu.make_async_copy(x_hbm.at[pl.ds(0, GROUP)], x_buf.at[g % 2], xin_sem.at[g % 2]).wait()

    def a_written(half):
        pltpu.make_async_copy(a_buf.at[half], a_hbm.at[pl.ds(0, HALF)], a_sem.at[half]).wait()

    def kv_written(g):
        pltpu.make_async_copy(x_buf.at[g % 2], kv_hbm.at[pl.ds(0, GROUP)], kv_sem.at[g % 2]).wait()

    def out_written():
        pltpu.make_async_copy(stage, out_hbm.at[pl.ds(0, GROUP)], out_sem.at[0]).wait()

    def kv_put(g):
        return [pltpu.make_async_copy(x_buf.at[g % 2, slot], kv_hbm.at[row_of(g, slot)], kv_sem.at[g % 2]) for slot in range(GROUP)]

    def c_copies(g):
        return (remote(o_buf.at[g, pl.ds(4, 4)], c_recv.at[g], send_sem.at[0], c_rsem.at[g], to_core),)

    def x_copies(g):
        return (remote(o_buf.at[g, pl.ds(2, 2)], x_recv.at[g], send_sem.at[1], x_rsem.at[g], to_x),)

    def y_copy(g):
        return remote(y_send.at[g], y_recv.at[g], send_sem.at[2], y_rsem.at[g], to_y)

    def f_copy(g, src, dst, device):
        return remote(fin.at[g, src], fin.at[g, dst], send_sem.at[3], f_rsem.at[g, min(dst, 4)], device)

    def from_core(g):
        return remote(fin.at[g, pl.ds(0, 4)], fin.at[g, pl.ds(4, 4)], send_sem.at[3], f_rsem.at[g, 4], to_core)

    def out_copy(g, slot):
        return pltpu.make_async_copy(stage.at[slot], out_hbm.at[row_of(g, slot)], out_sem.at[0])

    lane = lax.broadcasted_iota(jnp.int32, (CHUNK, PAIR), 1)
    low_half = lane < HEAD_DIM
    is_max = lax.broadcasted_iota(jnp.int32, (8, PAIR), 0) < HEADS // 2
    quad_lane = lax.broadcasted_iota(jnp.int32, (CHUNK, QUAD), 1)

    def block_diagonal(q_quad):
        zero = jnp.zeros_like(q_quad)
        return jnp.concatenate([jnp.where(quad_lane // HEAD_DIM == k, q_quad, zero) for k in range(4)], axis=0)

    def rotate(values, turned, tables, scale):
        return ((values.astype(F32) * tables[0] + turned * tables[1]) * scale).astype(BF16)

    def project(g, half):
        first = 4 - 4 * half

        @pl.when(g >= 1)
        def _():
            a_written(half)

        x = x_buf[g % 2, first:first + HALF].reshape(HALF * CHUNK, D_MODEL).astype(F32)
        normed = normalize(x, gain1_ref[...].reshape(1, D_MODEL), bias1_ref[...].reshape(1, D_MODEL))
        a_buf[half] = normed.reshape(HALF, CHUNK, D_MODEL)
        for copy in a_copies(g, half):
            copy.start()
        q_all = (jnp.dot(normed, wq[...], preferred_element_type=F32) + bias_q[...]).astype(BF16)
        tables = [row_tables(trig, row_of(g, first + k)) for k in range(HALF)]
        for pair in range(HEADS // 2):
            cols = slice(pair * PAIR, (pair + 1) * PAIR)
            turned = jnp.dot(q_all[:, cols], rot_ref[...], preferred_element_type=F32)
            for k in range(HALF):
                tokens = slice(k * CHUNK, (k + 1) * CHUNK)
                q_buf[first + k, :, cols] = rotate(q_all[tokens, cols], turned[tokens], tables[k], HEAD_DIM ** -0.5)

    def slot_at(j):
        return (j + HALF) % GROUP

    def score_unit(g, j, quad, s_buf):
        slot = slot_at(j)
        dims = slice(quad * QUAD, (quad + 1) * QUAD)
        row_len = len_ref[row_of(g, slot)]
        valid = cp_id * SLOTS + lax.broadcasted_iota(jnp.int32, (SLOTS, QUAD), 0) < row_len
        q4 = block_diagonal(q_buf[slot, :, dims])
        scores = lax.dot_general(kbuf[(g * GROUP + j) % K_BUFS, dims, :], q4, (((0,), (1,)), ((), ())), preferred_element_type=F32)
        s_buf[...] = jnp.where(valid, scores, NEG_BIG)

    def soft_unit(g, j, quad, s_buf, p_buf):
        top = jnp.full((8, QUAD), MAX_FLOOR, F32)
        for k in range(SLOTS // STRIP):
            top = jnp.maximum(top, jnp.max(s_buf[k * STRIP:(k + 1) * STRIP, :].reshape(STRIP // 8, 8, QUAD), axis=0))
        top = jnp.max(top, axis=0, keepdims=True)
        total = jnp.zeros((8, QUAD), F32)
        for k in range(SLOTS // STRIP):
            slots = slice(k * STRIP, (k + 1) * STRIP)
            probs = jnp.exp(s_buf[slots, :] - top)
            total = total + jnp.sum(probs.reshape(STRIP // 8, 8, QUAD), axis=0)
            p_buf[slots, :] = probs.astype(BF16)
        total = jnp.sum(total, axis=0, keepdims=True)
        for sub in range(2):
            pair = 2 * quad + sub
            cols = slice(sub * PAIR, (sub + 1) * PAIR)
            o_buf[g, slot_at(j), STATS + pair:STATS + pair + 1, :] = top[:, cols]
            o_buf[g, slot_at(j), STATS + 4 + pair:STATS + 5 + pair, :] = total[:, cols]

    def value_unit(g, j, quad, p_buf):
        slot = slot_at(j)
        for sub in range(2):
            pair = 2 * quad + sub
            both = jnp.dot(vbuf[(g * GROUP + j) % V_BUFS, pair * PAIR:(pair + 1) * PAIR, :], p_buf[:, sub * PAIR:(sub + 1) * PAIR], preferred_element_type=F32)
            o_buf[g, slot, pair * HEAD_DIM:(pair + 1) * HEAD_DIM, :] = jnp.where(low_half, both[:HEAD_DIM], both[HEAD_DIM:])

    def when_group(g, work):
        @pl.when(jnp.logical_and(g >= 0, g < GROUPS))
        def _():
            work(g)

    def attend_group(g):
        first = g * GROUP

        def fetch(j):
            for copy in kv_copies(first + j):
                copy.wait()

            @pl.when(first + j + AHEAD < ROWS)
            def _():
                for copy in kv_copies(first + j + AHEAD):
                    copy.start()

        def scores_of(j):
            score_unit(g, j, 0, s0)
            score_unit(g, j, 1, s1)

        def soft_of(j):
            soft_unit(g, j, 0, s0, p0)
            soft_unit(g, j, 1, s1, p1)

        def values_of(j):
            value_unit(g, j, 0, p0)
            value_unit(g, j, 1, p1)

        fetch(0)
        scores_of(0)
        fetch(1)
        soft_of(0)
        scores_of(1)

        def step(j, carry):
            fetch(j)
            values_of(j - 2)
            soft_of(j - 1)
            scores_of(j)

            @pl.when(j == HALF + 1)
            def _():
                for copy in c_copies(g):
                    copy.start()
                when_group(g - FORWARD_LAG, forward_stage)

            return carry

        lax.fori_loop(2, GROUP, step, 0)
        values_of(GROUP - 2)
        soft_of(GROUP - 1)
        values_of(GROUP - 1)

    def core_stage(g):
        for copy in c_copies(g):
            copy.wait_recv()
        for slot in (2, 3, 0, 1):
            mine = o_buf[g, slot, STATS:, :]
            theirs = c_recv[g, slot, STATS:, :]
            top = jnp.maximum(mine, theirs)
            w_mine = jnp.exp(mine - top)
            w_theirs = jnp.exp(theirs - top)
            total = mine * pltpu.roll(w_mine, 4, 0) + theirs * pltpu.roll(w_theirs, 4, 0)
            o_buf[g, slot, STATS:, :] = jnp.where(is_max, top, total)
            for pair in range(HEADS // 2):
                dims = slice(pair * HEAD_DIM, (pair + 1) * HEAD_DIM)
                o_buf[g, slot, dims, :] = o_buf[g, slot, dims, :] * w_mine[pair:pair + 1] + c_recv[g, slot, dims, :] * w_theirs[pair:pair + 1]
            if slot == 3:
                for copy in x_copies(g):
                    copy.start()

    def prepare(g):
        kv = (jnp.dot(a_buf[1, :2].reshape(2 * CHUNK, D_MODEL), wkv[...], preferred_element_type=F32) + bias_kv[...]).astype(BF16)
        tables = [row_tables(trig, row_of(g, slot)) for slot in range(2)]
        for pair in range(HEADS // 2):
            cols = slice(pair * PAIR, (pair + 1) * PAIR)
            turned = jnp.dot(kv[:, cols], rot_ref[...], preferred_element_type=F32)
            for slot in range(2):
                tokens = slice(slot * CHUNK, (slot + 1) * CHUNK)
                kv_self[slot, :, cols] = rotate(kv[tokens, cols], turned[tokens], tables[slot], 1.0)
        for slot in range(2):
            kv_self[slot, :, WIDTH:] = kv[slot * CHUNK:(slot + 1) * CHUNK, WIDTH:]
        causal = lax.broadcasted_iota(jnp.int32, (CHUNK, QUAD), 0) <= quad_lane % CHUNK
        for slot in range(2):
            for quad in range(2):
                dims = slice(quad * QUAD, (quad + 1) * QUAD)
                q4 = block_diagonal(q_buf[slot, :, dims])
                scores = lax.dot_general(kv_self[slot, :, dims], q4, (((1,), (1,)), ((), ())), preferred_element_type=F32)
                scores = jnp.where(causal, scores, NEG_BIG)
                top = jnp.max(scores, axis=0, keepdims=True)
                probs = jnp.where(causal, jnp.exp(scores - top), 0.0)
                total = jnp.sum(probs, axis=0, keepdims=True)
                packed = probs.astype(BF16)
                for sub in range(2):
                    pair = 2 * quad + sub
                    cols = slice(sub * PAIR, (sub + 1) * PAIR)
                    both = lax.dot_general(kv_self[slot, :, WIDTH + pair * PAIR:WIDTH + (pair + 1) * PAIR], packed[:, cols], (((0,), (0,)), ((), ())), preferred_element_type=F32)
                    own_o[slot, pair * HEAD_DIM:(pair + 1) * HEAD_DIM, :] = jnp.where(low_half, both[:HEAD_DIM], both[HEAD_DIM:])
                    own_stat[slot, pair:pair + 1, :] = top[:, cols]
                    own_stat[slot, 4 + pair:5 + pair, :] = total[:, cols]
        x_both = x_buf[g % 2, :2].reshape(2 * CHUNK, D_MODEL).astype(F32)
        normed = normalize(x_both, gain2_ref[...].reshape(1, D_MODEL), bias2_ref[...].reshape(1, D_MODEL))
        up = jnp.dot(normed, wu[...], preferred_element_type=F32) + bu_ref[...].astype(F32).reshape(1, FF)
        hidden = (0.5 * up * (1.0 + lax.erf(up * (0.5 ** 0.5)))).astype(BF16)
        mlp_acc[...] = jnp.dot(hidden, wd[...], preferred_element_type=F32)
        y_keep[g % 3] = x_both[:CHUNK] + bo_ref[...].astype(F32).reshape(1, D_MODEL) + bd_ref[...].astype(F32).reshape(1, D_MODEL)

    def keys_values(g):
        b = g % 2
        x_arrived(g)
        for half in range(2):
            first = half * HALF
            a = x_buf[b, first:first + HALF].reshape(HALF * CHUNK, D_MODEL)
            kv = (jnp.dot(a, wkv[...], preferred_element_type=F32) + bias_kv[...]).astype(BF16)
            for pair in range(HEADS // 2):
                cols = slice(pair * PAIR, (pair + 1) * PAIR)
                turned = jnp.dot(kv[:, cols], rot_ref[...], preferred_element_type=F32)
                for k in range(HALF):
                    tokens = slice(k * CHUNK, (k + 1) * CHUNK)
                    x_buf[b, first + k, :, cols] = rotate(kv[tokens, cols], turned[tokens], row_tables(trig, row_of(g, first + k)), 1.0)
            for k in range(HALF):
                x_buf[b, first + k, :, WIDTH:] = kv[k * CHUNK:(k + 1) * CHUNK, WIDTH:]
        for copy in kv_put(g):
            copy.start()

    def x_stage(g):
        for copy in x_copies(g):
            copy.wait_recv()
        for slot in range(2):
            mine = o_buf[g, slot, STATS:, :]
            theirs = x_recv[g, slot, STATS:, :]
            own = own_stat[slot]
            top = jnp.maximum(jnp.maximum(mine, theirs), own)
            w_mine = jnp.exp(mine - top)
            w_theirs = jnp.exp(theirs - top)
            w_own = jnp.exp(own - top)
            total = mine * pltpu.roll(w_mine, 4, 0) + theirs * pltpu.roll(w_theirs, 4, 0) + own * pltpu.roll(w_own, 4, 0)
            inverse = pltpu.roll(1.0 / jnp.where(is_max, 1.0, total), 4, 0)
            w_mine = w_mine * inverse
            w_theirs = w_theirs * inverse
            w_own = w_own * inverse
            values = []
            for pair in range(HEADS // 2):
                dims = slice(pair * HEAD_DIM, (pair + 1) * HEAD_DIM)
                one = slice(pair, pair + 1)
                values.append(o_buf[g, slot, dims, :] * w_mine[one] + x_recv[g, slot, dims, :] * w_theirs[one] + own_o[slot, dims, :] * w_own[one])
            turned = jnp.concatenate(values, axis=0).T
            for half in range(2):
                ctx[slot * CHUNK:(slot + 1) * CHUNK, half * QUAD:(half + 1) * QUAD] = turned[half * CHUNK:(half + 1) * CHUNK].astype(BF16)
        branch = jnp.dot(ctx[...], wo[...], preferred_element_type=F32) + mlp_acc[...]
        y_send[g] = branch[CHUNK:]
        y_copy(g).start()
        y_keep[g % 3] = y_keep[g % 3] + branch[:CHUNK]

    def y_stage(g):
        y_copy(g).wait_recv()
        fin[g, 0] = y_keep[g % 3] + y_recv[g]
        f_copy(g, 0, 2, to_x).start()
        f_copy(g, 0, 1, to_y).start()
        f_copy(g, 0, 4, to_core).start()

    def forward_stage(g):
        f_copy(g, 0, 1, to_y).wait_recv()
        f_copy(g, 0, 2, to_x).wait_recv()

        @pl.when(g % 2 == 0)
        def _():
            f_copy(g, 1, 3, to_x).start()

        @pl.when(g % 2 == 1)
        def _():
            f_copy(g, 2, 3, to_y).start()

        f_copy(g, 1, 5, to_core).start()
        f_copy(g, 2, 6, to_core).start()

    def diagonal_stage(g):
        f_copy(g, 1, 3, to_x).wait_recv()
        f_copy(g, 3, 7, to_core).start()

    def out_stage(g):
        from_core(g).wait_recv()

        @pl.when(g >= 1)
        def _():
            out_written()

        for slot in range(GROUP):
            stage[slot] = fin[g, slot].astype(BF16)
            out_copy(g, slot).start()

    wqkv_copy.start()
    for copy in x_in(0):
        copy.start()
    barrier = pltpu.get_barrier_semaphore()
    for device in (to_core, to_x, to_y):
        pl.semaphore_signal(barrier, inc=1, device_id=device, device_id_type=pl.DeviceIdType.MESH)

    dim = lane % HEAD_DIM
    freq = jnp.zeros((CHUNK, PAIR), F32)
    for k in range(ROT_DIM // 2):
        here = jnp.logical_and(dim % (ROT_DIM // 2) == k, dim < ROT_DIM)
        freq = jnp.where(here, float(np.float32(ROPE_BASE ** (-2.0 * k / ROT_DIM))), freq)

    def one_angle(r, carry):
        trig[0, pl.ds(r, 1), :] = len_ref[r].astype(F32) * freq[:1]
        return carry

    lax.fori_loop(0, ROWS, one_angle, 0)
    angles = trig[0]
    trig[1] = jnp.sin(angles)
    trig[0] = jnp.cos(angles)
    angles = lax.broadcasted_iota(jnp.int32, (CHUNK, PAIR), 0).astype(F32) * freq
    trig[2] = jnp.cos(angles)
    trig[3] = jnp.sin(angles)
    q_bias, k_bias, v_bias = bias_parts(bq_ref[...].astype(F32).reshape(1, 3 * WIDTH))
    bias_q[...] = q_bias
    bias_kv[:, :WIDTH] = k_bias
    bias_kv[:, WIDTH:] = v_bias
    wqkv_copy.wait()
    for n in range(AHEAD):
        for copy in kv_copies(n):
            copy.start()

    def arrange(r, carry):
        rows = pl.ds(pl.multiple_of(r * PAIR, PAIR), PAIR)
        low = lax.broadcasted_iota(jnp.int32, (PAIR, PAIR), 1) < HEAD_DIM
        for pair in range(HEADS // 2):
            q_part, k_part, v_part = pick_parts([wu[rows, (3 * pair + k) * PAIR:(3 * pair + k + 1) * PAIR] for k in range(3)], low)
            wq[rows, pair * PAIR:(pair + 1) * PAIR] = q_part
            wkv[rows, pair * PAIR:(pair + 1) * PAIR] = k_part
            wkv[rows, WIDTH + pair * PAIR:WIDTH + (pair + 1) * PAIR] = v_part
        return carry

    lax.fori_loop(0, D_MODEL // PAIR, arrange, 0)
    for copy in w_copies:
        copy.start()
    pl.semaphore_wait(barrier, 3)

    def iteration(i, carry):
        @pl.when(i + 1 < GROUPS)
        def _():
            for copy in x_in(i + 1):
                copy.start()

        @pl.when(i == GROUPS)
        def _():
            for half in range(2):
                a_written(half)

        @pl.when(jnp.logical_and(i > GROUPS, i < 2 * GROUPS))
        def _():
            kv_written(i - 1 - GROUPS)

        @pl.when(jnp.logical_and(i + 1 >= GROUPS, i + 1 < 2 * GROUPS))
        def _():
            for copy in a_back(i + 1 - GROUPS):
                copy.start()

        when_group(i - DIAGONAL_LAG, diagonal_stage)
        when_group(i - GROUPS, keys_values)

        @pl.when(i < GROUPS)
        def _():
            x_arrived(i)
            project(i, 0)
            project(i, 1)
            attend_group(i)
            core_stage(i)

        @pl.when(i >= GROUPS)
        def _():
            when_group(i - FORWARD_LAG, forward_stage)

        when_group(i - OUT_LAG, out_stage)
        when_group(i - 1, x_stage)

        @pl.when(i == 0)
        def _():
            for copy in w_copies[:2]:
                copy.wait()
            pltpu.make_async_copy(wo_hbm, wo, w_sem.at[3]).wait()

        when_group(i, prepare)
        when_group(i - 2, y_stage)
        return carry

    lax.fori_loop(0, GROUPS + OUT_LAG, iteration, 0)
    kv_written(GROUPS - 1)
    out_written()

    remote(o_buf.at[pl.ds(0, GROUPS // 2)], o_buf.at[pl.ds(0, GROUPS // 2)], send_sem.at[0], c_rsem.at[0], to_core).wait_send()
    remote(o_buf.at[pl.ds(0, GROUPS // 4)], o_buf.at[pl.ds(0, GROUPS // 4)], send_sem.at[1], x_rsem.at[0], to_x).wait_send()
    remote(y_send, y_recv, send_sem.at[2], y_rsem.at[0], to_y).wait_send()
    remote(fin.at[pl.ds(0, GROUPS - 1)], fin.at[pl.ds(0, GROUPS - 1)], send_sem.at[3], f_rsem.at[0, 0], to_x).wait_send()


def layer_call(lengths, k_cache, v_cache, x, gain1, bias1, gain2, bias2, w_qkv, b_qkv, rot, w_out, w_up, b_up, w_down, b_out, b_down):
    vmem = pl.BlockSpec(memory_space=pltpu.VMEM)
    dma = pltpu.SemaphoreType.DMA
    return pl.pallas_call(
        layer_kernel,
        in_specs=[pl.BlockSpec(memory_space=pltpu.SMEM), ANY, ANY, ANY, vmem, vmem, vmem, vmem, ANY, vmem, vmem, ANY, ANY, vmem, ANY, vmem, vmem],
        out_specs=[ANY, ANY, ANY],
        out_shape=[
            jax.ShapeDtypeStruct((ROWS, CHUNK, D_MODEL), BF16),
            jax.ShapeDtypeStruct((ROWS, CHUNK, D_MODEL), BF16),
            jax.ShapeDtypeStruct((ROWS, CHUNK, D_MODEL), BF16),
        ],
        scratch_shapes=[
            pltpu.VMEM((WIDTH, D_MODEL), BF16),
            pltpu.VMEM((D_MODEL, FF), BF16),
            pltpu.VMEM((FF, D_MODEL), BF16),
            pltpu.VMEM((D_MODEL, WIDTH), BF16),
            pltpu.VMEM((D_MODEL, 2 * WIDTH), BF16),
            pltpu.VMEM((1, WIDTH), F32),
            pltpu.VMEM((1, 2 * WIDTH), F32),
            pltpu.VMEM((4, CHUNK, PAIR), F32),
            pltpu.VMEM((K_BUFS, WIDTH, SLOTS), BF16),
            pltpu.VMEM((V_BUFS, WIDTH, SLOTS), BF16),
            pltpu.VMEM((SLOTS, QUAD), F32),
            pltpu.VMEM((SLOTS, QUAD), F32),
            pltpu.VMEM((SLOTS, QUAD), BF16),
            pltpu.VMEM((SLOTS, QUAD), BF16),
            pltpu.VMEM((2, GROUP, CHUNK, D_MODEL), BF16),
            pltpu.VMEM((2, HALF, CHUNK, D_MODEL), BF16),
            pltpu.VMEM((GROUP, CHUNK, WIDTH), BF16),
            pltpu.VMEM((2, CHUNK, 2 * WIDTH), BF16),
            pltpu.VMEM((2, QUAD, PAIR), F32),
            pltpu.VMEM((2, 8, PAIR), F32),
            pltpu.VMEM((2 * CHUNK, D_MODEL), F32),
            pltpu.VMEM((GROUPS, GROUP, SLAB, PAIR), F32),
            pltpu.VMEM((GROUPS, HALF, SLAB, PAIR), F32),
            pltpu.VMEM((GROUPS, 2, SLAB, PAIR), F32),
            pltpu.VMEM((2 * CHUNK, WIDTH), BF16),
            pltpu.VMEM((GROUPS, CHUNK, D_MODEL), F32),
            pltpu.VMEM((3, CHUNK, D_MODEL), F32),
            pltpu.VMEM((GROUPS, CHUNK, D_MODEL), F32),
            pltpu.VMEM((GROUPS, GROUP, CHUNK, D_MODEL), F32),
            pltpu.VMEM((GROUP, CHUNK, D_MODEL), BF16),
            dma((4,)), dma((K_BUFS,)), dma((V_BUFS,)), dma((2,)), dma((2,)), dma((2,)),
            dma((4,)), dma((GROUPS,)), dma((GROUPS,)), dma((GROUPS,)), dma((GROUPS, 5)), dma((1,)),
        ],
        compiler_params=pltpu.CompilerParams(collective_id=0, has_side_effects=True, vmem_limit_bytes=67_000_000),
        cost_estimate=pl.CostEstimate(flops=30 * 10 ** 9, bytes_accessed=100 << 20, transcendentals=0),
        name="layer",
    )(lengths, k_cache, v_cache, x, gain1, bias1, gain2, bias2, w_qkv, b_qkv, rot, w_out, w_up, b_up, w_down, b_out, b_down)


def solution(mesh):
    in_specs = (P("dp", None, None), P("dp"), P("dp", "tp", "cp", None), P("dp", "tp", "cp", None), P(), P(), P(), P(), P(None, "tp"), P("tp"), P("tp", None), P(), P(None, "tp"), P("tp"), P("tp", None), P())
    out_specs = (P("dp", None, None), P("dp", "tp", None, None), P("dp", "tp", None, None))

    def local_layer(hidden_in, lengths, k_block, v_block, ln1_gain, ln1_bias, ln2_gain, ln2_bias, w_qkv, b_qkv, w_out, b_out, w_up, b_up, w_down, b_down):
        slot_minor = lambda cache: jnp.swapaxes(cache, 2, 3).reshape(ROWS, WIDTH, SLOTS)
        rot = jnp.asarray(rotate_matrix(), BF16)
        through, _, kv = layer_call(lengths, slot_minor(k_block), slot_minor(v_block), hidden_in, ln1_gain, ln1_bias, ln2_gain, ln2_bias, w_qkv, b_qkv, rot, w_out, w_up, b_up, w_down, b_out, b_down)
        return tail_call(kv, through)

    return jax.shard_map(local_layer, mesh=mesh, in_specs=in_specs, out_specs=out_specs, check_vma=False)
```

```python
import functools
import numpy as np
import jax
import jax.numpy as jnp
from jax import lax
from jax.experimental import pallas as pl
from jax.experimental.pallas import tpu as pltpu
from jax.sharding import PartitionSpec as P

EPSILON = 1e-5
NEG_BIG = -1e30
MAX_FLOOR = -1e29
ROPE_BASE = 10000.0
HEAD_DIM = 64
ROT_DIM = 16
PAIR = 2 * HEAD_DIM
ROWS = 64
CHUNK = 64
HEADS = 8
WIDTH = HEADS * HEAD_DIM
SLOTS = 512
D_MODEL = 1024
FF = 2048
GROUP = 8
GROUPS = ROWS // GROUP
K_BUFS = 3
V_BUFS = 5
AHEAD = 2
STRIP = 64
FORWARD_LAG = 5
DIAGONAL_LAG = 9
OUT_LAG = 9
QUAD = 4 * HEAD_DIM
HALF = GROUP // 2
TAIL_ROWS = 8
STATS = 4 * HEAD_DIM
SLAB = STATS + 8
TAIL_SLOTS = 2
F32 = jnp.float32
BF16 = jnp.bfloat16
ANY = pl.BlockSpec(memory_space=pl.ANY)


def normalize(x_f32, gain, bias):
    row_mean = jnp.mean(x_f32, axis=-1, keepdims=True)
    centered = x_f32 - row_mean
    variance = jnp.mean(centered * centered, axis=-1, keepdims=True)
    return (centered * lax.rsqrt(variance + EPSILON) * gain + bias).astype(BF16)


def rotate_matrix():
    matrix = np.zeros((PAIR, PAIR), np.float32)
    half = ROT_DIM // 2
    for base in (0, HEAD_DIM):
        for i in range(half):
            matrix[base + half + i, base + i] = -1.0
            matrix[base + i, base + half + i] = 1.0
    return matrix


def swap_halves(pair):
    return jnp.concatenate([pair[:, HEAD_DIM:], pair[:, :HEAD_DIM]], axis=1)


def pick_parts(blocks, low_half):
    first, second, third = blocks
    return jnp.where(low_half, first, second), swap_halves(jnp.where(low_half, third, first)), jnp.where(low_half, second, third)


def bias_parts(bias_row):
    low_half = lax.broadcasted_iota(jnp.int32, (1, PAIR), 1) < HEAD_DIM
    parts = [pick_parts([bias_row[:, (3 * pair + k) * PAIR:(3 * pair + k + 1) * PAIR] for k in range(3)], low_half) for pair in range(HEADS // 2)]
    return [jnp.concatenate([parts[pair][k] for pair in range(HEADS // 2)], axis=1) for k in range(3)]


def row_tables(trig, row):
    cos_len = trig[0, pl.ds(row, 1), :]
    sin_len = trig[1, pl.ds(row, 1), :]
    cos_c = trig[2]
    sin_c = trig[3]
    return cos_len * cos_c - sin_len * sin_c, sin_len * cos_c + cos_len * sin_c


def tail_kernel(kv_hbm, through_hbm, out_hbm, k_hbm, v_hbm, kv_all, passing, k_stage, v_stage, kv_sem, in_sem, out_sem, k_sem, v_sem):
    blocks = ROWS // TAIL_ROWS

    def rows(i):
        return pl.ds(i * TAIL_ROWS, TAIL_ROWS)

    kv_in = lambda i: pltpu.make_async_copy(kv_hbm.at[rows(i)], kv_all.at[i], kv_sem.at[i])
    pass_in = lambda i: pltpu.make_async_copy(through_hbm.at[rows(i)], passing.at[rows(i)], in_sem.at[i])
    pass_out = lambda i: pltpu.make_async_copy(passing.at[rows(i)], out_hbm.at[rows(i)], out_sem.at[0])
    k_put = lambda i: pltpu.make_async_copy(k_stage.at[i % TAIL_SLOTS], k_hbm.at[rows(i)], k_sem.at[i % TAIL_SLOTS])
    v_put = lambda i: pltpu.make_async_copy(v_stage.at[i % TAIL_SLOTS], v_hbm.at[rows(i)], v_sem.at[i % TAIL_SLOTS])

    for i in range(blocks):
        kv_in(i).start()
        pass_in(i).start()

    def step(i, carry):
        @pl.when(i >= TAIL_SLOTS)
        def _():
            k_put(i - TAIL_SLOTS).wait()
            v_put(i - TAIL_SLOTS).wait()

        kv_in(i).wait()
        slot = i % TAIL_SLOTS
        for row in range(TAIL_ROWS):
            for head in range(HEADS):
                dims = slice(head * HEAD_DIM, (head + 1) * HEAD_DIM)
                k_stage[slot, row, head] = kv_all[i, row, :, dims]
                v_stage[slot, row, head] = kv_all[i, row, :, WIDTH + head * HEAD_DIM:WIDTH + (head + 1) * HEAD_DIM]
        k_put(i).start()
        v_put(i).start()
        pass_in(i).wait()
        pass_out(i).start()
        return carry

    lax.fori_loop(0, blocks, step, 0)
    for i in range(blocks - TAIL_SLOTS, blocks):
        k_put(i).wait()
        v_put(i).wait()
    pltpu.make_async_copy(passing, out_hbm, out_sem.at[0]).wait()


def tail_call(kv, through):
    blocks = ROWS // TAIL_ROWS
    dma = pltpu.SemaphoreType.DMA
    return pl.pallas_call(
        tail_kernel,
        in_specs=[ANY, ANY],
        out_specs=[ANY, ANY, ANY],
        out_shape=[
            jax.ShapeDtypeStruct((ROWS, CHUNK, D_MODEL), BF16),
            jax.ShapeDtypeStruct((ROWS, HEADS, CHUNK, HEAD_DIM), BF16),
            jax.ShapeDtypeStruct((ROWS, HEADS, CHUNK, HEAD_DIM), BF16),
        ],
        scratch_shapes=[
            pltpu.VMEM((blocks, TAIL_ROWS, CHUNK, D_MODEL), BF16),
            pltpu.VMEM((ROWS, CHUNK, D_MODEL), BF16),
            pltpu.VMEM((TAIL_SLOTS, TAIL_ROWS, HEADS, CHUNK, HEAD_DIM), BF16),
            pltpu.VMEM((TAIL_SLOTS, TAIL_ROWS, HEADS, CHUNK, HEAD_DIM), BF16),
            dma((blocks,)), dma((blocks,)), dma((1,)), dma((TAIL_SLOTS,)), dma((TAIL_SLOTS,)),
        ],
        cost_estimate=pl.CostEstimate(flops=1 << 20, bytes_accessed=42 << 20, transcendentals=0),
        compiler_params=pltpu.CompilerParams(vmem_limit_bytes=60_000_000),
        name="tail",
    )(kv, through)


def layer_kernel(len_ref, kc_hbm, vc_hbm, x_hbm, gain1_ref, bias1_ref, gain2_ref, bias2_ref, wqkv_hbm, bq_ref, rot_ref, wo_hbm, wu_hbm, bu_ref, wd_hbm, bo_ref, bd_ref,
                 out_hbm, a_hbm, kv_hbm,
                 wo, wu, wd, wq, wkv, bias_q, bias_kv, trig, kbuf, vbuf, s0, s1, p0, p1, x_buf, a_buf, q_buf, kv_self, own_o, own_stat, mlp_acc,
                 o_buf, c_recv, x_recv, ctx, y_send, y_keep, y_recv, fin, stage,
                 w_sem, k_sem, v_sem, xin_sem, a_sem, kv_sem, send_sem, c_rsem, x_rsem, y_rsem, f_rsem, out_sem):
    tp_id = lax.axis_index("tp")
    cp_id = lax.axis_index("cp")
    chip_x = cp_id // 2
    core = cp_id % 2
    to_core = {"cp": 2 * chip_x + 1 - core}
    to_x = {"cp": 2 * (1 - chip_x) + core}
    to_y = {"tp": 1 - tp_id}

    def flip(bit, mine):
        return bit + mine - 2 * bit * mine

    def row_of(group, slot):
        return group * GROUP + 4 * flip(slot // 4, core) + 2 * flip((slot // 2) % 2, chip_x) + flip(slot % 2, tp_id)

    def remote(src, dst, ssem, rsem, device):
        return pltpu.make_async_remote_copy(src_ref=src, dst_ref=dst, send_sem=ssem, recv_sem=rsem, device_id=device, device_id_type=pl.DeviceIdType.MESH)

    def kv_copies(n):
        kb = n % K_BUFS
        vb = n % V_BUFS
        row = row_of(n // GROUP, (n % GROUP + 4) % GROUP)
        return (pltpu.make_async_copy(kc_hbm.at[row], kbuf.at[kb], k_sem.at[kb]), pltpu.make_async_copy(vc_hbm.at[row], vbuf.at[vb], v_sem.at[vb]))

    def x_in(g):
        return [pltpu.make_async_copy(x_hbm.at[row_of(g, slot)], x_buf.at[g % 2, slot], xin_sem.at[g % 2]) for slot in range(GROUP)]

    def a_copies(g, half):
        first = 4 - 4 * half
        return [pltpu.make_async_copy(a_buf.at[half, k], a_hbm.at[row_of(g, first + k)], a_sem.at[half]) for k in range(HALF)]

    wqkv_copy = pltpu.make_async_copy(wqkv_hbm, wu.at[:, pl.ds(0, 3 * WIDTH)], w_sem.at[0])
    w_copies = [pltpu.make_async_copy(wu_hbm, wu, w_sem.at[1]), pltpu.make_async_copy(wd_hbm, wd, w_sem.at[2])]
    for head in range(HEADS):
        w_copies.append(pltpu.make_async_copy(wo_hbm.at[pl.ds(head * HEAD_DIM, HEAD_DIM)], wo.at[pl.ds((head % 2) * QUAD + (head // 2) * HEAD_DIM, HEAD_DIM)], w_sem.at[3]))

    def a_back(g):
        return [pltpu.make_async_copy(a_hbm.at[row_of(g, slot)], x_buf.at[g % 2, slot], xin_sem.at[g % 2]) for slot in range(GROUP)]

    def x_arrived(g):
        pltpu.make_async_copy(x_hbm.at[pl.ds(0, GROUP)], x_buf.at[g % 2], xin_sem.at[g % 2]).wait()

    def a_written(half):
        pltpu.make_async_copy(a_buf.at[half], a_hbm.at[pl.ds(0, HALF)], a_sem.at[half]).wait()

    def kv_written(g):
        pltpu.make_async_copy(x_buf.at[g % 2], kv_hbm.at[pl.ds(0, GROUP)], kv_sem.at[g % 2]).wait()

    def out_written():
        pltpu.make_async_copy(stage, out_hbm.at[pl.ds(0, GROUP)], out_sem.at[0]).wait()

    def kv_put(g):
        return [pltpu.make_async_copy(x_buf.at[g % 2, slot], kv_hbm.at[row_of(g, slot)], kv_sem.at[g % 2]) for slot in range(GROUP)]

    def c_copies(g):
        return (remote(o_buf.at[g, pl.ds(4, 4)], c_recv.at[g], send_sem.at[0], c_rsem.at[g], to_core),)

    def x_copies(g):
        return (remote(o_buf.at[g, pl.ds(2, 2)], x_recv.at[g], send_sem.at[1], x_rsem.at[g], to_x),)

    def y_copy(g):
        return remote(y_send.at[g], y_recv.at[g], send_sem.at[2], y_rsem.at[g], to_y)

    def f_copy(g, src, dst, device):
        return remote(fin.at[g, src], fin.at[g, dst], send_sem.at[3], f_rsem.at[g, min(dst, 4)], device)

    def from_core(g):
        return remote(fin.at[g, pl.ds(0, 4)], fin.at[g, pl.ds(4, 4)], send_sem.at[3], f_rsem.at[g, 4], to_core)

    def out_copy(g, slot):
        return pltpu.make_async_copy(stage.at[slot], out_hbm.at[row_of(g, slot)], out_sem.at[0])

    lane = lax.broadcasted_iota(jnp.int32, (CHUNK, PAIR), 1)
    low_half = lane < HEAD_DIM
    is_max = lax.broadcasted_iota(jnp.int32, (8, PAIR), 0) < HEADS // 2
    quad_lane = lax.broadcasted_iota(jnp.int32, (CHUNK, QUAD), 1)

    def block_diagonal(q_quad):
        zero = jnp.zeros_like(q_quad)
        return jnp.concatenate([jnp.where(quad_lane // HEAD_DIM == k, q_quad, zero) for k in range(4)], axis=0)

    def rotate(values, turned, tables, scale):
        return ((values.astype(F32) * tables[0] + turned * tables[1]) * scale).astype(BF16)

    def project(g, half):
        first = 4 - 4 * half

        @pl.when(g >= 1)
        def _():
            a_written(half)

        x = x_buf[g % 2, first:first + HALF].reshape(HALF * CHUNK, D_MODEL).astype(F32)
        normed = normalize(x, gain1_ref[...].reshape(1, D_MODEL), bias1_ref[...].reshape(1, D_MODEL))
        a_buf[half] = normed.reshape(HALF, CHUNK, D_MODEL)
        for copy in a_copies(g, half):
            copy.start()
        q_all = (jnp.dot(normed, wq[...], preferred_element_type=F32) + bias_q[...]).astype(BF16)
        tables = [row_tables(trig, row_of(g, first + k)) for k in range(HALF)]
        for pair in range(HEADS // 2):
            cols = slice(pair * PAIR, (pair + 1) * PAIR)
            turned = jnp.dot(q_all[:, cols], rot_ref[...], preferred_element_type=F32)
            for k in range(HALF):
                tokens = slice(k * CHUNK, (k + 1) * CHUNK)
                q_buf[first + k, :, cols] = rotate(q_all[tokens, cols], turned[tokens], tables[k], HEAD_DIM ** -0.5)

    def slot_at(j):
        return (j + HALF) % GROUP

    def score_unit(g, j, quad, s_buf):
        slot = slot_at(j)
        dims = slice(quad * QUAD, (quad + 1) * QUAD)
        row_len = len_ref[row_of(g, slot)]
        valid = cp_id * SLOTS + lax.broadcasted_iota(jnp.int32, (SLOTS, QUAD), 0) < row_len
        q4 = block_diagonal(q_buf[slot, :, dims])
        scores = lax.dot_general(kbuf[(g * GROUP + j) % K_BUFS, dims, :], q4, (((0,), (1,)), ((), ())), preferred_element_type=F32)
        s_buf[...] = jnp.where(valid, scores, NEG_BIG)

    def soft_unit(g, j, quad, s_buf, p_buf):
        top = jnp.full((8, QUAD), MAX_FLOOR, F32)
        for k in range(SLOTS // STRIP):
            top = jnp.maximum(top, jnp.max(s_buf[k * STRIP:(k + 1) * STRIP, :].reshape(STRIP // 8, 8, QUAD), axis=0))
        top = jnp.max(top, axis=0, keepdims=True)
        total = jnp.zeros((8, QUAD), F32)
        for k in range(SLOTS // STRIP):
            slots = slice(k * STRIP, (k + 1) * STRIP)
            probs = jnp.exp(s_buf[slots, :] - top)
            total = total + jnp.sum(probs.reshape(STRIP // 8, 8, QUAD), axis=0)
            p_buf[slots, :] = probs.astype(BF16)
        total = jnp.sum(total, axis=0, keepdims=True)
        for sub in range(2):
            pair = 2 * quad + sub
            cols = slice(sub * PAIR, (sub + 1) * PAIR)
            o_buf[g, slot_at(j), STATS + pair:STATS + pair + 1, :] = top[:, cols]
            o_buf[g, slot_at(j), STATS + 4 + pair:STATS + 5 + pair, :] = total[:, cols]

    def value_unit(g, j, quad, p_buf):
        slot = slot_at(j)
        for sub in range(2):
            pair = 2 * quad + sub
            both = jnp.dot(vbuf[(g * GROUP + j) % V_BUFS, pair * PAIR:(pair + 1) * PAIR, :], p_buf[:, sub * PAIR:(sub + 1) * PAIR], preferred_element_type=F32)
            o_buf[g, slot, pair * HEAD_DIM:(pair + 1) * HEAD_DIM, :] = jnp.where(low_half, both[:HEAD_DIM], both[HEAD_DIM:])

    def when_group(g, work):
        @pl.when(jnp.logical_and(g >= 0, g < GROUPS))
        def _():
            work(g)

    def attend_group(g):
        first = g * GROUP

        def fetch(j):
            for copy in kv_copies(first + j):
                copy.wait()

            @pl.when(first + j + AHEAD < ROWS)
            def _():
                for copy in kv_copies(first + j + AHEAD):
                    copy.start()

        def scores_of(j):
            score_unit(g, j, 0, s0)
            score_unit(g, j, 1, s1)

        def soft_of(j):
            soft_unit(g, j, 0, s0, p0)
            soft_unit(g, j, 1, s1, p1)

        def values_of(j):
            value_unit(g, j, 0, p0)
            value_unit(g, j, 1, p1)

        fetch(0)
        scores_of(0)
        fetch(1)
        soft_of(0)
        scores_of(1)

        def step(j, carry):
            fetch(j)
            values_of(j - 2)
            soft_of(j - 1)
            scores_of(j)

            @pl.when(j == HALF + 1)
            def _():
                for copy in c_copies(g):
                    copy.start()
                when_group(g - FORWARD_LAG, forward_stage)

            return carry

        lax.fori_loop(2, GROUP, step, 0)
        values_of(GROUP - 2)
        soft_of(GROUP - 1)
        values_of(GROUP - 1)

    def core_stage(g):
        for copy in c_copies(g):
            copy.wait_recv()
        for slot in (2, 3, 0, 1):
            mine = o_buf[g, slot, STATS:, :]
            theirs = c_recv[g, slot, STATS:, :]
            top = jnp.maximum(mine, theirs)
            w_mine = jnp.exp(mine - top)
            w_theirs = jnp.exp(theirs - top)
            total = mine * pltpu.roll(w_mine, 4, 0) + theirs * pltpu.roll(w_theirs, 4, 0)
            o_buf[g, slot, STATS:, :] = jnp.where(is_max, top, total)
            for pair in range(HEADS // 2):
                dims = slice(pair * HEAD_DIM, (pair + 1) * HEAD_DIM)
                o_buf[g, slot, dims, :] = o_buf[g, slot, dims, :] * w_mine[pair:pair + 1] + c_recv[g, slot, dims, :] * w_theirs[pair:pair + 1]
            if slot == 3:
                for copy in x_copies(g):
                    copy.start()

    def prepare(g):
        kv = (jnp.dot(a_buf[1, :2].reshape(2 * CHUNK, D_MODEL), wkv[...], preferred_element_type=F32) + bias_kv[...]).astype(BF16)
        tables = [row_tables(trig, row_of(g, slot)) for slot in range(2)]
        for pair in range(HEADS // 2):
            cols = slice(pair * PAIR, (pair + 1) * PAIR)
            turned = jnp.dot(kv[:, cols], rot_ref[...], preferred_element_type=F32)
            for slot in range(2):
                tokens = slice(slot * CHUNK, (slot + 1) * CHUNK)
                kv_self[slot, :, cols] = rotate(kv[tokens, cols], turned[tokens], tables[slot], 1.0)
        for slot in range(2):
            kv_self[slot, :, WIDTH:] = kv[slot * CHUNK:(slot + 1) * CHUNK, WIDTH:]
        causal = lax.broadcasted_iota(jnp.int32, (CHUNK, QUAD), 0) <= quad_lane % CHUNK
        for slot in range(2):
            for quad in range(2):
                dims = slice(quad * QUAD, (quad + 1) * QUAD)
                q4 = block_diagonal(q_buf[slot, :, dims])
                scores = lax.dot_general(kv_self[slot, :, dims], q4, (((1,), (1,)), ((), ())), preferred_element_type=F32)
                scores = jnp.where(causal, scores, NEG_BIG)
                top = jnp.max(scores, axis=0, keepdims=True)
                probs = jnp.where(causal, jnp.exp(scores - top), 0.0)
                total = jnp.sum(probs, axis=0, keepdims=True)
                packed = probs.astype(BF16)
                for sub in range(2):
                    pair = 2 * quad + sub
                    cols = slice(sub * PAIR, (sub + 1) * PAIR)
                    both = lax.dot_general(kv_self[slot, :, WIDTH + pair * PAIR:WIDTH + (pair + 1) * PAIR], packed[:, cols], (((0,), (0,)), ((), ())), preferred_element_type=F32)
                    own_o[slot, pair * HEAD_DIM:(pair + 1) * HEAD_DIM, :] = jnp.where(low_half, both[:HEAD_DIM], both[HEAD_DIM:])
                    own_stat[slot, pair:pair + 1, :] = top[:, cols]
                    own_stat[slot, 4 + pair:5 + pair, :] = total[:, cols]
        x_both = x_buf[g % 2, :2].reshape(2 * CHUNK, D_MODEL).astype(F32)
        normed = normalize(x_both, gain2_ref[...].reshape(1, D_MODEL), bias2_ref[...].reshape(1, D_MODEL))
        up = jnp.dot(normed, wu[...], preferred_element_type=F32) + bu_ref[...].astype(F32).reshape(1, FF)
        hidden = (0.5 * up * (1.0 + lax.erf(up * (0.5 ** 0.5)))).astype(BF16)
        mlp_acc[...] = jnp.dot(hidden, wd[...], preferred_element_type=F32)
        y_keep[g % 3] = x_both[:CHUNK] + bo_ref[...].astype(F32).reshape(1, D_MODEL) + bd_ref[...].astype(F32).reshape(1, D_MODEL)

    def keys_values(g):
        b = g % 2
        x_arrived(g)
        for half in range(2):
            first = half * HALF
            a = x_buf[b, first:first + HALF].reshape(HALF * CHUNK, D_MODEL)
            kv = (jnp.dot(a, wkv[...], preferred_element_type=F32) + bias_kv[...]).astype(BF16)
            for pair in range(HEADS // 2):
                cols = slice(pair * PAIR, (pair + 1) * PAIR)
                turned = jnp.dot(kv[:, cols], rot_ref[...], preferred_element_type=F32)
                for k in range(HALF):
                    tokens = slice(k * CHUNK, (k + 1) * CHUNK)
                    x_buf[b, first + k, :, cols] = rotate(kv[tokens, cols], turned[tokens], row_tables(trig, row_of(g, first + k)), 1.0)
            for k in range(HALF):
                x_buf[b, first + k, :, WIDTH:] = kv[k * CHUNK:(k + 1) * CHUNK, WIDTH:]
        for copy in kv_put(g):
            copy.start()

    def x_stage(g):
        for copy in x_copies(g):
            copy.wait_recv()
        for slot in range(2):
            mine = o_buf[g, slot, STATS:, :]
            theirs = x_recv[g, slot, STATS:, :]
            own = own_stat[slot]
            top = jnp.maximum(jnp.maximum(mine, theirs), own)
            w_mine = jnp.exp(mine - top)
            w_theirs = jnp.exp(theirs - top)
            w_own = jnp.exp(own - top)
            total = mine * pltpu.roll(w_mine, 4, 0) + theirs * pltpu.roll(w_theirs, 4, 0) + own * pltpu.roll(w_own, 4, 0)
            inverse = pltpu.roll(1.0 / jnp.where(is_max, 1.0, total), 4, 0)
            w_mine = w_mine * inverse
            w_theirs = w_theirs * inverse
            w_own = w_own * inverse
            values = []
            for pair in range(HEADS // 2):
                dims = slice(pair * HEAD_DIM, (pair + 1) * HEAD_DIM)
                one = slice(pair, pair + 1)
                values.append(o_buf[g, slot, dims, :] * w_mine[one] + x_recv[g, slot, dims, :] * w_theirs[one] + own_o[slot, dims, :] * w_own[one])
            turned = jnp.concatenate(values, axis=0).T
            for half in range(2):
                ctx[slot * CHUNK:(slot + 1) * CHUNK, half * QUAD:(half + 1) * QUAD] = turned[half * CHUNK:(half + 1) * CHUNK].astype(BF16)
        branch = jnp.dot(ctx[...], wo[...], preferred_element_type=F32) + mlp_acc[...]
        y_send[g] = branch[CHUNK:]
        y_copy(g).start()
        y_keep[g % 3] = y_keep[g % 3] + branch[:CHUNK]

    def y_stage(g):
        y_copy(g).wait_recv()
        fin[g, 0] = y_keep[g % 3] + y_recv[g]
        f_copy(g, 0, 2, to_x).start()
        f_copy(g, 0, 1, to_y).start()
        f_copy(g, 0, 4, to_core).start()

    def forward_stage(g):
        f_copy(g, 0, 1, to_y).wait_recv()
        f_copy(g, 0, 2, to_x).wait_recv()

        @pl.when(g % 2 == 0)
        def _():
            f_copy(g, 1, 3, to_x).start()

        @pl.when(g % 2 == 1)
        def _():
            f_copy(g, 2, 3, to_y).start()

        f_copy(g, 1, 5, to_core).start()
        f_copy(g, 2, 6, to_core).start()

    def diagonal_stage(g):
        f_copy(g, 1, 3, to_x).wait_recv()
        f_copy(g, 3, 7, to_core).start()

    def out_stage(g):
        @pl.when(g >= 1)
        def _():
            out_written()

        for slot in range(GROUP):
            if slot == 4:
                from_core(g).wait_recv()
            stage[slot] = fin[g, slot].astype(BF16)
            out_copy(g, slot).start()

    wqkv_copy.start()
    for copy in x_in(0):
        copy.start()
    barrier = pltpu.get_barrier_semaphore()
    for device in (to_core, to_x, to_y):
        pl.semaphore_signal(barrier, inc=1, device_id=device, device_id_type=pl.DeviceIdType.MESH)

    dim = lane % HEAD_DIM
    freq = jnp.zeros((CHUNK, PAIR), F32)
    for k in range(ROT_DIM // 2):
        here = jnp.logical_and(dim % (ROT_DIM // 2) == k, dim < ROT_DIM)
        freq = jnp.where(here, float(np.float32(ROPE_BASE ** (-2.0 * k / ROT_DIM))), freq)

    def one_angle(r, carry):
        trig[0, pl.ds(r, 1), :] = len_ref[r].astype(F32) * freq[:1]
        return carry

    lax.fori_loop(0, ROWS, one_angle, 0)
    angles = trig[0]
    trig[1] = jnp.sin(angles)
    trig[0] = jnp.cos(angles)
    angles = lax.broadcasted_iota(jnp.int32, (CHUNK, PAIR), 0).astype(F32) * freq
    trig[2] = jnp.cos(angles)
    trig[3] = jnp.sin(angles)
    q_bias, k_bias, v_bias = bias_parts(bq_ref[...].astype(F32).reshape(1, 3 * WIDTH))
    bias_q[...] = q_bias
    bias_kv[:, :WIDTH] = k_bias
    bias_kv[:, WIDTH:] = v_bias
    wqkv_copy.wait()
    for n in range(AHEAD):
        for copy in kv_copies(n):
            copy.start()

    def arrange(r, carry):
        rows = pl.ds(pl.multiple_of(r * PAIR, PAIR), PAIR)
        low = lax.broadcasted_iota(jnp.int32, (PAIR, PAIR), 1) < HEAD_DIM
        for pair in range(HEADS // 2):
            q_part, k_part, v_part = pick_parts([wu[rows, (3 * pair + k) * PAIR:(3 * pair + k + 1) * PAIR] for k in range(3)], low)
            wq[rows, pair * PAIR:(pair + 1) * PAIR] = q_part
            wkv[rows, pair * PAIR:(pair + 1) * PAIR] = k_part
            wkv[rows, WIDTH + pair * PAIR:WIDTH + (pair + 1) * PAIR] = v_part
        return carry

    lax.fori_loop(0, D_MODEL // PAIR, arrange, 0)
    for copy in w_copies:
        copy.start()
    pl.semaphore_wait(barrier, 3)

    def iteration(i, carry):
        @pl.when(i + 1 < GROUPS)
        def _():
            for copy in x_in(i + 1):
                copy.start()

        @pl.when(i == GROUPS)
        def _():
            for half in range(2):
                a_written(half)

        @pl.when(jnp.logical_and(i > GROUPS, i < 2 * GROUPS))
        def _():
            kv_written(i - 1 - GROUPS)

        @pl.when(jnp.logical_and(i + 1 >= GROUPS, i + 1 < 2 * GROUPS))
        def _():
            for copy in a_back(i + 1 - GROUPS):
                copy.start()

        when_group(i - DIAGONAL_LAG, diagonal_stage)
        when_group(i - GROUPS, keys_values)

        @pl.when(i < GROUPS)
        def _():
            x_arrived(i)
            project(i, 0)
            project(i, 1)
            attend_group(i)
            core_stage(i)

        @pl.when(i >= GROUPS)
        def _():
            when_group(i - FORWARD_LAG, forward_stage)

        when_group(i - OUT_LAG, out_stage)
        when_group(i - 1, x_stage)

        @pl.when(i == 0)
        def _():
            for copy in w_copies[:2]:
                copy.wait()
            pltpu.make_async_copy(wo_hbm, wo, w_sem.at[3]).wait()

        when_group(i, prepare)
        when_group(i - 2, y_stage)
        return carry

    lax.fori_loop(0, GROUPS + OUT_LAG, iteration, 0)
    kv_written(GROUPS - 1)
    out_written()

    remote(o_buf.at[pl.ds(0, GROUPS // 2)], o_buf.at[pl.ds(0, GROUPS // 2)], send_sem.at[0], c_rsem.at[0], to_core).wait_send()
    remote(o_buf.at[pl.ds(0, GROUPS // 4)], o_buf.at[pl.ds(0, GROUPS // 4)], send_sem.at[1], x_rsem.at[0], to_x).wait_send()
    remote(y_send, y_recv, send_sem.at[2], y_rsem.at[0], to_y).wait_send()
    remote(fin.at[pl.ds(0, GROUPS - 1)], fin.at[pl.ds(0, GROUPS - 1)], send_sem.at[3], f_rsem.at[0, 0], to_x).wait_send()


def layer_call(lengths, k_cache, v_cache, x, gain1, bias1, gain2, bias2, w_qkv, b_qkv, rot, w_out, w_up, b_up, w_down, b_out, b_down):
    vmem = pl.BlockSpec(memory_space=pltpu.VMEM)
    dma = pltpu.SemaphoreType.DMA
    return pl.pallas_call(
        layer_kernel,
        in_specs=[pl.BlockSpec(memory_space=pltpu.SMEM), ANY, ANY, ANY, vmem, vmem, vmem, vmem, ANY, vmem, vmem, ANY, ANY, vmem, ANY, vmem, vmem],
        out_specs=[ANY, ANY, ANY],
        out_shape=[
            jax.ShapeDtypeStruct((ROWS, CHUNK, D_MODEL), BF16),
            jax.ShapeDtypeStruct((ROWS, CHUNK, D_MODEL), BF16),
            jax.ShapeDtypeStruct((ROWS, CHUNK, D_MODEL), BF16),
        ],
        scratch_shapes=[
            pltpu.VMEM((WIDTH, D_MODEL), BF16),
            pltpu.VMEM((D_MODEL, FF), BF16),
            pltpu.VMEM((FF, D_MODEL), BF16),
            pltpu.VMEM((D_MODEL, WIDTH), BF16),
            pltpu.VMEM((D_MODEL, 2 * WIDTH), BF16),
            pltpu.VMEM((1, WIDTH), F32),
            pltpu.VMEM((1, 2 * WIDTH), F32),
            pltpu.VMEM((4, CHUNK, PAIR), F32),
            pltpu.VMEM((K_BUFS, WIDTH, SLOTS), BF16),
            pltpu.VMEM((V_BUFS, WIDTH, SLOTS), BF16),
            pltpu.VMEM((SLOTS, QUAD), F32),
            pltpu.VMEM((SLOTS, QUAD), F32),
            pltpu.VMEM((SLOTS, QUAD), BF16),
            pltpu.VMEM((SLOTS, QUAD), BF16),
            pltpu.VMEM((2, GROUP, CHUNK, D_MODEL), BF16),
            pltpu.VMEM((2, HALF, CHUNK, D_MODEL), BF16),
            pltpu.VMEM((GROUP, CHUNK, WIDTH), BF16),
            pltpu.VMEM((2, CHUNK, 2 * WIDTH), BF16),
            pltpu.VMEM((2, QUAD, PAIR), F32),
            pltpu.VMEM((2, 8, PAIR), F32),
            pltpu.VMEM((2 * CHUNK, D_MODEL), F32),
            pltpu.VMEM((GROUPS, GROUP, SLAB, PAIR), F32),
            pltpu.VMEM((GROUPS, HALF, SLAB, PAIR), F32),
            pltpu.VMEM((GROUPS, 2, SLAB, PAIR), F32),
            pltpu.VMEM((2 * CHUNK, WIDTH), BF16),
            pltpu.VMEM((GROUPS, CHUNK, D_MODEL), F32),
            pltpu.VMEM((3, CHUNK, D_MODEL), F32),
            pltpu.VMEM((GROUPS, CHUNK, D_MODEL), F32),
            pltpu.VMEM((GROUPS, GROUP, CHUNK, D_MODEL), F32),
            pltpu.VMEM((GROUP, CHUNK, D_MODEL), BF16),
            dma((4,)), dma((K_BUFS,)), dma((V_BUFS,)), dma((2,)), dma((2,)), dma((2,)),
            dma((4,)), dma((GROUPS,)), dma((GROUPS,)), dma((GROUPS,)), dma((GROUPS, 5)), dma((1,)),
        ],
        compiler_params=pltpu.CompilerParams(collective_id=0, has_side_effects=True, vmem_limit_bytes=67_000_000),
        cost_estimate=pl.CostEstimate(flops=30 * 10 ** 9, bytes_accessed=100 << 20, transcendentals=0),
        name="layer",
    )(lengths, k_cache, v_cache, x, gain1, bias1, gain2, bias2, w_qkv, b_qkv, rot, w_out, w_up, b_up, w_down, b_out, b_down)


def solution(mesh):
    in_specs = (P("dp", None, None), P("dp"), P("dp", "tp", "cp", None), P("dp", "tp", "cp", None), P(), P(), P(), P(), P(None, "tp"), P("tp"), P("tp", None), P(), P(None, "tp"), P("tp"), P("tp", None), P())
    out_specs = (P("dp", None, None), P("dp", "tp", None, None), P("dp", "tp", None, None))

    def local_layer(hidden_in, lengths, k_block, v_block, ln1_gain, ln1_bias, ln2_gain, ln2_bias, w_qkv, b_qkv, w_out, b_out, w_up, b_up, w_down, b_down):
        slot_minor = lambda cache: jnp.swapaxes(cache, 2, 3).reshape(ROWS, WIDTH, SLOTS)
        rot = jnp.asarray(rotate_matrix(), BF16)
        through, _, kv = layer_call(lengths, slot_minor(k_block), slot_minor(v_block), hidden_in, ln1_gain, ln1_bias, ln2_gain, ln2_bias, w_qkv, b_qkv, rot, w_out, w_up, b_up, w_down, b_out, b_down)
        return tail_call(kv, through)

    return jax.shard_map(local_layer, mesh=mesh, in_specs=in_specs, out_specs=out_specs, check_vma=False)
```
